128 devices in a mesh: gx: 8 (over z, core), gy: 16 (over y, x).
Axes of the slice: x: 4, y: 4, z: 4, core: 2. Of those that a mesh axis runs over, the one named last changes fastest.
Arguments:
- gradient: float32 [64, 4096], P('gx', 'gy'), may hold values from -6 to 6
- warm_start: float32 [64, 4096], P('gx', 'gy'), may hold values from -3 to 3
- viscosity: float32 [32, 64, 4096], P(None, 'gx', 'gy'), may hold values from 1 to 10
- friction_coef: float32 [64, 4096], P('gx', 'gy'), may hold values from 0.5 to 5
- slide_dir: float32 [2, 64, 4096], P(None, 'gx', 'gy'), may hold values from -4 to 4
- obs_weight: float32 [64, 4096], P('gx', 'gy'), may hold values from 0.5 to 2
- ice_mask: int32 [64, 4096], P('gx', 'gy'), may hold values 0 or 1
- grounded: int32 [64, 4096], P('gx', 'gy'), may hold values 0 or 1
Outputs:
- solution: float32 [64, 4096], P('gx', 'gy')
- residual: float32 [64, 4096], P('gx', 'gy')
The draws below stay inside these ranges and needn't reach their ends.
All inputs are finite; a program needn't handle non-finite values. No bound on the sum of `ice_mask` or of `grounded` on one device may be relied on, other than what follows from the above.
Results may differ from the reference program's by a relative error of at most 0.00075.
Values sent between devices are 32-bit elements; how exact they have to be, the bound alone decides.
A program may use at most 128 MiB of HBM per device.

```python
import math
import jax
import jax.numpy as jnp

NZ = 32
ITERS = 2
NX = 64
NY = 4096


def plant(entries, rng, smallest, high):
    spot = [jax.random.randint(jax.random.fold_in(rng, axis), (), 0, length) for axis, length in enumerate(entries.shape)]
    longest = entries.shape.index(max(entries.shape))
    neighbour = spot[:longest] + [(spot[longest] + 1) % entries.shape[longest]] + spot[longest + 1:]
    return entries.at[tuple(spot)].set(smallest).at[tuple(neighbour)].set(high)


def block_levels(own_key, dims, shards, smallest, high):
    def one(dim, parts):
        steps = jax.random.uniform(jax.random.fold_in(jax.random.fold_in(own_key, 6), dim), (parts,), jnp.float32, smallest / len(shards), high / len(shards))
        return jnp.repeat(jnp.exp(steps), dims[dim] // parts).reshape((-1,) + (1,) * (len(dims) - dim - 1))

    gain = one(*shards[0])
    for cut in shards[1:]:
        gain = gain * one(*cut)
    return gain


def normal_values(key, dims, scale, limit, pieces=(), kind=jnp.bfloat16):
    values = jax.random.normal(key, dims, jnp.float32) * scale
    if len(pieces) > 0:
        values = block_levels(key, dims, pieces, -0.22, 0.18) * values
    return jnp.clip(values, min=-limit, max=limit).astype(kind)


def setup_inputs(seed: int = 0) -> dict:
    keys = jax.random.split(jax.random.key(seed), 9)
    gradient = normal_values(keys[0], (NX, NY), 1.0, 6.0, ((0, 8), (1, 16)), jnp.float32)
    warm_start = normal_values(keys[1], (NX, NY), 0.5, 3.0, ((0, 8), (1, 16)), jnp.float32)
    viscosity = jnp.clip(jnp.exp(math.log(10.0) - 2.3025851 * jax.random.uniform(keys[2], (NZ, NX, NY), jnp.float32) ** block_levels(keys[2], (NZ, NX, NY), ((1, 8), (2, 16)), -0.2, 0.2)), 1.0, 10.0)
    friction_coef = jnp.clip(jnp.exp(math.log(5.0) - 2.3025851 * jax.random.uniform(keys[3], (NX, NY), jnp.float32) ** block_levels(keys[3], (NX, NY), ((0, 8), (1, 16)), -0.2, 0.2)), 0.5, 5.0)
    slide_dir = normal_values(keys[4], (2, NX, NY), 1.0, 4.0, ((1, 8), (2, 16)), jnp.float32)
    obs_weight = jnp.clip(jnp.exp(math.log(2.0) - 1.3862944 * jax.random.uniform(keys[5], (NX, NY), jnp.float32) ** block_levels(keys[5], (NX, NY), ((0, 8), (1, 16)), -0.2, 0.2)), 0.5, 2.0)
    ice_mask = plant((jax.random.randint(keys[6], (NX, NY), 0, 8) < 7).astype(jnp.int32), jax.random.fold_in(keys[6], 1), 0, 1)
    grounded = plant((jax.random.randint(keys[7], (NX, NY), 0, 4) < 3).astype(jnp.int32), jax.random.fold_in(keys[7], 1), 0, 1)
    return {"gradient": gradient, "warm_start": warm_start, "viscosity": viscosity, "friction_coef": friction_coef, "slide_dir": slide_dir, "obs_weight": obs_weight, "ice_mask": ice_mask, "grounded": grounded}


vert_coupling = 128.0
sink_rate = 0.0625
bed_drag = 0.5
offset_weight = 0.0019
cross_share = 0.5
reg_gamma = 0.02
reg_smooth = 1.0
diag_scale = 0.003

neighbour_offsets = [(step_z, step_x, step_y) for step_z in (-1, 0, 1) for step_x in (-1, 0, 1) for step_y in (-1, 0, 1) if step_x != 0 or step_y != 0]


def couple(field_ext, eta_ext):
    levels = eta_ext.shape[0]
    span_x = eta_ext.shape[1] - 2
    span_y = eta_ext.shape[2] - 2
    padded_field = jnp.pad(field_ext, ((0, 0), (1, 1), (0, 0), (0, 0)))
    padded_eta = jnp.pad(eta_ext, ((1, 1), (0, 0), (0, 0)))
    center = eta_ext[:, 1:1 + span_x, 1:1 + span_y]
    along_one = jnp.zeros((levels, span_x, span_y), jnp.float32)
    along_two = jnp.zeros((levels, span_x, span_y), jnp.float32)
    for step_z, step_x, step_y in neighbour_offsets:
        near_eta = padded_eta[1 + step_z:1 + step_z + levels, 1 + step_x:1 + step_x + span_x, 1 + step_y:1 + step_y + span_y]
        weight = (offset_weight / (abs(step_x) + abs(step_y) + abs(step_z))) * 0.5 * (center + near_eta)
        near_field = padded_field[:, 1 + step_z:1 + step_z + levels, 1 + step_x:1 + step_x + span_x, 1 + step_y:1 + step_y + span_y]
        along_one = along_one + weight * near_field[0]
        along_two = along_two + weight * near_field[1]
        if step_x != 0 and step_y != 0:
            twist_weight = (cross_share * step_x * step_y) * weight
            along_one = along_one + twist_weight * near_field[1]
            along_two = along_two + twist_weight * near_field[0]
    return jnp.stack([along_one, along_two])


def tridiagonal(link_weights, diagonal, rhs_cols):
    levels = diagonal.shape[0]
    pivot_value = diagonal[0]
    ratios = [-link_weights[0] / pivot_value]
    partial_value = [rhs_cols[:, 0] / pivot_value]
    for layer_index in range(1, levels):
        pivot_value = diagonal[layer_index] + link_weights[layer_index - 1] * ratios[-1]
        partial_value.append((rhs_cols[:, layer_index] + link_weights[layer_index - 1] * partial_value[-1]) / pivot_value)
        if layer_index < levels - 1:
            ratios.append(-link_weights[layer_index] / pivot_value)
    result = [partial_value[-1]]
    for layer_index in range(levels - 2, -1, -1):
        result.insert(0, partial_value[layer_index] - ratios[layer_index] * result[0])
    return jnp.stack(result, axis=1)


def responses(viscosity, friction):
    levels = viscosity.shape[0]
    link_weights = vert_coupling * 0.5 * (viscosity[:-1] + viscosity[1:])
    zero_layer = jnp.zeros_like(viscosity[:1])
    diagonal = jnp.concatenate([zero_layer, link_weights]) + jnp.concatenate([link_weights, zero_layer]) + sink_rate * viscosity
    diagonal = diagonal.at[0].add(bed_drag * friction)
    unit_rhs = jnp.zeros((2,) + viscosity.shape, jnp.float32)
    unit_rhs = unit_rhs.at[0, 0].set(1.0).at[1, levels - 1].set(1.0)
    solved = tridiagonal(link_weights, diagonal, unit_rhs)
    return solved[0], solved[1]


def regularize(centre_ext):
    middle = centre_ext[1:-1, 1:-1]
    beside_all = centre_ext[2:, 1:-1] + centre_ext[:-2, 1:-1] + centre_ext[1:-1, 2:] + centre_ext[1:-1, :-2]
    return reg_gamma * (middle + reg_smooth * (4.0 * middle - beside_all))


def reference(gradient, warm_start, viscosity, friction_coef, slide_dir, obs_weight, ice_mask, grounded):
    ice_float = ice_mask.astype(jnp.float32)
    ground_float = grounded.astype(jnp.float32)
    friction = ground_float * friction_coef
    source = (ice_float * ground_float * friction_coef)[None] * slide_dir
    obs = ice_float * obs_weight
    inverse_diag = 1.0 / (reg_gamma * (1.0 + 4.0 * reg_smooth) + diag_scale * ice_float * ground_float * friction_coef * friction_coef)
    bottom_resp, top_resp = responses(viscosity, friction)
    eta_ext = jnp.pad(viscosity, ((0, 0), (1, 1), (1, 1)))

    def hessian(direction):
        spread = source * direction[None]
        first_state = bottom_resp[None] * spread[:, None]
        coupled = couple(jnp.pad(first_state, ((0, 0), (0, 0), (1, 1), (1, 1))), eta_ext)
        surface = spread * bottom_resp[-1][None] + jnp.sum(top_resp[None] * coupled, axis=1)
        traction = obs[None] * surface
        second_state = top_resp[None] * traction[:, None]
        coupled_back = couple(jnp.pad(second_state, ((0, 0), (0, 0), (1, 1), (1, 1))), eta_ext)
        basal_part = traction * top_resp[0][None] + jnp.sum(bottom_resp[None] * coupled_back, axis=1)
        return jnp.sum(source * basal_part, axis=0) + regularize(jnp.pad(direction, 1))

    solution = warm_start
    residual = gradient - hessian(warm_start)
    precond = inverse_diag * residual
    direction = precond
    norm_now = jnp.sum(residual * precond)
    for iteration in range(ITERS):
        image_vec = hessian(direction)
        step_size = norm_now / jnp.sum(direction * image_vec)
        solution = solution + step_size * direction
        residual = residual - step_size * image_vec
        precond = inverse_diag * residual
        norm_next = jnp.sum(residual * precond)
        direction = precond + (norm_next / norm_now) * direction
        norm_now = norm_next
    return solution, residual
```

```python
import functools

import jax
import jax.numpy as jnp
from jax import lax
from jax.experimental import pallas as pl
from jax.experimental.pallas import tpu as pltpu
from jax.sharding import PartitionSpec as P

MESH = pl.DeviceIdType.MESH
F32 = jnp.float32

VERT_COUPLING = 128.0
SINK_RATE = 0.0625
BED_DRAG = 0.5
OFFSET_WEIGHT = 0.0019
CROSS_SHARE = 0.5
REG_GAMMA = 0.02
REG_SMOOTH = 1.0
DIAG_SCALE = 0.003

ROWS = 8
LANES = 128
NEIGHBOURS = [(dx, dy) for dx in (-1, 0, 1) for dy in (-1, 0, 1) if (dx, dy) != (0, 0)]
SIDEWAYS = [(dx, dy) for dx in (-1, 0, 1) for dy in (-1, 1)]


def row_roll(tile, shift):
    return pltpu.roll(tile, shift % ROWS, axis=0)


def lane_roll(tile, shift):
    shift = shift % LANES
    return tile if shift == 0 else pltpu.roll(tile, shift, axis=1)


def kernel(
    grad_h, warm_h, eta_h, coef_h, slide_h, weight_h, ice_h, ground_h,
    sol_o, res_o,
    grad_v, warm_v, eta_v, coef_v, slide_v, weight_v, ice_v, ground_v,
    w_v, u_v, inva_v,
    wrow_s, wrow_r, wedge_s, wedge_r,
    frow_s, frow_r, fedge_s, fedge_r,
    krow_s, krow_r, kedge_s, kedge_r,
    suma_s, suma_r, sumb_s, sumb_r,
    in_sem, row_send, row_recv, edge_send, edge_recv, suma_send, suma_recv, sumb_send, sumb_recv,
    *, nx, ny, levels,
):
    mx = lax.axis_index("gx")
    my = lax.axis_index("gy")

    def at(dx, dy):
        return (lax.rem(mx + (dx + nx), nx), lax.rem(my + (dy + ny), ny))

    pairs = [
        (eta_h, eta_v), (coef_h, coef_v), (ground_h, ground_v), (ice_h, ice_v),
        (slide_h, slide_v), (weight_h, weight_v), (grad_h, grad_v), (warm_h, warm_v),
    ]
    loads = [pltpu.make_async_copy(src, dst, in_sem.at[i]) for i, (src, dst) in enumerate(pairs)]
    for load in loads:
        load.start()

    barrier = pltpu.get_barrier_semaphore()
    peers = [at(dx, dy) for dx, dy in NEIGHBOURS]
    peers += [at(k, 0) for k in range(2, nx - 1)]
    peers += [at(0, k) for k in range(2, ny - 1)]
    for peer in peers:
        pl.semaphore_signal(barrier, inc=1, device_id=peer, device_id_type=MESH)

    row_id = lax.broadcasted_iota(jnp.int32, (ROWS, LANES), 0)
    lane_id = lax.broadcasted_iota(jnp.int32, (ROWS, LANES), 1)
    row_first = row_id == 0
    row_last = row_id == ROWS - 1
    lane_first = lane_id == 0
    lane_last = lane_id == LANES - 1
    low_half = lane_id < LANES // 2

    def tiles(value):
        return [value[:, :LANES], value[:, LANES:]]

    for load in loads[:3]:
        load.wait()
    friction = ground_v[...].astype(F32) * coef_v[...]

    slot = lambda z, f: 2 * (levels - 1 - z) + f
    rows_packed = None
    edge_packed = jnp.zeros((ROWS, LANES), F32)
    w = jnp.ones((ROWS, 2 * LANES), F32)
    eta = eta_v[levels - 1]
    flux = SINK_RATE * eta
    for z in range(levels - 1, -1, -1):
        if z < levels - 1:
            above, eta = eta, eta_v[z]
            inva = 1.0 / ((0.5 * VERT_COUPLING) * (above + eta))
            inva_v[z] = inva
            w = w + flux * inva
            flux = flux + (SINK_RATE * eta) * w
        for f, field in enumerate((w, eta * w)):
            m = slot(z, f)
            w_v[m] = field
            r = m % 4
            parts = [row_roll(t, 2 * r) for t in tiles(field)]
            if r == 0:
                rows_packed = parts
            else:
                here = (row_id == 2 * r) | (row_id == 2 * r - 1)
                rows_packed = [jnp.where(here, a, b) for a, b in zip(parts, rows_packed)]
            if r == 3:
                wrow_s[m // 4, :, :LANES] = rows_packed[0]
                wrow_s[m // 4, :, LANES:] = rows_packed[1]
            t0, t1 = tiles(field)
            both = lane_roll(jnp.where(low_half, t0, t1), 2 * m)
            here = (lane_id == 2 * m) | (lane_id == (2 * m - 1) % LANES)
            edge_packed = jnp.where(here, both, edge_packed)
    wedge_s[...] = edge_packed
    total = flux + BED_DRAG * friction * w
    gain = 1.0 / total

    pl.semaphore_wait(barrier, len(peers))

    sends = []

    def send_rows(stage, src, dst):
        out = []
        for k, dx in enumerate((1, -1)):
            copy = pltpu.make_async_remote_copy(
                src_ref=src, dst_ref=dst.at[k],
                send_sem=row_send.at[stage, k], recv_sem=row_recv.at[stage, k],
                device_id=at(dx, 0), device_id_type=MESH,
            )
            copy.start()
            out.append(copy)
        sends.extend(out)
        return out

    def send_edges(stage, src, dst):
        out = []
        for k, (dx, dy) in enumerate(SIDEWAYS):
            copy = pltpu.make_async_remote_copy(
                src_ref=src, dst_ref=dst.at[k],
                send_sem=edge_send.at[stage, k], recv_sem=edge_recv.at[stage, k],
                device_id=at(dx, dy), device_id_type=MESH,
            )
            copy.start()
            out.append(copy)
        sends.extend(out)
        return out

    w_copies = send_edges(0, wedge_s, wedge_r) + send_rows(0, wrow_s, wrow_r)

    for load in loads[3:]:
        load.wait()
    ice = ice_v[...].astype(F32)
    coef = coef_v[...]
    stuck = ice * ground_v[...].astype(F32)
    source_gain = stuck * coef * gain
    fields = [
        source_gain * slide_v[0],
        source_gain * slide_v[1],
        ice * weight_v[...],
        1.0 / (REG_GAMMA * (1.0 + 4.0 * REG_SMOOTH) + DIAG_SCALE * stuck * coef * coef),
        grad_v[...],
        warm_v[...],
    ]

    def pack_edges(values):
        packed = jnp.zeros((ROWS, LANES), F32)
        for f, value in enumerate(values):
            t0, t1 = tiles(value)
            both = lane_roll(jnp.where(low_half, t0, t1), 16 * f)
            group = ((lane_id + 8) % LANES) // 16 == f
            packed = jnp.where(group, both, packed)
        return packed

    for f, value in enumerate(fields):
        frow_s[f] = value
    fedge_s[...] = pack_edges(fields)
    f_copies = send_edges(1, fedge_s, fedge_r) + send_rows(1, frow_s, frow_r)

    u = jnp.ones((ROWS, 2 * LANES), F32)
    flux = SINK_RATE * eta_v[0] + BED_DRAG * friction
    u_v[0] = u
    for z in range(1, levels):
        u = u + flux * inva_v[z - 1]
        flux = flux + (SINK_RATE * eta_v[z]) * u
        u_v[z] = u

    has_up = mx < nx - 1
    has_down = mx > 0
    has_right = my < ny - 1
    has_left = my > 0

    def inside(value, *flags):
        keep = flags[0]
        for flag in flags[1:]:
            keep = keep & flag
        return jnp.where(keep, value, 0.0)

    def join_edges(ref, from_right):
        def got(dx, dy):
            return ref[SIDEWAYS.index((-dx, -dy))]

        own = jnp.where(
            from_right, inside(got(0, 1), has_right), inside(got(0, -1), has_left)
        )
        up = jnp.where(
            from_right, inside(got(1, 1), has_right, has_up), inside(got(1, -1), has_left, has_up)
        )
        down = jnp.where(
            from_right,
            inside(got(-1, 1), has_right, has_down),
            inside(got(-1, -1), has_left, has_down),
        )
        return own, up, down

    for copy in w_copies:
        copy.wait_recv()

    even_lane = lane_id % 2 == 0
    even_row = row_id % 2 == 0
    e_own, e_up, e_down = join_edges(wedge_r, even_lane)
    e_beyond = jnp.where(row_id < 4, e_up, e_down)
    e_plus = row_roll(jnp.where(row_first, e_beyond, e_own), -1)
    e_minus = row_roll(jnp.where(row_last, e_beyond, e_own), 1)
    edge_of = {0: e_own, 1: e_plus, -1: e_minus}

    sums = {n: [None, None] for n in NEIGHBOURS}
    beyond_rows = [None, None]
    for zi in range(levels):
        z = levels - 1 - zi
        eta = eta_v[z]
        u = u_v[z]
        near_u = jnp.zeros_like(u)
        near_eu = jnp.zeros_like(u)
        if z > 0:
            near_u = near_u + u_v[z - 1]
            near_eu = near_eu + u_v[z - 1] * eta_v[z - 1]
        if z < levels - 1:
            near_u = near_u + u_v[z + 1]
            near_eu = near_eu + u_v[z + 1] * eta_v[z + 1]
        eu = eta * u
        straight = (eu + 0.5 * near_eu, u + 0.5 * near_u)
        slanted = (0.5 * eu + (1.0 / 3.0) * near_eu, 0.5 * u + (1.0 / 3.0) * near_u)
        for f in range(2):
            m = slot(z, f)
            g, r = m // 4, m % 4
            if r == 0:
                from_down = inside(wrow_r[0, g], has_down)
                from_up = inside(wrow_r[1, g], has_up)
                beyond_rows = [
                    jnp.where(even_row, a, b) for a, b in zip(tiles(from_up), tiles(from_down))
                ]
            own = tiles(w_v[m])
            beyond = [row_roll(t, -2 * r) for t in beyond_rows]
            by_row = {
                0: own,
                1: [row_roll(jnp.where(row_first, b, t), -1) for b, t in zip(beyond, own)],
                -1: [row_roll(jnp.where(row_last, b, t), 1) for b, t in zip(beyond, own)],
            }
            weights = {1: tiles(straight[f]), 2: tiles(slanted[f])}
            for dx in (-1, 0, 1):
                t0, t1 = by_row[dx]
                edge = lane_roll(edge_of[dx], -2 * m)
                by_lane = {
                    0: [t0, t1],
                    1: [
                        lane_roll(jnp.where(lane_first, t1, t0), -1),
                        lane_roll(jnp.where(lane_first, edge, t1), -1),
                    ],
                    -1: [
                        lane_roll(jnp.where(lane_last, edge, t0), 1),
                        lane_roll(jnp.where(lane_last, t0, t1), 1),
                    ],
                }
                for dy in (-1, 0, 1):
                    if (dx, dy) == (0, 0):
                        continue
                    for j in range(2):
                        term = weights[abs(dx) + abs(dy)][j] * by_lane[dy][j]
                        old = sums[dx, dy][j]
                        sums[dx, dy][j] = term if old is None else old + term
    scaled = [(0.5 * OFFSET_WEIGHT) * t for t in tiles(gain)]
    coefs = []
    for i, n in enumerate(NEIGHBOURS):
        pair = [scaled[j] * sums[n][j] for j in range(2)]
        coefs.append(jnp.concatenate(pair, axis=1))
        krow_s[i, :, :LANES] = pair[0]
        krow_s[i, :, LANES:] = pair[1]
    kedge_s[...] = pack_edges(coefs)
    k_copies = send_edges(2, kedge_s, kedge_r) + send_rows(2, krow_s, krow_r)

    group_right = lane_id % 16 < 8

    def wide(values, row_ref, edge_ref):
        joined = join_edges(edge_ref, group_right)
        out = []
        for f, value in enumerate(values):
            rows = [
                tiles(value),
                tiles(inside(row_ref[1, f], has_up)),
                tiles(inside(row_ref[0, f], has_down)),
            ]
            out.append(
                [rows[i] + [lane_roll(joined[i], -16 * f)] for i in range(3)]
            )
        return out

    for copy in f_copies:
        copy.wait_recv()
    src0, src1, obs, diag, grad, warm = wide(fields, frow_r, fedge_r)

    def each(fn, *args):
        return [[fn(*(a[i][j] for a in args)) for j in range(3)] for i in range(3)]

    def from_row(a, dx):
        if dx == 0:
            return a
        mask = row_first if dx > 0 else row_last
        return [
            [row_roll(jnp.where(mask, a[(i + dx) % 3][j], a[i][j]), -dx) for j in range(3)]
            for i in range(3)
        ]

    def from_lane(a, dy):
        if dy == 0:
            return a
        mask = lane_first if dy > 0 else lane_last
        return [
            [lane_roll(jnp.where(mask, a[i][(j + dy) % 3], a[i][j]), -dy) for j in range(3)]
            for i in range(3)
        ]

    def plus(*args):
        return each(lambda *t: functools.reduce(lambda a, b: a + b, t), *args)

    def times(a, b):
        return each(lambda s, t: s * t, a, b)

    def axpy(factor, a, b):
        return each(lambda s, t: factor * s + t, a, b)

    def smooth(q):
        return each(
            lambda c, a, b, d, e: REG_GAMMA * (c + REG_SMOOTH * (4.0 * c - (a + b + d + e))),
            q, from_row(q, 1), from_row(q, -1), from_lane(q, 1), from_lane(q, -1),
        )

    def to_surface(q):
        spread = [times(src0, q), times(src1, q)]
        result = list(spread)
        for dx in (-1, 0, 1):
            near_row = [from_row(s, dx) for s in spread]
            for dy in (-1, 0, 1):
                if (dx, dy) == (0, 0):
                    continue
                near = [from_lane(s, dy) for s in near_row]
                weight = stencil[NEIGHBOURS.index((dx, dy))]
                for c in range(2):
                    value = near[c]
                    if dx * dy:
                        value = axpy(CROSS_SHARE * dx * dy, near[1 - c], value)
                    result[c] = plus(result[c], times(weight, value))
        return result

    def to_bed(surface):
        traction = [times(obs, s) for s in surface]
        result = list(traction)
        twisted = {
            s: [axpy(CROSS_SHARE * s, traction[1 - c], traction[c]) for c in range(2)]
            for s in (-1, 1)
        }
        for dy in (-1, 0, 1):
            for c in range(2):
                gathered = None
                for dx in (-1, 0, 1):
                    if (dx, dy) == (0, 0):
                        continue
                    value = twisted[dx * dy][c] if dx * dy else traction[c]
                    weight = stencil[NEIGHBOURS.index((-dx, -dy))]
                    term = from_row(times(weight, value), dx)
                    gathered = term if gathered is None else plus(gathered, term)
                result[c] = plus(result[c], from_lane(gathered, dy))
        return plus(times(src0, result[0]), times(src1, result[1]))

    def hessian(q):
        return plus(to_bed(to_surface(q)), smooth(q))

    for copy in k_copies:
        copy.wait_recv()
    stencil = wide(coefs, krow_r, kedge_r)

    resid = each(lambda a, b: a - b, grad, hessian(warm))
    dir0 = times(diag, resid)
    img0 = hessian(dir0)
    dir1 = times(diag, img0)
    surf1 = to_surface(dir1)
    smooth1 = smooth(dir1)

    def own_sum(fn):
        t = fn(0) + fn(1)
        return jnp.sum(t, axis=0, keepdims=True)

    dots = [
        own_sum(lambda j: resid[0][j] * dir0[0][j]),
        own_sum(lambda j: dir0[0][j] * img0[0][j]),
        own_sum(lambda j: img0[0][j] * dir1[0][j]),
        own_sum(
            lambda j: obs[0][j] * (surf1[0][0][j] * surf1[0][0][j] + surf1[1][0][j] * surf1[1][0][j])
            + dir1[0][j] * smooth1[0][j]
        ),
    ]
    partial = jnp.zeros((ROWS, LANES), F32)
    for q, value in enumerate(dots):
        partial = jnp.where(row_id == q, value, partial)

    def exchange(value, stage_ref, recv_ref, send_sems, recv_sems, me, n, device):
        stage_ref[...] = value
        out = []
        for k in range(1, n):
            copy = pltpu.make_async_remote_copy(
                src_ref=stage_ref, dst_ref=recv_ref.at[me],
                send_sem=send_sems.at[k], recv_sem=recv_sems.at[k],
                device_id=device(k), device_id_type=MESH,
            )
            copy.start()
            out.append(copy)
        recv_ref[me] = value
        sends.extend(out)
        return out

    a_copies = exchange(
        partial, suma_s, suma_r, suma_send, suma_recv, mx, nx, lambda k: at(k, 0)
    )
    img1 = plus(to_bed(surf1), smooth1)
    for copy in a_copies:
        copy.wait_recv()
    partial = suma_r[0]
    for k in range(1, nx):
        partial = partial + suma_r[k]
    b_copies = exchange(
        partial, sumb_s, sumb_r, sumb_send, sumb_recv, my, ny, lambda k: at(0, k)
    )
    for copy in b_copies:
        copy.wait_recv()
    partial = sumb_r[0]
    for k in range(1, ny):
        partial = partial + sumb_r[k]
    full = jnp.sum(partial, axis=1, keepdims=True)
    s0, s1, s2, s3 = (jnp.broadcast_to(full[q : q + 1], (ROWS, LANES)) for q in range(4))

    step0 = s0 / s1
    ratio = (step0 * step0 * s2 - s0) / s0
    grow = 1.0 + ratio
    bend = grow * grow * s1 - 2.0 * grow * step0 * s2 + step0 * step0 * s3
    step1 = ratio * s0 / bend
    for j in range(2):
        cols = slice(j * LANES, (j + 1) * LANES)
        along = grow * dir0[0][j] - step0 * dir1[0][j]
        image = grow * img0[0][j] - step0 * img1[0][j]
        sol_o[:, cols] = warm[0][j] + step0 * dir0[0][j] + step1 * along
        res_o[:, cols] = resid[0][j] - step0 * img0[0][j] - step1 * image

    for copy in sends:
        copy.wait_send()


def solution(mesh):
    nx, ny = mesh.shape["gx"], mesh.shape["gy"]

    def on_device(grad, warm, eta, coef, slide, weight, ice, ground):
        levels, rows, cols = eta.shape
        vmem = lambda *shape: pltpu.VMEM(shape, F32)
        wslots = levels // 2
        dma = lambda *shape: pltpu.SemaphoreType.DMA(shape)
        call = pl.pallas_call(
            functools.partial(kernel, nx=nx, ny=ny, levels=levels),
            out_shape=(
                jax.ShapeDtypeStruct((rows, cols), F32),
                jax.ShapeDtypeStruct((rows, cols), F32),
            ),
            in_specs=[pl.BlockSpec(memory_space=pl.ANY)] * 8,
            out_specs=(
                pl.BlockSpec(memory_space=pltpu.VMEM),
                pl.BlockSpec(memory_space=pltpu.VMEM),
            ),
            scratch_shapes=[
                vmem(rows, cols), vmem(rows, cols), vmem(levels, rows, cols), vmem(rows, cols),
                vmem(2, rows, cols), vmem(rows, cols),
                pltpu.VMEM((rows, cols), jnp.int32), pltpu.VMEM((rows, cols), jnp.int32),
                vmem(2 * levels, rows, cols), vmem(levels, rows, cols), vmem(levels, rows, cols),
                vmem(wslots, rows, cols), vmem(2, wslots, rows, cols),
                vmem(rows, LANES), vmem(6, rows, LANES),
                vmem(6, rows, cols), vmem(2, 6, rows, cols),
                vmem(rows, LANES), vmem(6, rows, LANES),
                vmem(8, rows, cols), vmem(2, 8, rows, cols),
                vmem(rows, LANES), vmem(6, rows, LANES),
                vmem(rows, LANES), vmem(nx, rows, LANES),
                vmem(rows, LANES), vmem(ny, rows, LANES),
                dma(8), dma(3, 2), dma(3, 2), dma(3, 6), dma(3, 6),
                dma(nx), dma(nx), dma(ny), dma(ny),
            ],
            compiler_params=pltpu.CompilerParams(collective_id=0, has_side_effects=True),
        )
        return call(grad, warm, eta, coef, slide, weight, ice, ground)

    return jax.shard_map(
        on_device,
        mesh=mesh,
        in_specs=(
            P("gx", "gy"), P("gx", "gy"), P(None, "gx", "gy"), P("gx", "gy"),
            P(None, "gx", "gy"), P("gx", "gy"), P("gx", "gy"), P("gx", "gy"),
        ),
        out_specs=(P("gx", "gy"), P("gx", "gy")),
        check_vma=False,
    )
```

```python
import functools

import jax
import jax.numpy as jnp
from jax import lax
from jax.experimental import pallas as pl
from jax.experimental.pallas import tpu as pltpu
from jax.sharding import PartitionSpec as P

MESH = pl.DeviceIdType.MESH
F32 = jnp.float32

VERT_COUPLING = 128.0
SINK_RATE = 0.0625
BED_DRAG = 0.5
OFFSET_WEIGHT = 0.0019
CROSS_SHARE = 0.5
REG_GAMMA = 0.02
REG_SMOOTH = 1.0
DIAG_SCALE = 0.003

ROWS = 8
LANES = 128
NEIGHBOURS = [(dx, dy) for dx in (-1, 0, 1) for dy in (-1, 0, 1) if (dx, dy) != (0, 0)]
SIDEWAYS = [(dx, dy) for dx in (-1, 0, 1) for dy in (-1, 1)]


def row_roll(tile, shift):
    return pltpu.roll(tile, shift % ROWS, axis=0)


def lane_roll(tile, shift):
    shift = shift % LANES
    return tile if shift == 0 else pltpu.roll(tile, shift, axis=1)


def kernel(
    grad_h, warm_h, eta_h, coef_h, slide_h, weight_h, ice_h, ground_h,
    sol_o, res_o,
    grad_v, warm_v, eta_v, coef_v, slide_v, weight_v, ice_v, ground_v,
    w_v, wahead_v, wbehind_v, u_v, inva_v, pack_v,
    wrow_s, wrow_r, wedge_s, wedge_r,
    frow_s, frow_r, fedge_s, fedge_r,
    krow_s, krow_r, kedge_s, kedge_r,
    suma_s, suma_r, sumb_s, sumb_r,
    in_sem, row_send, row_recv, edge_send, edge_recv, suma_send, suma_recv, sumb_send, sumb_recv,
    *, nx, ny, levels,
):
    mx = lax.axis_index("gx")
    my = lax.axis_index("gy")

    def at(dx, dy):
        return (lax.rem(mx + (dx + nx), nx), lax.rem(my + (dy + ny), ny))

    pairs = [
        (eta_h, eta_v), (coef_h, coef_v), (ground_h, ground_v), (ice_h, ice_v),
        (slide_h, slide_v), (weight_h, weight_v), (grad_h, grad_v), (warm_h, warm_v),
    ]
    loads = [pltpu.make_async_copy(src, dst, in_sem.at[i]) for i, (src, dst) in enumerate(pairs)]
    for load in loads:
        load.start()

    barrier = pltpu.get_barrier_semaphore()
    peers = [at(dx, dy) for dx, dy in NEIGHBOURS]
    peers += [at(k, 0) for k in range(2, nx - 1)]
    peers += [at(0, k) for k in range(2, ny - 1)]
    for peer in peers:
        pl.semaphore_signal(barrier, inc=1, device_id=peer, device_id_type=MESH)

    row_id = lax.broadcasted_iota(jnp.int32, (ROWS, LANES), 0)
    lane_id = lax.broadcasted_iota(jnp.int32, (ROWS, LANES), 1)
    row_first = row_id == 0
    row_last = row_id == ROWS - 1
    lane_first = lane_id == 0
    lane_last = lane_id == LANES - 1
    low_half = lane_id < LANES // 2

    def tiles(value):
        return [value[:, :LANES], value[:, LANES:]]

    for load in loads[:3]:
        load.wait()
    friction = ground_v[...].astype(F32) * coef_v[...]

    slot = lambda z, f: 2 * (levels - 1 - z) + f

    def pack_row(packed, value, row, m):
        parts = [row_roll(t, m % ROWS - row) for t in tiles(value)]
        if m % ROWS == 0:
            return parts
        return [jnp.where(row_id == m % ROWS, a, b) for a, b in zip(parts, packed)]

    def put(ref, index, pair):
        ref[index + (slice(None), slice(0, LANES))] = pair[0]
        ref[index + (slice(None), slice(LANES, 2 * LANES))] = pair[1]

    def pack_lanes(packed, both, m):
        here = (lane_id == 2 * m) | (lane_id == (2 * m - 1) % LANES)
        return jnp.where(here, lane_roll(both, 2 * m), packed)

    first_rows = last_rows = None
    edge_packed = jnp.zeros((ROWS, LANES), F32)
    w = jnp.ones((ROWS, 2 * LANES), F32)
    eta = eta_v[levels - 1]
    flux = SINK_RATE * eta
    for z in range(levels - 1, -1, -1):
        if z < levels - 1:
            above, eta = eta, eta_v[z]
            inva = 1.0 / ((0.5 * VERT_COUPLING) * (above + eta))
            inva_v[z] = inva
            w = w + flux * inva
            flux = flux + (SINK_RATE * eta) * w
        for f, field in enumerate((w, eta * w)):
            m = slot(z, f)
            w_v[m] = field
            last_rows = pack_row(last_rows, field, ROWS - 1, m)
            first_rows = pack_row(first_rows, field, 0, m)
            if m % ROWS == ROWS - 1:
                put(wrow_s, (0, m // ROWS), last_rows)
                put(wrow_s, (1, m // ROWS), first_rows)
            t0, t1 = tiles(field)
            ahead = lane_roll(t0, -1)
            behind = lane_roll(t1, 1)
            wahead_v[m] = ahead
            wbehind_v[m] = behind
            edge_packed = pack_lanes(edge_packed, jnp.where(low_half, behind, ahead), m)
    wedge_s[...] = edge_packed
    total = flux + BED_DRAG * friction * w
    gain = 1.0 / total

    pl.semaphore_wait(barrier, len(peers))

    sends = []

    def send_rows(stage, src, dst, split=False):
        out = []
        for k, dx in enumerate((1, -1)):
            copy = pltpu.make_async_remote_copy(
                src_ref=src.at[k] if split else src, dst_ref=dst.at[k],
                send_sem=row_send.at[stage, k], recv_sem=row_recv.at[stage, k],
                device_id=at(dx, 0), device_id_type=MESH,
            )
            copy.start()
            out.append(copy)
        sends.extend(out)
        return out

    def send_edges(stage, src, dst):
        out = []
        for k, (dx, dy) in enumerate(SIDEWAYS):
            copy = pltpu.make_async_remote_copy(
                src_ref=src, dst_ref=dst.at[k],
                send_sem=edge_send.at[stage, k], recv_sem=edge_recv.at[stage, k],
                device_id=at(dx, dy), device_id_type=MESH,
            )
            copy.start()
            out.append(copy)
        sends.extend(out)
        return out

    w_copies = send_edges(0, wedge_s, wedge_r) + send_rows(0, wrow_s, wrow_r, split=True)

    for load in loads[3:]:
        load.wait()
    ice = ice_v[...].astype(F32)
    coef = coef_v[...]
    stuck = ice * ground_v[...].astype(F32)
    source_gain = stuck * coef * gain
    fields = [
        source_gain * slide_v[0],
        source_gain * slide_v[1],
        ice * weight_v[...],
        1.0 / (REG_GAMMA * (1.0 + 4.0 * REG_SMOOTH) + DIAG_SCALE * stuck * coef * coef),
        grad_v[...],
        warm_v[...],
    ]

    def pack_edges(values):
        packed = jnp.zeros((ROWS, LANES), F32)
        for f, value in enumerate(values):
            t0, t1 = tiles(value)
            both = lane_roll(jnp.where(low_half, t0, t1), 16 * f)
            group = ((lane_id + 8) % LANES) // 16 == f
            packed = jnp.where(group, both, packed)
        return packed

    for f, value in enumerate(fields):
        frow_s[f] = value
    fedge_s[...] = pack_edges(fields)
    f_copies = send_edges(1, fedge_s, fedge_r) + send_rows(1, frow_s, frow_r)

    u = jnp.ones((ROWS, 2 * LANES), F32)
    flux = SINK_RATE * eta_v[0] + BED_DRAG * friction
    u_v[0] = u
    for z in range(1, levels):
        u = u + flux * inva_v[z - 1]
        flux = flux + (SINK_RATE * eta_v[z]) * u
        u_v[z] = u

    has_up = mx < nx - 1
    has_down = mx > 0
    has_right = my < ny - 1
    has_left = my > 0

    def inside(value, *flags):
        keep = flags[0]
        for flag in flags[1:]:
            keep = keep & flag
        return jnp.where(keep, value, 0.0)

    def join_edges(ref, from_right):
        def got(dx, dy):
            return ref[SIDEWAYS.index((-dx, -dy))]

        own = jnp.where(
            from_right, inside(got(0, 1), has_right), inside(got(0, -1), has_left)
        )
        up = jnp.where(
            from_right, inside(got(1, 1), has_right, has_up), inside(got(1, -1), has_left, has_up)
        )
        down = jnp.where(
            from_right,
            inside(got(-1, 1), has_right, has_down),
            inside(got(-1, -1), has_left, has_down),
        )
        return own, up, down

    row_packs = {}
    straight_edge = jnp.zeros((ROWS, LANES), F32)
    slanted_edge = jnp.zeros((ROWS, LANES), F32)
    sums = {n: [None, None] for n in NEIGHBOURS}

    def add(table, key, j, term):
        table[key][j] = term if table[key][j] is None else table[key][j] + term

    def seam(ahead0, ahead1, behind0, behind1):
        return (
            [jnp.where(lane_last, ahead1, ahead0), ahead1],
            [behind0, jnp.where(lane_first, behind0, behind1)],
        )

    for z in range(levels - 1, -1, -1):
        u = u_v[z]
        eu = eta_v[z] * u
        near_u = near_eu = None
        for other in (z - 1, z + 1):
            if 0 <= other < levels:
                beside = u_v[other]
                near_u = beside if near_u is None else near_u + beside
                beside = eta_v[other] * beside
                near_eu = beside if near_eu is None else near_eu + beside
        straight = (eu + 0.5 * near_eu, u + 0.5 * near_u)
        slanted = (0.5 * eu + (1.0 / 3.0) * near_eu, 0.5 * u + (1.0 / 3.0) * near_u)
        for f in range(2):
            m = slot(z, f)
            for kind, value in enumerate((straight[f], slanted[f])):
                for side, row in enumerate((0, ROWS - 1)):
                    packed = pack_row(row_packs.get((kind, side)), value, row, m)
                    row_packs[kind, side] = packed
                    if m % ROWS == ROWS - 1:
                        put(pack_v, (kind, side, m // ROWS), packed)
            s_pair, d_pair = tiles(straight[f]), tiles(slanted[f])
            straight_edge = pack_lanes(straight_edge, jnp.where(low_half, *s_pair), m)
            slanted_edge = pack_lanes(slanted_edge, jnp.where(low_half, *d_pair), m)
            t0, t1 = tiles(w_v[m])
            plus_pair, minus_pair = seam(wahead_v[m], lane_roll(t1, -1), lane_roll(t0, 1), wbehind_v[m])
            by_lane = {0: [t0, t1], 1: plus_pair, -1: minus_pair}
            for j in range(2):
                for dy in (-1, 1):
                    add(sums, (0, dy), j, s_pair[j] * by_lane[dy][j])
                for dx in (-1, 1):
                    s_rolled = row_roll(s_pair[j], dx)
                    d_rolled = row_roll(d_pair[j], dx)
                    for dy in (-1, 0, 1):
                        rolled = d_rolled if dy else s_rolled
                        add(sums, (dx, dy), j, rolled * by_lane[dy][j])

    for copy in w_copies:
        copy.wait_recv()

    even_lane = lane_id % 2 == 0
    e_own, e_up, e_down = join_edges(wedge_r, ~even_lane)
    e_beyond = jnp.where(row_id < 4, e_up, e_down)
    edge_of = {
        0: e_own,
        1: row_roll(jnp.where(row_first, e_beyond, e_own), -1),
        -1: row_roll(jnp.where(row_last, e_beyond, e_own), 1),
    }
    edge_sums = {}
    for dx in (-1, 0, 1):
        product = (slanted_edge if dx else straight_edge) * edge_of[dx]
        for dy in (-1, 1):
            part = jnp.where(even_lane == (dy < 0), product, 0.0)
            edge_sums[dx, dy] = jnp.sum(part, axis=1, keepdims=True)

    row_sums = {(dx, dy): [None, None] for dx in (-1, 1) for dy in (-1, 0, 1)}
    for side, flag in ((0, has_down), (1, has_up)):
        dx = 2 * side - 1
        for g in range(2 * levels // ROWS):
            t0, t1 = tiles(inside(wrow_r[side, g], flag))
            plus_pair, minus_pair = seam(
                lane_roll(t0, -1), lane_roll(t1, -1), lane_roll(t0, 1), lane_roll(t1, 1)
            )
            by_lane = {0: [t0, t1], 1: plus_pair, -1: minus_pair}
            for dy in (-1, 0, 1):
                weight = tiles(pack_v[1 if dy else 0, side, g])
                for j in range(2):
                    add(row_sums, (dx, dy), j, weight[j] * by_lane[dy][j])

    for (dx, dy), pair in sums.items():
        for j in range(2):
            value = pair[j]
            if dx:
                beyond = jnp.sum(row_sums[dx, dy][j], axis=0, keepdims=True)
                value = jnp.where(row_last if dx > 0 else row_first, beyond, row_roll(value, -dx))
            if dy and j == (dy + 1) // 2:
                value = jnp.where(lane_last if dy > 0 else lane_first, edge_sums[dx, dy], value)
            pair[j] = value
    scaled = [(0.5 * OFFSET_WEIGHT) * t for t in tiles(gain)]
    coefs = []
    for i, n in enumerate(NEIGHBOURS):
        pair = [scaled[j] * sums[n][j] for j in range(2)]
        coefs.append(jnp.concatenate(pair, axis=1))
        krow_s[i, :, :LANES] = pair[0]
        krow_s[i, :, LANES:] = pair[1]
    kedge_s[...] = pack_edges(coefs)
    k_copies = send_edges(2, kedge_s, kedge_r) + send_rows(2, krow_s, krow_r)

    group_right = lane_id % 16 < 8

    def wide(values, row_ref, edge_ref):
        joined = join_edges(edge_ref, group_right)
        out = []
        for f, value in enumerate(values):
            rows = [
                tiles(value),
                tiles(inside(row_ref[1, f], has_up)),
                tiles(inside(row_ref[0, f], has_down)),
            ]
            out.append(
                [rows[i] + [lane_roll(joined[i], -16 * f)] for i in range(3)]
            )
        return out

    for copy in f_copies:
        copy.wait_recv()
    src0, src1, obs, diag, grad, warm = wide(fields, frow_r, fedge_r)

    def each(fn, *args):
        return [[fn(*(a[i][j] for a in args)) for j in range(3)] for i in range(3)]

    def from_row(a, dx):
        if dx == 0:
            return a
        mask = row_first if dx > 0 else row_last
        return [
            [row_roll(jnp.where(mask, a[(i + dx) % 3][j], a[i][j]), -dx) for j in range(3)]
            for i in range(3)
        ]

    def from_lane(a, dy):
        if dy == 0:
            return a
        mask = lane_first if dy > 0 else lane_last
        return [
            [lane_roll(jnp.where(mask, a[i][(j + dy) % 3], a[i][j]), -dy) for j in range(3)]
            for i in range(3)
        ]

    def plus(*args):
        return each(lambda *t: functools.reduce(lambda a, b: a + b, t), *args)

    def times(a, b):
        return each(lambda s, t: s * t, a, b)

    def axpy(factor, a, b):
        return each(lambda s, t: factor * s + t, a, b)

    def smooth(q):
        return each(
            lambda c, a, b, d, e: REG_GAMMA * (c + REG_SMOOTH * (4.0 * c - (a + b + d + e))),
            q, from_row(q, 1), from_row(q, -1), from_lane(q, 1), from_lane(q, -1),
        )

    def to_surface(q):
        spread = [times(src0, q), times(src1, q)]
        result = list(spread)
        for dx in (-1, 0, 1):
            near_row = [from_row(s, dx) for s in spread]
            for dy in (-1, 0, 1):
                if (dx, dy) == (0, 0):
                    continue
                near = [from_lane(s, dy) for s in near_row]
                weight = stencil[NEIGHBOURS.index((dx, dy))]
                for c in range(2):
                    value = near[c]
                    if dx * dy:
                        value = axpy(CROSS_SHARE * dx * dy, near[1 - c], value)
                    result[c] = plus(result[c], times(weight, value))
        return result

    def to_bed(surface):
        traction = [times(obs, s) for s in surface]
        result = list(traction)
        twisted = {
            s: [axpy(CROSS_SHARE * s, traction[1 - c], traction[c]) for c in range(2)]
            for s in (-1, 1)
        }
        for dy in (-1, 0, 1):
            for c in range(2):
                gathered = None
                for dx in (-1, 0, 1):
                    if (dx, dy) == (0, 0):
                        continue
                    value = twisted[dx * dy][c] if dx * dy else traction[c]
                    weight = stencil[NEIGHBOURS.index((-dx, -dy))]
                    term = from_row(times(weight, value), dx)
                    gathered = term if gathered is None else plus(gathered, term)
                result[c] = plus(result[c], from_lane(gathered, dy))
        return plus(times(src0, result[0]), times(src1, result[1]))

    def hessian(q):
        return plus(to_bed(to_surface(q)), smooth(q))

    for copy in k_copies:
        copy.wait_recv()
    stencil = wide(coefs, krow_r, kedge_r)

    resid = each(lambda a, b: a - b, grad, hessian(warm))
    dir0 = times(diag, resid)
    img0 = hessian(dir0)
    dir1 = times(diag, img0)
    surf1 = to_surface(dir1)
    smooth1 = smooth(dir1)

    def own_sum(fn):
        t = fn(0) + fn(1)
        return jnp.sum(t, axis=0, keepdims=True)

    dots = [
        own_sum(lambda j: resid[0][j] * dir0[0][j]),
        own_sum(lambda j: dir0[0][j] * img0[0][j]),
        own_sum(lambda j: img0[0][j] * dir1[0][j]),
        own_sum(
            lambda j: obs[0][j] * (surf1[0][0][j] * surf1[0][0][j] + surf1[1][0][j] * surf1[1][0][j])
            + dir1[0][j] * smooth1[0][j]
        ),
    ]
    partial = jnp.zeros((ROWS, LANES), F32)
    for q, value in enumerate(dots):
        partial = jnp.where(row_id == q, value, partial)

    def exchange(value, stage_ref, recv_ref, send_sems, recv_sems, me, n, device):
        stage_ref[...] = value
        out = []
        for k in range(1, n):
            copy = pltpu.make_async_remote_copy(
                src_ref=stage_ref, dst_ref=recv_ref.at[me],
                send_sem=send_sems.at[k], recv_sem=recv_sems.at[k],
                device_id=device(k), device_id_type=MESH,
            )
            copy.start()
            out.append(copy)
        recv_ref[me] = value
        sends.extend(out)
        return out

    a_copies = exchange(
        partial, suma_s, suma_r, suma_send, suma_recv, mx, nx, lambda k: at(k, 0)
    )
    img1 = plus(to_bed(surf1), smooth1)
    for copy in a_copies:
        copy.wait_recv()
    partial = suma_r[0]
    for k in range(1, nx):
        partial = partial + suma_r[k]
    b_copies = exchange(
        partial, sumb_s, sumb_r, sumb_send, sumb_recv, my, ny, lambda k: at(0, k)
    )
    for copy in b_copies:
        copy.wait_recv()
    partial = sumb_r[0]
    for k in range(1, ny):
        partial = partial + sumb_r[k]
    full = jnp.sum(partial, axis=1, keepdims=True)
    s0, s1, s2, s3 = (jnp.broadcast_to(full[q : q + 1], (ROWS, LANES)) for q in range(4))

    step0 = s0 / s1
    ratio = (step0 * step0 * s2 - s0) / s0
    grow = 1.0 + ratio
    bend = grow * grow * s1 - 2.0 * grow * step0 * s2 + step0 * step0 * s3
    step1 = ratio * s0 / bend
    for j in range(2):
        cols = slice(j * LANES, (j + 1) * LANES)
        along = grow * dir0[0][j] - step0 * dir1[0][j]
        image = grow * img0[0][j] - step0 * img1[0][j]
        sol_o[:, cols] = warm[0][j] + step0 * dir0[0][j] + step1 * along
        res_o[:, cols] = resid[0][j] - step0 * img0[0][j] - step1 * image

    for copy in sends:
        copy.wait_send()


def solution(mesh):
    nx, ny = mesh.shape["gx"], mesh.shape["gy"]

    def on_device(grad, warm, eta, coef, slide, weight, ice, ground):
        levels, rows, cols = eta.shape
        vmem = lambda *shape: pltpu.VMEM(shape, F32)
        wtiles = 2 * levels // ROWS
        dma = lambda *shape: pltpu.SemaphoreType.DMA(shape)
        call = pl.pallas_call(
            functools.partial(kernel, nx=nx, ny=ny, levels=levels),
            out_shape=(
                jax.ShapeDtypeStruct((rows, cols), F32),
                jax.ShapeDtypeStruct((rows, cols), F32),
            ),
            in_specs=[pl.BlockSpec(memory_space=pl.ANY)] * 8,
            out_specs=(
                pl.BlockSpec(memory_space=pltpu.VMEM),
                pl.BlockSpec(memory_space=pltpu.VMEM),
            ),
            scratch_shapes=[
                vmem(rows, cols), vmem(rows, cols), vmem(levels, rows, cols), vmem(rows, cols),
                vmem(2, rows, cols), vmem(rows, cols),
                pltpu.VMEM((rows, cols), jnp.int32), pltpu.VMEM((rows, cols), jnp.int32),
                vmem(2 * levels, rows, cols), vmem(2 * levels, rows, LANES), vmem(2 * levels, rows, LANES),
                vmem(levels, rows, cols), vmem(levels, rows, cols), vmem(2, 2, wtiles, rows, cols),
                vmem(2, wtiles, rows, cols), vmem(2, wtiles, rows, cols),
                vmem(rows, LANES), vmem(6, rows, LANES),
                vmem(6, rows, cols), vmem(2, 6, rows, cols),
                vmem(rows, LANES), vmem(6, rows, LANES),
                vmem(8, rows, cols), vmem(2, 8, rows, cols),
                vmem(rows, LANES), vmem(6, rows, LANES),
                vmem(rows, LANES), vmem(nx, rows, LANES),
                vmem(rows, LANES), vmem(ny, rows, LANES),
                dma(8), dma(3, 2), dma(3, 2), dma(3, 6), dma(3, 6),
                dma(nx), dma(nx), dma(ny), dma(ny),
            ],
            compiler_params=pltpu.CompilerParams(collective_id=0, has_side_effects=True),
        )
        return call(grad, warm, eta, coef, slide, weight, ice, ground)

    return jax.shard_map(
        on_device,
        mesh=mesh,
        in_specs=(
            P("gx", "gy"), P("gx", "gy"), P(None, "gx", "gy"), P("gx", "gy"),
            P(None, "gx", "gy"), P("gx", "gy"), P("gx", "gy"), P("gx", "gy"),
        ),
        out_specs=(P("gx", "gy"), P("gx", "gy")),
        check_vma=False,
    )
```

```python
import functools

import jax
import jax.numpy as jnp
from jax import lax
from jax.experimental import pallas as pl
from jax.experimental.pallas import tpu as pltpu
from jax.sharding import PartitionSpec as P

MESH = pl.DeviceIdType.MESH
F32 = jnp.float32

VERT_COUPLING = 128.0
SINK_RATE = 0.0625
BED_DRAG = 0.5
OFFSET_WEIGHT = 0.0019
CROSS_SHARE = 0.5
REG_GAMMA = 0.02
REG_SMOOTH = 1.0
DIAG_SCALE = 0.003

ROWS = 8
LANES = 128
NEIGHBOURS = [(dx, dy) for dx in (-1, 0, 1) for dy in (-1, 0, 1) if (dx, dy) != (0, 0)]
CORNERS_FIRST = sorted(NEIGHBOURS, key=lambda n: -abs(n[0]) - abs(n[1]))
SIDEWAYS = [(dx, dy) for dx in (-1, 0, 1) for dy in (-1, 1)]


def row_roll(tile, shift):
    return pltpu.roll(tile, shift % ROWS, axis=0)


def lane_roll(tile, shift):
    shift = shift % LANES
    return tile if shift == 0 else pltpu.roll(tile, shift, axis=1)


def kernel(
    grad_h, warm_h, eta_h, coef_h, slide_h, weight_h, ice_h, ground_h,
    sol_o, res_o, step_o, along_o, image_o,
    grad_v, warm_v, eta_v, coef_v, slide_v, weight_v, ice_v, ground_v,
    w_v, wahead_v, wbehind_v, u_v, inva_v, pack_v,
    wrow_s, wrow_r, wedge_s, wedge_r,
    frow_s, frow_r, fedge_s, fedge_r,
    krow_s, krow_r, kedge_s, kedge_r,
    suma_s, suma_r, sumb_s, sumb_r,
    in_sem, row_send, row_recv, edge_send, edge_recv, known_sem, suma_send, suma_recv, sumb_send, sumb_recv,
    *, nx, ny, levels,
):
    mx = lax.axis_index("gx")
    my = lax.axis_index("gy")

    def at(dx, dy):
        return (mx + dx, my + dy)

    def exists(dx, dy):
        tests = []
        if dx:
            tests.append(mx < nx - dx if dx > 0 else mx >= -dx)
        if dy:
            tests.append(my < ny - dy if dy > 0 else my >= -dy)
        return functools.reduce(lambda a, b: a & b, tests)

    def when(flag, *actions):
        @pl.when(flag)
        def _():
            for action in actions:
                action()

    def signal(sem, peer):
        pl.semaphore_signal(sem, inc=1, device_id=peer, device_id_type=MESH)

    barrier = pltpu.get_barrier_semaphore()
    for n in CORNERS_FIRST:
        when(exists(*n), functools.partial(signal, barrier, at(*n)))

    pairs = [
        (eta_h, eta_v), (coef_h, coef_v), (ground_h, ground_v), (ice_h, ice_v),
        (slide_h, slide_v), (weight_h, weight_v), (grad_h, grad_v), (warm_h, warm_v),
    ]
    loads = [pltpu.make_async_copy(src, dst, in_sem.at[i]) for i, (src, dst) in enumerate(pairs)]
    for load in loads:
        load.start()

    row_id = lax.broadcasted_iota(jnp.int32, (ROWS, LANES), 0)
    lane_id = lax.broadcasted_iota(jnp.int32, (ROWS, LANES), 1)
    row_first = row_id == 0
    row_last = row_id == ROWS - 1
    lane_first = lane_id == 0
    lane_last = lane_id == LANES - 1
    low_half = lane_id < LANES // 2

    def tiles(value):
        return [value[:, :LANES], value[:, LANES:]]

    for load in loads[:3]:
        load.wait()
    friction = ground_v[...].astype(F32) * coef_v[...]

    slot = lambda z, f: 2 * (levels - 1 - z) + f

    def pack_row(packed, value, row, m):
        parts = [row_roll(t, m % ROWS - row) for t in tiles(value)]
        if m % ROWS == 0:
            return parts
        return [jnp.where(row_id == m % ROWS, a, b) for a, b in zip(parts, packed)]

    def put(ref, index, pair):
        ref[index + (slice(None), slice(0, LANES))] = pair[0]
        ref[index + (slice(None), slice(LANES, 2 * LANES))] = pair[1]

    def pack_lanes(packed, both, m):
        here = (lane_id == 2 * m) | (lane_id == (2 * m - 1) % LANES)
        return jnp.where(here, lane_roll(both, 2 * m), packed)

    first_rows = last_rows = None
    edge_packed = jnp.zeros((ROWS, LANES), F32)
    w = jnp.ones((ROWS, 2 * LANES), F32)
    eta = eta_v[levels - 1]
    flux = SINK_RATE * eta
    for z in range(levels - 1, -1, -1):
        if z < levels - 1:
            above, eta = eta, eta_v[z]
            inva = 1.0 / ((0.5 * VERT_COUPLING) * (above + eta))
            inva_v[z] = inva
            w = w + flux * inva
            flux = flux + (SINK_RATE * eta) * w
        for f, field in enumerate((w, eta * w)):
            m = slot(z, f)
            w_v[m] = field
            last_rows = pack_row(last_rows, field, ROWS - 1, m)
            first_rows = pack_row(first_rows, field, 0, m)
            if m % ROWS == ROWS - 1:
                put(wrow_s, (0, m // ROWS), last_rows)
                put(wrow_s, (1, m // ROWS), first_rows)
            t0, t1 = tiles(field)
            ahead = lane_roll(t0, -1)
            behind = lane_roll(t1, 1)
            wahead_v[m] = ahead
            wbehind_v[m] = behind
            edge_packed = pack_lanes(edge_packed, jnp.where(low_half, behind, ahead), m)
    wedge_s[...] = edge_packed
    total = flux + BED_DRAG * friction * w
    gain = 1.0 / total

    def count(*offsets):
        return 1 + sum(jnp.where(exists(*n), 1, 0) for n in offsets)

    pl.semaphore_wait(barrier, count((1, 0), (-1, 0)) * count((0, 1), (0, -1)) - 1)

    ends = []

    def send(*copies):
        for (dx, dy), copy in copies:
            when(exists(dx, dy), copy.start)
            ends.append((exists(dx, dy), copy))
        return copies

    def arrive(copies):
        for (dx, dy), copy in copies:
            when(exists(-dx, -dy), copy.wait_recv)

    def exchange_edges(stage, edge, edge_in, row_of, rows_in):
        out = []
        for k, n in enumerate(SIDEWAYS):
            out.append((n, pltpu.make_async_remote_copy(
                src_ref=edge, dst_ref=edge_in.at[k],
                send_sem=edge_send.at[stage, k], recv_sem=edge_recv.at[stage, k],
                device_id=at(*n), device_id_type=MESH,
            )))
        for k, dx in enumerate((1, -1)):
            out.append(((dx, 0), pltpu.make_async_remote_copy(
                src_ref=row_of(k), dst_ref=rows_in.at[k],
                send_sem=row_send.at[stage, k], recv_sem=row_recv.at[stage, k],
                device_id=at(dx, 0), device_id_type=MESH,
            )))
        return send(*out)

    w_copies = exchange_edges(0, wedge_s, wedge_r, lambda k: wrow_s.at[k], wrow_r)

    for load in loads[3:]:
        load.wait()
    ice = ice_v[...].astype(F32)
    coef = coef_v[...]
    stuck = ice * ground_v[...].astype(F32)
    source_gain = stuck * coef * gain
    fields = [
        source_gain * slide_v[0],
        source_gain * slide_v[1],
        ice * weight_v[...],
        1.0 / (REG_GAMMA * (1.0 + 4.0 * REG_SMOOTH) + DIAG_SCALE * stuck * coef * coef),
        grad_v[...],
        warm_v[...],
    ]

    def pack_edges(values):
        packed = jnp.zeros((ROWS, LANES), F32)
        for f, value in enumerate(values):
            t0, t1 = tiles(value)
            both = lane_roll(jnp.where(low_half, t0, t1), 16 * f)
            group = ((lane_id + 8) % LANES) // 16 == f
            packed = jnp.where(group, both, packed)
        return packed

    for f, value in enumerate(fields):
        frow_s[f] = value
    fedge_s[...] = pack_edges(fields)
    f_copies = exchange_edges(1, fedge_s, fedge_r, lambda k: frow_s, frow_r)

    u = jnp.ones((ROWS, 2 * LANES), F32)
    flux = SINK_RATE * eta_v[0] + BED_DRAG * friction
    u_v[0] = u
    for z in range(1, levels):
        u = u + flux * inva_v[z - 1]
        flux = flux + (SINK_RATE * eta_v[z]) * u
        u_v[z] = u

    has_up, has_down = exists(1, 0), exists(-1, 0)
    has_right, has_left = exists(0, 1), exists(0, -1)

    def inside(value, *flags):
        keep = flags[0]
        for flag in flags[1:]:
            keep = keep & flag
        return jnp.where(keep, value, 0.0)

    def join_edges(ref, from_right):
        def got(dx, dy):
            return ref[SIDEWAYS.index((-dx, -dy))]

        own = jnp.where(
            from_right, inside(got(0, 1), has_right), inside(got(0, -1), has_left)
        )
        up = jnp.where(
            from_right, inside(got(1, 1), has_right, has_up), inside(got(1, -1), has_left, has_up)
        )
        down = jnp.where(
            from_right,
            inside(got(-1, 1), has_right, has_down),
            inside(got(-1, -1), has_left, has_down),
        )
        return own, up, down

    row_packs = {}
    straight_edge = jnp.zeros((ROWS, LANES), F32)
    slanted_edge = jnp.zeros((ROWS, LANES), F32)
    sums = {n: [None, None] for n in NEIGHBOURS}

    def add(table, key, j, term):
        table[key][j] = term if table[key][j] is None else table[key][j] + term

    def seam(ahead0, ahead1, behind0, behind1):
        return (
            [jnp.where(lane_last, ahead1, ahead0), ahead1],
            [behind0, jnp.where(lane_first, behind0, behind1)],
        )

    for z in range(levels - 1, -1, -1):
        u = u_v[z]
        eu = eta_v[z] * u
        near_u = near_eu = None
        for other in (z - 1, z + 1):
            if 0 <= other < levels:
                beside = u_v[other]
                near_u = beside if near_u is None else near_u + beside
                beside = eta_v[other] * beside
                near_eu = beside if near_eu is None else near_eu + beside
        straight = (eu + 0.5 * near_eu, u + 0.5 * near_u)
        slanted = (0.5 * eu + (1.0 / 3.0) * near_eu, 0.5 * u + (1.0 / 3.0) * near_u)
        for f in range(2):
            m = slot(z, f)
            for kind, value in enumerate((straight[f], slanted[f])):
                for side, row in enumerate((0, ROWS - 1)):
                    packed = pack_row(row_packs.get((kind, side)), value, row, m)
                    row_packs[kind, side] = packed
                    if m % ROWS == ROWS - 1:
                        put(pack_v, (kind, side, m // ROWS), packed)
            s_pair, d_pair = tiles(straight[f]), tiles(slanted[f])
            straight_edge = pack_lanes(straight_edge, jnp.where(low_half, *s_pair), m)
            slanted_edge = pack_lanes(slanted_edge, jnp.where(low_half, *d_pair), m)
            t0, t1 = tiles(w_v[m])
            plus_pair, minus_pair = seam(wahead_v[m], lane_roll(t1, -1), lane_roll(t0, 1), wbehind_v[m])
            by_lane = {0: [t0, t1], 1: plus_pair, -1: minus_pair}
            for j in range(2):
                for dy in (-1, 1):
                    add(sums, (0, dy), j, s_pair[j] * by_lane[dy][j])
                for dx in (-1, 1):
                    s_rolled = row_roll(s_pair[j], dx)
                    d_rolled = row_roll(d_pair[j], dx)
                    for dy in (-1, 0, 1):
                        rolled = d_rolled if dy else s_rolled
                        add(sums, (dx, dy), j, rolled * by_lane[dy][j])

    arrive(w_copies)

    def greet(round, reach):
        for k, n in enumerate(((reach, 0), (-reach, 0), (0, reach), (0, -reach))):
            if abs(n[0]) < nx and abs(n[1]) < ny:
                when(exists(*n), functools.partial(signal, known_sem.at[round, k], at(*n)))

    def greeted(round, reach):
        for k, n in enumerate(((-reach, 0), (reach, 0), (0, -reach), (0, reach))):
            if abs(n[0]) < nx and abs(n[1]) < ny:
                when(exists(*n), functools.partial(pl.semaphore_wait, known_sem.at[round, k], 1))

    greet(0, 2)

    even_lane = lane_id % 2 == 0
    e_own, e_up, e_down = join_edges(wedge_r, ~even_lane)
    e_beyond = jnp.where(row_id < 4, e_up, e_down)
    edge_of = {
        0: e_own,
        1: row_roll(jnp.where(row_first, e_beyond, e_own), -1),
        -1: row_roll(jnp.where(row_last, e_beyond, e_own), 1),
    }
    edge_sums = {}
    for dx in (-1, 0, 1):
        product = (slanted_edge if dx else straight_edge) * edge_of[dx]
        for dy in (-1, 1):
            part = jnp.where(even_lane == (dy < 0), product, 0.0)
            edge_sums[dx, dy] = jnp.sum(part, axis=1, keepdims=True)

    row_sums = {(dx, dy): [None, None] for dx in (-1, 1) for dy in (-1, 0, 1)}
    for side, flag in ((0, has_down), (1, has_up)):
        dx = 2 * side - 1
        for g in range(2 * levels // ROWS):
            t0, t1 = tiles(inside(wrow_r[side, g], flag))
            plus_pair, minus_pair = seam(
                lane_roll(t0, -1), lane_roll(t1, -1), lane_roll(t0, 1), lane_roll(t1, 1)
            )
            by_lane = {0: [t0, t1], 1: plus_pair, -1: minus_pair}
            for dy in (-1, 0, 1):
                weight = tiles(pack_v[1 if dy else 0, side, g])
                for j in range(2):
                    add(row_sums, (dx, dy), j, weight[j] * by_lane[dy][j])

    for (dx, dy), pair in sums.items():
        for j in range(2):
            value = pair[j]
            if dx:
                beyond = jnp.sum(row_sums[dx, dy][j], axis=0, keepdims=True)
                value = jnp.where(row_last if dx > 0 else row_first, beyond, row_roll(value, -dx))
            if dy and j == (dy + 1) // 2:
                value = jnp.where(lane_last if dy > 0 else lane_first, edge_sums[dx, dy], value)
            pair[j] = value
    scaled = [(0.5 * OFFSET_WEIGHT) * t for t in tiles(gain)]
    coefs = []
    for i, n in enumerate(NEIGHBOURS):
        pair = [scaled[j] * sums[n][j] for j in range(2)]
        coefs.append(jnp.concatenate(pair, axis=1))
        krow_s[i, :, :LANES] = pair[0]
        krow_s[i, :, LANES:] = pair[1]
    kedge_s[...] = pack_edges(coefs)
    k_copies = exchange_edges(2, kedge_s, kedge_r, lambda k: krow_s, krow_r)

    group_right = lane_id % 16 < 8

    def wide(values, row_ref, edge_ref):
        joined = join_edges(edge_ref, group_right)
        out = []
        for f, value in enumerate(values):
            rows = [
                tiles(value),
                tiles(inside(row_ref[1, f], has_up)),
                tiles(inside(row_ref[0, f], has_down)),
            ]
            out.append(
                [rows[i] + [lane_roll(joined[i], -16 * f)] for i in range(3)]
            )
        return out

    arrive(f_copies)
    src0, src1, obs, diag, grad, warm = wide(fields, frow_r, fedge_r)

    def each(fn, *args):
        return [[fn(*(a[i][j] for a in args)) for j in range(3)] for i in range(3)]

    def from_row(a, dx):
        if dx == 0:
            return a
        mask = row_first if dx > 0 else row_last
        return [
            [row_roll(jnp.where(mask, a[(i + dx) % 3][j], a[i][j]), -dx) for j in range(3)]
            for i in range(3)
        ]

    def from_lane(a, dy):
        if dy == 0:
            return a
        mask = lane_first if dy > 0 else lane_last
        return [
            [lane_roll(jnp.where(mask, a[i][(j + dy) % 3], a[i][j]), -dy) for j in range(3)]
            for i in range(3)
        ]

    def plus(*args):
        return each(lambda *t: functools.reduce(lambda a, b: a + b, t), *args)

    def times(a, b):
        return each(lambda s, t: s * t, a, b)

    def axpy(factor, a, b):
        return each(lambda s, t: factor * s + t, a, b)

    def smooth(q):
        return each(
            lambda c, a, b, d, e: REG_GAMMA * (c + REG_SMOOTH * (4.0 * c - (a + b + d + e))),
            q, from_row(q, 1), from_row(q, -1), from_lane(q, 1), from_lane(q, -1),
        )

    def to_surface(q):
        spread = [times(src0, q), times(src1, q)]
        result = list(spread)
        for dx in (-1, 0, 1):
            near_row = [from_row(s, dx) for s in spread]
            for dy in (-1, 0, 1):
                if (dx, dy) == (0, 0):
                    continue
                near = [from_lane(s, dy) for s in near_row]
                weight = stencil[NEIGHBOURS.index((dx, dy))]
                for c in range(2):
                    value = near[c]
                    if dx * dy:
                        value = axpy(CROSS_SHARE * dx * dy, near[1 - c], value)
                    result[c] = plus(result[c], times(weight, value))
        return result

    def to_bed(surface):
        traction = [times(obs, s) for s in surface]
        result = list(traction)
        twisted = {
            s: [axpy(CROSS_SHARE * s, traction[1 - c], traction[c]) for c in range(2)]
            for s in (-1, 1)
        }
        for dy in (-1, 0, 1):
            for c in range(2):
                gathered = None
                for dx in (-1, 0, 1):
                    if (dx, dy) == (0, 0):
                        continue
                    value = twisted[dx * dy][c] if dx * dy else traction[c]
                    weight = stencil[NEIGHBOURS.index((-dx, -dy))]
                    term = from_row(times(weight, value), dx)
                    gathered = term if gathered is None else plus(gathered, term)
                result[c] = plus(result[c], from_lane(gathered, dy))
        return plus(times(src0, result[0]), times(src1, result[1]))

    def hessian(q):
        return plus(to_bed(to_surface(q)), smooth(q))

    greeted(0, 2)
    greet(1, 4)
    greeted(1, 4)
    greet(2, 8)
    arrive(k_copies)
    stencil = wide(coefs, krow_r, kedge_r)

    resid = each(lambda a, b: a - b, grad, hessian(warm))
    dir0 = times(diag, resid)
    img0 = hessian(dir0)
    dir1 = times(diag, img0)
    surf1 = to_surface(dir1)
    smooth1 = smooth(dir1)

    def own_sum(fn):
        t = fn(0) + fn(1)
        return jnp.sum(t, axis=0, keepdims=True)

    dots = [
        own_sum(lambda j: resid[0][j] * dir0[0][j]),
        own_sum(lambda j: dir0[0][j] * img0[0][j]),
        own_sum(lambda j: img0[0][j] * dir1[0][j]),
        own_sum(
            lambda j: obs[0][j] * (surf1[0][0][j] * surf1[0][0][j] + surf1[1][0][j] * surf1[1][0][j])
            + dir1[0][j] * smooth1[0][j]
        ),
    ]
    partial = jnp.zeros((ROWS, LANES), F32)
    for q, value in enumerate(dots):
        partial = jnp.where(row_id == q, value, partial)

    def exchange(value, stage_ref, recv_ref, send_sems, recv_sems, me, n, device):
        stage_ref[...] = value
        out = []
        for k in range(1, n):
            copy = pltpu.make_async_remote_copy(
                src_ref=stage_ref, dst_ref=recv_ref.at[me],
                send_sem=send_sems.at[k], recv_sem=recv_sems.at[k],
                device_id=device(k), device_id_type=MESH,
            )
            copy.start()
            out.append(copy)
            ends.append((None, copy))
        recv_ref[me] = value
        return out

    a_copies = exchange(
        partial, suma_s, suma_r, suma_send, suma_recv, mx, nx, lambda k: (lax.rem(mx + k, nx), my)
    )
    img1 = plus(to_bed(surf1), smooth1)
    for copy in a_copies:
        copy.wait_recv()
    partial = suma_r[0]
    for k in range(1, nx):
        partial = partial + suma_r[k]
    greeted(2, 8)
    b_copies = exchange(
        partial, sumb_s, sumb_r, sumb_send, sumb_recv, my, ny, lambda k: (mx, lax.rem(my + k, ny))
    )
    for copy in b_copies:
        copy.wait_recv()
    partial = sumb_r[0]
    for k in range(1, ny):
        partial = partial + sumb_r[k]
    full = jnp.sum(partial, axis=1, keepdims=True)
    s0, s1, s2, s3 = (jnp.broadcast_to(full[q : q + 1], (ROWS, LANES)) for q in range(4))

    step0 = s0 / s1
    ratio = (step0 * step0 * s2 - s0) / s0
    grow = 1.0 + ratio
    bend = grow * grow * s1 - 2.0 * grow * step0 * s2 + step0 * step0 * s3
    step1 = ratio * s0 / bend
    for j in range(2):
        cols = slice(j * LANES, (j + 1) * LANES)
        sol_o[:, cols] = warm[0][j] + step0 * dir0[0][j]
        res_o[:, cols] = resid[0][j] - step0 * img0[0][j]
        step_o[:, cols] = step1
        along_o[:, cols] = grow * dir0[0][j] - step0 * dir1[0][j]
        image_o[:, cols] = grow * img0[0][j] - step0 * img1[0][j]

    for flag, copy in ends:
        if flag is None:
            copy.wait_send()
        else:
            when(flag, copy.wait_send)


def solution(mesh):
    nx, ny = mesh.shape["gx"], mesh.shape["gy"]

    def on_device(grad, warm, eta, coef, slide, weight, ice, ground):
        levels, rows, cols = eta.shape
        vmem = lambda *shape: pltpu.VMEM(shape, F32)
        wtiles = 2 * levels // ROWS
        dma = lambda *shape: pltpu.SemaphoreType.DMA(shape)
        call = pl.pallas_call(
            functools.partial(kernel, nx=nx, ny=ny, levels=levels),
            out_shape=(pltpu.VMEM((rows, cols), F32),) * 5,
            in_specs=[pl.BlockSpec(memory_space=pl.ANY)] * 8,
            out_specs=(pl.BlockSpec(memory_space=pltpu.VMEM),) * 5,
            scratch_shapes=[
                vmem(rows, cols), vmem(rows, cols), vmem(levels, rows, cols), vmem(rows, cols),
                vmem(2, rows, cols), vmem(rows, cols),
                pltpu.VMEM((rows, cols), jnp.int32), pltpu.VMEM((rows, cols), jnp.int32),
                vmem(2 * levels, rows, cols), vmem(2 * levels, rows, LANES), vmem(2 * levels, rows, LANES),
                vmem(levels, rows, cols), vmem(levels, rows, cols), vmem(2, 2, wtiles, rows, cols),
                vmem(2, wtiles, rows, cols), vmem(2, wtiles, rows, cols),
                vmem(rows, LANES), vmem(6, rows, LANES),
                vmem(6, rows, cols), vmem(2, 6, rows, cols),
                vmem(rows, LANES), vmem(6, rows, LANES),
                vmem(8, rows, cols), vmem(2, 8, rows, cols),
                vmem(rows, LANES), vmem(6, rows, LANES),
                vmem(rows, LANES), vmem(nx, rows, LANES),
                vmem(rows, LANES), vmem(ny, rows, LANES),
                dma(8), dma(3, 2), dma(3, 2), dma(3, 6), dma(3, 6),
                pltpu.SemaphoreType.REGULAR((3, 4)),
                dma(nx), dma(nx), dma(ny), dma(ny),
            ],
            compiler_params=pltpu.CompilerParams(collective_id=0, has_side_effects=True),
        )
        sol, res, step, along, image = call(grad, warm, eta, coef, slide, weight, ice, ground)
        return sol + step * along, res - step * image

    return jax.shard_map(
        on_device,
        mesh=mesh,
        in_specs=(
            P("gx", "gy"), P("gx", "gy"), P(None, "gx", "gy"), P("gx", "gy"),
            P(None, "gx", "gy"), P("gx", "gy"), P("gx", "gy"), P("gx", "gy"),
        ),
        out_specs=(P("gx", "gy"), P("gx", "gy")),
        check_vma=False,
    )
```

```python
import collections
import functools

import jax
import jax.numpy as jnp
from jax import lax
from jax.experimental import pallas as pl
from jax.experimental.pallas import tpu as pltpu
from jax.sharding import PartitionSpec as P

MESH = pl.DeviceIdType.MESH
F32 = jnp.float32

VERT_COUPLING = 128.0
SINK_RATE = 0.0625
BED_DRAG = 0.5
OFFSET_WEIGHT = 0.0019
CROSS_SHARE = 0.5
REG_GAMMA = 0.02
REG_SMOOTH = 1.0
DIAG_SCALE = 0.003

ROWS = 8
LANES = 128
NEIGHBOURS = [(dx, dy) for dx in (-1, 0, 1) for dy in (-1, 0, 1) if (dx, dy) != (0, 0)]
CORNERS_FIRST = sorted(NEIGHBOURS, key=lambda n: -abs(n[0]) - abs(n[1]))
SIDEWAYS = [(dx, dy) for dx in (-1, 0, 1) for dy in (-1, 1)]

Operator = collections.namedtuple("Operator", "source half_obs stencil")


def row_roll(tile, shift):
    return pltpu.roll(tile, shift % ROWS, axis=0)


def lane_roll(tile, shift):
    shift = shift % LANES
    return tile if shift == 0 else pltpu.roll(tile, shift, axis=1)


def kernel(
    grad_h, warm_h, eta_h, coef_h, slide_h, weight_h, ice_h, ground_h,
    sol_o, res_o, step_o, along_o, image_o,
    grad_v, warm_v, eta_v, coef_v, slide_v, weight_v, ice_v, ground_v,
    w_v, wahead_v, wbehind_v, u_v, inva_v, pack_v,
    wrow_s, wrow_r, wedge_s, wedge_r,
    frow_s, frow_r, fedge_s, fedge_r,
    krow_s, krow_r, kedge_s, kedge_r,
    suma_s, suma_r, sumb_s, sumb_r,
    in_sem, row_send, row_recv, edge_send, edge_recv, known_sem, suma_send, suma_recv, sumb_send, sumb_recv,
    *, nx, ny, levels,
):
    mx = lax.axis_index("gx")
    my = lax.axis_index("gy")

    def at(dx, dy):
        return (mx + dx, my + dy)

    def exists(dx, dy):
        tests = []
        if dx:
            tests.append(mx < nx - dx if dx > 0 else mx >= -dx)
        if dy:
            tests.append(my < ny - dy if dy > 0 else my >= -dy)
        return functools.reduce(lambda a, b: a & b, tests)

    def when(flag, *actions):
        @pl.when(flag)
        def _():
            for action in actions:
                action()

    def signal(sem, peer):
        pl.semaphore_signal(sem, inc=1, device_id=peer, device_id_type=MESH)

    barrier = pltpu.get_barrier_semaphore()
    for n in CORNERS_FIRST:
        when(exists(*n), functools.partial(signal, barrier, at(*n)))

    pairs = [
        (eta_h, eta_v), (coef_h, coef_v), (ground_h, ground_v), (ice_h, ice_v),
        (slide_h, slide_v), (weight_h, weight_v), (grad_h, grad_v), (warm_h, warm_v),
    ]
    loads = [pltpu.make_async_copy(src, dst, in_sem.at[i]) for i, (src, dst) in enumerate(pairs)]
    for load in loads:
        load.start()

    row_id = lax.broadcasted_iota(jnp.int32, (ROWS, LANES), 0)
    lane_id = lax.broadcasted_iota(jnp.int32, (ROWS, LANES), 1)
    row_first = row_id == 0
    row_last = row_id == ROWS - 1
    lane_first = lane_id == 0
    lane_last = lane_id == LANES - 1
    low_half = lane_id < LANES // 2

    def tiles(value):
        return [value[:, :LANES], value[:, LANES:]]

    for load in loads[:3]:
        load.wait()
    friction = ground_v[...].astype(F32) * coef_v[...]

    slot = lambda z, f: 2 * (levels - 1 - z) + f

    def pack_row(packed, value, row, m):
        parts = [row_roll(t, m % ROWS - row) for t in tiles(value)]
        if m % ROWS == 0:
            return parts
        return [jnp.where(row_id == m % ROWS, a, b) for a, b in zip(parts, packed)]

    def put(ref, index, pair):
        ref[index + (slice(None), slice(0, LANES))] = pair[0]
        ref[index + (slice(None), slice(LANES, 2 * LANES))] = pair[1]

    def pack_lanes(packed, both, m):
        here = (lane_id == 2 * m) | (lane_id == (2 * m - 1) % LANES)
        return jnp.where(here, lane_roll(both, 2 * m), packed)

    first_rows = last_rows = None
    edge_packed = jnp.zeros((ROWS, LANES), F32)
    w = jnp.ones((ROWS, 2 * LANES), F32)
    eta = eta_v[levels - 1]
    flux = SINK_RATE * eta
    for z in range(levels - 1, -1, -1):
        if z < levels - 1:
            above, eta = eta, eta_v[z]
            inva = 1.0 / ((0.5 * VERT_COUPLING) * (above + eta))
            inva_v[z] = inva
            w = w + flux * inva
            flux = flux + (SINK_RATE * eta) * w
        for f, field in enumerate((w, eta * w)):
            m = slot(z, f)
            w_v[m] = field
            last_rows = pack_row(last_rows, field, ROWS - 1, m)
            first_rows = pack_row(first_rows, field, 0, m)
            if m % ROWS == ROWS - 1:
                put(wrow_s, (0, m // ROWS), last_rows)
                put(wrow_s, (1, m // ROWS), first_rows)
            t0, t1 = tiles(field)
            ahead = lane_roll(t0, -1)
            behind = lane_roll(t1, 1)
            wahead_v[m] = ahead
            wbehind_v[m] = behind
            edge_packed = pack_lanes(edge_packed, jnp.where(low_half, behind, ahead), m)
    wedge_s[...] = edge_packed
    total = flux + BED_DRAG * friction * w
    gain = 1.0 / total

    def count(*offsets):
        return 1 + sum(jnp.where(exists(*n), 1, 0) for n in offsets)

    pl.semaphore_wait(barrier, count((1, 0), (-1, 0)) * count((0, 1), (0, -1)) - 1)

    ends = []

    def send(*copies):
        for (dx, dy), copy in copies:
            when(exists(dx, dy), copy.start)
            ends.append((exists(dx, dy), copy))
        return copies

    def arrive(copies):
        for (dx, dy), copy in copies:
            when(exists(-dx, -dy), copy.wait_recv)

    def exchange_edges(stage, edge, edge_in, row_of, rows_in):
        out = []
        for k, n in enumerate(SIDEWAYS):
            out.append((n, pltpu.make_async_remote_copy(
                src_ref=edge, dst_ref=edge_in.at[k],
                send_sem=edge_send.at[stage, k], recv_sem=edge_recv.at[stage, k],
                device_id=at(*n), device_id_type=MESH,
            )))
        for k, dx in enumerate((1, -1)):
            out.append(((dx, 0), pltpu.make_async_remote_copy(
                src_ref=row_of(k), dst_ref=rows_in.at[k],
                send_sem=row_send.at[stage, k], recv_sem=row_recv.at[stage, k],
                device_id=at(dx, 0), device_id_type=MESH,
            )))
        return send(*out)

    w_copies = exchange_edges(0, wedge_s, wedge_r, lambda k: wrow_s.at[k], wrow_r)

    for load in loads[3:]:
        load.wait()
    ice = ice_v[...].astype(F32)
    coef = coef_v[...]
    stuck = ice * ground_v[...].astype(F32)
    source_gain = stuck * coef * gain
    fields = [
        source_gain * (slide_v[0] + slide_v[1]),
        source_gain * (slide_v[0] - slide_v[1]),
        0.5 * ice * weight_v[...],
        1.0 / (REG_GAMMA * (1.0 + 4.0 * REG_SMOOTH) + DIAG_SCALE * stuck * coef * coef),
        grad_v[...],
        warm_v[...],
    ]

    def pack_edges(values):
        packed = jnp.zeros((ROWS, LANES), F32)
        for f, value in enumerate(values):
            t0, t1 = tiles(value)
            both = lane_roll(jnp.where(low_half, t0, t1), 16 * f)
            group = ((lane_id + 8) % LANES) // 16 == f
            packed = jnp.where(group, both, packed)
        return packed

    for f, value in enumerate(fields):
        frow_s[f] = value
    fedge_s[...] = pack_edges(fields)
    f_copies = exchange_edges(1, fedge_s, fedge_r, lambda k: frow_s, frow_r)

    u = jnp.ones((ROWS, 2 * LANES), F32)
    flux = SINK_RATE * eta_v[0] + BED_DRAG * friction
    u_v[0] = u
    for z in range(1, levels):
        u = u + flux * inva_v[z - 1]
        flux = flux + (SINK_RATE * eta_v[z]) * u
        u_v[z] = u

    has_up, has_down = exists(1, 0), exists(-1, 0)
    has_right, has_left = exists(0, 1), exists(0, -1)

    def inside(value, *flags):
        keep = flags[0]
        for flag in flags[1:]:
            keep = keep & flag
        return jnp.where(keep, value, 0.0)

    def join_edges(ref, from_right):
        def got(dx, dy):
            return ref[SIDEWAYS.index((-dx, -dy))]

        own = jnp.where(
            from_right, inside(got(0, 1), has_right), inside(got(0, -1), has_left)
        )
        up = jnp.where(
            from_right, inside(got(1, 1), has_right, has_up), inside(got(1, -1), has_left, has_up)
        )
        down = jnp.where(
            from_right,
            inside(got(-1, 1), has_right, has_down),
            inside(got(-1, -1), has_left, has_down),
        )
        return own, up, down

    row_packs = {}
    straight_edge = jnp.zeros((ROWS, LANES), F32)
    slanted_edge = jnp.zeros((ROWS, LANES), F32)
    sums = {n: [None, None] for n in NEIGHBOURS}

    def add(table, key, j, term):
        table[key][j] = term if table[key][j] is None else table[key][j] + term

    def seam(ahead0, ahead1, behind0, behind1):
        return (
            [jnp.where(lane_last, ahead1, ahead0), ahead1],
            [behind0, jnp.where(lane_first, behind0, behind1)],
        )

    for z in range(levels - 1, -1, -1):
        u = u_v[z]
        eu = eta_v[z] * u
        near_u = near_eu = None
        for other in (z - 1, z + 1):
            if 0 <= other < levels:
                beside = u_v[other]
                near_u = beside if near_u is None else near_u + beside
                beside = eta_v[other] * beside
                near_eu = beside if near_eu is None else near_eu + beside
        straight = (eu + 0.5 * near_eu, u + 0.5 * near_u)
        slanted = (0.5 * eu + (1.0 / 3.0) * near_eu, 0.5 * u + (1.0 / 3.0) * near_u)
        for f in range(2):
            m = slot(z, f)
            for kind, value in enumerate((straight[f], slanted[f])):
                for side, row in enumerate((0, ROWS - 1)):
                    packed = pack_row(row_packs.get((kind, side)), value, row, m)
                    row_packs[kind, side] = packed
                    if m % ROWS == ROWS - 1:
                        put(pack_v, (kind, side, m // ROWS), packed)
            s_pair, d_pair = tiles(straight[f]), tiles(slanted[f])
            straight_edge = pack_lanes(straight_edge, jnp.where(low_half, *s_pair), m)
            slanted_edge = pack_lanes(slanted_edge, jnp.where(low_half, *d_pair), m)
            t0, t1 = tiles(w_v[m])
            plus_pair, minus_pair = seam(wahead_v[m], lane_roll(t1, -1), lane_roll(t0, 1), wbehind_v[m])
            by_lane = {0: [t0, t1], 1: plus_pair, -1: minus_pair}
            for j in range(2):
                for dy in (-1, 1):
                    add(sums, (0, dy), j, s_pair[j] * by_lane[dy][j])
                for dx in (-1, 1):
                    s_rolled = row_roll(s_pair[j], dx)
                    d_rolled = row_roll(d_pair[j], dx)
                    for dy in (-1, 0, 1):
                        rolled = d_rolled if dy else s_rolled
                        add(sums, (dx, dy), j, rolled * by_lane[dy][j])

    arrive(w_copies)

    def greet(round, reach):
        for k, n in enumerate(((reach, 0), (-reach, 0), (0, reach), (0, -reach))):
            if abs(n[0]) < nx and abs(n[1]) < ny:
                when(exists(*n), functools.partial(signal, known_sem.at[round, k], at(*n)))

    def greeted(round, reach):
        for k, n in enumerate(((-reach, 0), (reach, 0), (0, -reach), (0, reach))):
            if abs(n[0]) < nx and abs(n[1]) < ny:
                when(exists(*n), functools.partial(pl.semaphore_wait, known_sem.at[round, k], 1))

    greet(0, 2)

    even_lane = lane_id % 2 == 0
    e_own, e_up, e_down = join_edges(wedge_r, ~even_lane)
    e_beyond = jnp.where(row_id < 4, e_up, e_down)
    edge_of = {
        0: e_own,
        1: row_roll(jnp.where(row_first, e_beyond, e_own), -1),
        -1: row_roll(jnp.where(row_last, e_beyond, e_own), 1),
    }
    edge_sums = {}
    for dx in (-1, 0, 1):
        product = (slanted_edge if dx else straight_edge) * edge_of[dx]
        for dy in (-1, 1):
            part = jnp.where(even_lane == (dy < 0), product, 0.0)
            edge_sums[dx, dy] = jnp.sum(part, axis=1, keepdims=True)

    row_sums = {(dx, dy): [None, None] for dx in (-1, 1) for dy in (-1, 0, 1)}
    for side, flag in ((0, has_down), (1, has_up)):
        dx = 2 * side - 1
        for g in range(2 * levels // ROWS):
            t0, t1 = tiles(inside(wrow_r[side, g], flag))
            plus_pair, minus_pair = seam(
                lane_roll(t0, -1), lane_roll(t1, -1), lane_roll(t0, 1), lane_roll(t1, 1)
            )
            by_lane = {0: [t0, t1], 1: plus_pair, -1: minus_pair}
            for dy in (-1, 0, 1):
                weight = tiles(pack_v[1 if dy else 0, side, g])
                for j in range(2):
                    add(row_sums, (dx, dy), j, weight[j] * by_lane[dy][j])

    for (dx, dy), pair in sums.items():
        for j in range(2):
            value = pair[j]
            if dx:
                beyond = jnp.sum(row_sums[dx, dy][j], axis=0, keepdims=True)
                value = jnp.where(row_last if dx > 0 else row_first, beyond, row_roll(value, -dx))
            if dy and j == (dy + 1) // 2:
                value = jnp.where(lane_last if dy > 0 else lane_first, edge_sums[dx, dy], value)
            pair[j] = value
    scaled = [(0.5 * OFFSET_WEIGHT) * t for t in tiles(gain)]
    coefs = []
    for i, n in enumerate(NEIGHBOURS):
        pair = [scaled[j] * sums[n][j] for j in range(2)]
        coefs.append(jnp.concatenate(pair, axis=1))
        krow_s[i, :, :LANES] = pair[0]
        krow_s[i, :, LANES:] = pair[1]
    kedge_s[...] = pack_edges(coefs)
    k_copies = exchange_edges(2, kedge_s, kedge_r, lambda k: krow_s, krow_r)

    group_right = lane_id % 16 < 8

    def wide(values, row_ref, edge_ref):
        joined = join_edges(edge_ref, group_right)
        out = []
        for f, value in enumerate(values):
            rows = [
                tiles(value),
                tiles(inside(row_ref[1, f], has_up)),
                tiles(inside(row_ref[0, f], has_down)),
            ]
            out.append(
                [rows[i] + [lane_roll(joined[i], -16 * f)] for i in range(3)]
            )
        return out

    arrive(f_copies)
    *source, half_obs, diag, grad, warm = wide(fields, frow_r, fedge_r)

    def each(fn, *args):
        return [[fn(*(a[i][j] for a in args)) for j in range(3)] for i in range(len(args[0]))]

    def from_row(a, dx):
        if dx == 0:
            return a
        mask = row_first if dx > 0 else row_last
        return [
            [row_roll(jnp.where(mask, a[(i + dx) % len(a)][j], a[i][j]), -dx) for j in range(3)]
            for i in range(len(a))
        ]

    def from_lane(a, dy):
        if dy == 0:
            return a
        mask = lane_first if dy > 0 else lane_last
        return [
            [lane_roll(jnp.where(mask, a[i][(j + dy) % 3], a[i][j]), -dy) for j in range(3)]
            for i in range(len(a))
        ]

    def plus(*args):
        return each(lambda *t: functools.reduce(lambda a, b: a + b, t), *args)

    def times(a, b):
        return each(lambda s, t: s * t, a, b)

    def smooth(q):
        return each(
            lambda c, a, b, d, e: REG_GAMMA * (c + REG_SMOOTH * (4.0 * c - (a + b + d + e))),
            q, from_row(q, 1), from_row(q, -1), from_lane(q, 1), from_lane(q, -1),
        )

    def to_surface(op, q):
        out = []
        for c in range(2):
            spread = times(op.source[c], q)
            result = spread
            for dy in (-1, 0, 1):
                near_lane = from_lane(spread, dy)
                for dx in (-1, 0, 1):
                    if (dx, dy) != (0, 0):
                        result = plus(result, times(op.stencil[c][dx, dy], from_row(near_lane, dx)))
            out.append(result)
        return out

    def to_bed(op, surface):
        out = []
        for c in range(2):
            traction = times(op.half_obs, surface[c])
            result = traction
            for dy in (-1, 0, 1):
                gathered = None
                for dx in (-1, 0, 1):
                    if (dx, dy) != (0, 0):
                        term = from_row(times(op.stencil[c][-dx, -dy], traction), dx)
                        gathered = term if gathered is None else plus(gathered, term)
                result = plus(result, from_lane(gathered, dy))
            out.append(times(op.source[c], result))
        return plus(*out)

    def hessian(op, q):
        return plus(to_bed(op, to_surface(op, q)), smooth(q))

    def operator(source, half_obs, coefs):
        return Operator(source, half_obs, [
            {
                (dx, dy): each(lambda t: (1.0 + sign * CROSS_SHARE * dx * dy) * t, value) if dx * dy else value
                for (dx, dy), value in coefs.items()
            }
            for sign in (1, -1)
        ])

    def narrow(a):
        return [a[0], [jnp.where(row_id < ROWS // 2, a[1][j], a[2][j]) for j in range(3)]]

    greeted(0, 2)
    greet(1, 4)
    greeted(1, 4)
    greet(2, 8)
    arrive(k_copies)
    coefs = dict(zip(NEIGHBOURS, wide(coefs, krow_r, kedge_r)))
    resid = each(lambda a, b: a - b, grad, hessian(operator(source, half_obs, coefs), warm))
    resid, diag = narrow(resid), narrow(diag)
    op = operator([narrow(t) for t in source], narrow(half_obs), {n: narrow(t) for n, t in coefs.items()})
    dir0 = times(diag, resid)
    img0 = hessian(op, dir0)
    dir1 = times(diag, img0)
    surf1 = to_surface(op, dir1)
    smooth1 = smooth(dir1)

    def own_sum(fn):
        t = fn(0) + fn(1)
        return jnp.sum(t, axis=0, keepdims=True)

    dots = [
        own_sum(lambda j: resid[0][j] * dir0[0][j]),
        own_sum(lambda j: dir0[0][j] * img0[0][j]),
        own_sum(lambda j: img0[0][j] * dir1[0][j]),
        own_sum(
            lambda j: half_obs[0][j] * (surf1[0][0][j] * surf1[0][0][j] + surf1[1][0][j] * surf1[1][0][j])
            + dir1[0][j] * smooth1[0][j]
        ),
    ]
    partial = jnp.zeros((ROWS, LANES), F32)
    for q, value in enumerate(dots):
        partial = jnp.where(row_id == q, value, partial)
    partial = jnp.sum(partial, axis=1, keepdims=True)
    partial = jnp.sum(jnp.where(lane_id // 32 == row_id, partial, 0.0), axis=0, keepdims=True)

    def exchange(value, stage_ref, recv_ref, send_sems, recv_sems, me, n, device):
        stage_ref[...] = value
        out = []
        for k in range(1, n):
            copy = pltpu.make_async_remote_copy(
                src_ref=stage_ref, dst_ref=recv_ref.at[me],
                send_sem=send_sems.at[k], recv_sem=recv_sems.at[k],
                device_id=device(k), device_id_type=MESH,
            )
            copy.start()
            out.append(copy)
            ends.append((None, copy))
        recv_ref[me] = value
        return out

    a_copies = exchange(
        partial, suma_s, suma_r, suma_send, suma_recv, mx, nx, lambda k: (lax.rem(mx + k, nx), my)
    )
    img1 = plus(to_bed(op, surf1), smooth1)
    for copy in a_copies:
        copy.wait_recv()
    partial = suma_r[0]
    for k in range(1, nx):
        partial = partial + suma_r[k]
    greeted(2, 8)
    b_copies = exchange(
        partial, sumb_s, sumb_r, sumb_send, sumb_recv, my, ny, lambda k: (mx, lax.rem(my + k, ny))
    )
    for copy in b_copies:
        copy.wait_recv()
    partial = sumb_r[0]
    for k in range(1, ny):
        partial = partial + sumb_r[k]
    s0, s1, s2, s3 = (
        jnp.broadcast_to(partial[:, 32 * q : 32 * q + 1], (ROWS, LANES)) for q in range(4)
    )

    step0 = s0 / s1
    ratio = (step0 * step0 * s2 - s0) / s0
    grow = 1.0 + ratio
    bend = grow * grow * s1 - 2.0 * grow * step0 * s2 + step0 * step0 * s3
    step1 = ratio * s0 / bend
    for j in range(2):
        cols = slice(j * LANES, (j + 1) * LANES)
        sol_o[:, cols] = warm[0][j] + step0 * dir0[0][j]
        res_o[:, cols] = resid[0][j] - step0 * img0[0][j]
        step_o[:, cols] = step1
        along_o[:, cols] = grow * dir0[0][j] - step0 * dir1[0][j]
        image_o[:, cols] = grow * img0[0][j] - step0 * img1[0][j]

    for flag, copy in ends:
        if flag is None:
            copy.wait_send()
        else:
            when(flag, copy.wait_send)


def solution(mesh):
    nx, ny = mesh.shape["gx"], mesh.shape["gy"]

    def on_device(grad, warm, eta, coef, slide, weight, ice, ground):
        levels, rows, cols = eta.shape
        vmem = lambda *shape: pltpu.VMEM(shape, F32)
        wtiles = 2 * levels // ROWS
        dma = lambda *shape: pltpu.SemaphoreType.DMA(shape)
        call = pl.pallas_call(
            functools.partial(kernel, nx=nx, ny=ny, levels=levels),
            out_shape=(pltpu.VMEM((rows, cols), F32),) * 5,
            in_specs=[pl.BlockSpec(memory_space=pl.ANY)] * 8,
            out_specs=(pl.BlockSpec(memory_space=pltpu.VMEM),) * 5,
            scratch_shapes=[
                vmem(rows, cols), vmem(rows, cols), vmem(levels, rows, cols), vmem(rows, cols),
                vmem(2, rows, cols), vmem(rows, cols),
                pltpu.VMEM((rows, cols), jnp.int32), pltpu.VMEM((rows, cols), jnp.int32),
                vmem(2 * levels, rows, cols), vmem(2 * levels, rows, LANES), vmem(2 * levels, rows, LANES),
                vmem(levels, rows, cols), vmem(levels, rows, cols), vmem(2, 2, wtiles, rows, cols),
                vmem(2, wtiles, rows, cols), vmem(2, wtiles, rows, cols),
                vmem(rows, LANES), vmem(6, rows, LANES),
                vmem(6, rows, cols), vmem(2, 6, rows, cols),
                vmem(rows, LANES), vmem(6, rows, LANES),
                vmem(8, rows, cols), vmem(2, 8, rows, cols),
                vmem(rows, LANES), vmem(6, rows, LANES),
                vmem(1, LANES), vmem(nx, 1, LANES),
                vmem(1, LANES), vmem(ny, 1, LANES),
                dma(8), dma(3, 2), dma(3, 2), dma(3, 6), dma(3, 6),
                pltpu.SemaphoreType.REGULAR((3, 4)),
                dma(nx), dma(nx), dma(ny), dma(ny),
            ],
            compiler_params=pltpu.CompilerParams(collective_id=0, has_side_effects=True),
        )
        sol, res, step, along, image = call(grad, warm, eta, coef, slide, weight, ice, ground)
        return sol + step * along, res - step * image

    return jax.shard_map(
        on_device,
        mesh=mesh,
        in_specs=(
            P("gx", "gy"), P("gx", "gy"), P(None, "gx", "gy"), P("gx", "gy"),
            P(None, "gx", "gy"), P("gx", "gy"), P("gx", "gy"), P("gx", "gy"),
        ),
        out_specs=(P("gx", "gy"), P("gx", "gy")),
        check_vma=False,
    )
```

```python
import collections
import functools

import jax
import jax.numpy as jnp
from jax import lax
from jax.experimental import pallas as pl
from jax.experimental.pallas import tpu as pltpu
from jax.sharding import PartitionSpec as P

MESH = pl.DeviceIdType.MESH
F32 = jnp.float32

VERT_COUPLING = 128.0
SINK_RATE = 0.0625
BED_DRAG = 0.5
OFFSET_WEIGHT = 0.0019
CROSS_SHARE = 0.5
REG_GAMMA = 0.02
REG_SMOOTH = 1.0
DIAG_SCALE = 0.003

ROWS = 8
LANES = 128
NEIGHBOURS = [(dx, dy) for dx in (-1, 0, 1) for dy in (-1, 0, 1) if (dx, dy) != (0, 0)]
CORNERS_FIRST = sorted(NEIGHBOURS, key=lambda n: -abs(n[0]) - abs(n[1]))
SIDEWAYS = [(dx, dy) for dx in (-1, 0, 1) for dy in (-1, 1)]

Operator = collections.namedtuple("Operator", "source half_obs stencil")


def row_roll(tile, shift):
    return pltpu.roll(tile, shift % ROWS, axis=0)


def lane_roll(tile, shift):
    shift = shift % LANES
    return tile if shift == 0 else pltpu.roll(tile, shift, axis=1)


def kernel(
    grad_h, warm_h, eta_h, coef_h, slide_h, weight_h, ice_h, ground_h,
    sol_o, res_o, step_o, along_o, image_o,
    grad_v, warm_v, eta_v, coef_v, slide_v, weight_v, ice_v, ground_v,
    w_v, wahead_v, wbehind_v, u_v, inva_v, pack_v,
    first_s, first_r, edge_s, edge_r,
    krow_s, krow_r, kedge_s, kedge_r,
    suma_s, suma_r, sumb_s, sumb_r,
    local_sem, row_recv, edge_recv, known_sem, sum_send, suma_recv, sumb_recv,
    *, nx, ny, levels,
):
    mx = lax.axis_index("gx")
    my = lax.axis_index("gy")

    def at(dx, dy):
        return (mx + dx, my + dy)

    def exists(dx, dy):
        tests = []
        if dx:
            tests.append(mx < nx - dx if dx > 0 else mx >= -dx)
        if dy:
            tests.append(my < ny - dy if dy > 0 else my >= -dy)
        return functools.reduce(lambda a, b: a & b, tests)

    def when(flag, *actions):
        @pl.when(flag)
        def _():
            for action in actions:
                action()

    def signal(sem, peer):
        pl.semaphore_signal(sem, inc=1, device_id=peer, device_id_type=MESH)

    barrier = pltpu.get_barrier_semaphore()
    for n in CORNERS_FIRST:
        when(exists(*n), functools.partial(signal, barrier, at(*n)))

    pairs = [
        (eta_h, eta_v), (coef_h, coef_v), (ground_h, ground_v), (ice_h, ice_v),
        (slide_h, slide_v), (weight_h, weight_v), (grad_h, grad_v), (warm_h, warm_v),
    ]
    loads = [pltpu.make_async_copy(src, dst, local_sem.at[i]) for i, (src, dst) in enumerate(pairs)]
    for load in loads:
        load.start()

    row_id = lax.broadcasted_iota(jnp.int32, (ROWS, LANES), 0)
    lane_id = lax.broadcasted_iota(jnp.int32, (ROWS, LANES), 1)
    row_first = row_id == 0
    row_last = row_id == ROWS - 1
    lane_first = lane_id == 0
    lane_last = lane_id == LANES - 1
    low_half = lane_id < LANES // 2

    def tiles(value):
        return [value[:, :LANES], value[:, LANES:]]

    for load in loads[:3]:
        load.wait()
    friction = ground_v[...].astype(F32) * coef_v[...]

    slot = lambda z, f: 2 * (levels - 1 - z) + f
    wtiles = 2 * levels // ROWS

    def pack_row(packed, value, row, m):
        parts = [row_roll(t, m % ROWS - row) for t in tiles(value)]
        if m % ROWS == 0:
            return parts
        return [jnp.where(row_id == m % ROWS, a, b) for a, b in zip(parts, packed)]

    def put(ref, index, pair):
        ref[index + (slice(None), slice(0, LANES))] = pair[0]
        ref[index + (slice(None), slice(LANES, 2 * LANES))] = pair[1]

    def pack_lanes(packed, both, m):
        here = (lane_id == 2 * m) | (lane_id == (2 * m - 1) % LANES)
        return jnp.where(here, lane_roll(both, 2 * m), packed)

    first_rows = last_rows = None
    edge_packed = jnp.zeros((ROWS, LANES), F32)
    w = jnp.ones((ROWS, 2 * LANES), F32)
    eta = eta_v[levels - 1]
    flux = SINK_RATE * eta
    for z in range(levels - 1, -1, -1):
        if z < levels - 1:
            above, eta = eta, eta_v[z]
            inva = 1.0 / ((0.5 * VERT_COUPLING) * (above + eta))
            inva_v[z] = inva
            w = w + flux * inva
            flux = flux + (SINK_RATE * eta) * w
        for f, field in enumerate((w, eta * w)):
            m = slot(z, f)
            w_v[m] = field
            last_rows = pack_row(last_rows, field, ROWS - 1, m)
            first_rows = pack_row(first_rows, field, 0, m)
            if m % ROWS == ROWS - 1:
                put(first_s, (0, m // ROWS), last_rows)
                put(first_s, (1, m // ROWS), first_rows)
            t0, t1 = tiles(field)
            ahead = lane_roll(t0, -1)
            behind = lane_roll(t1, 1)
            wahead_v[m] = ahead
            wbehind_v[m] = behind
            edge_packed = pack_lanes(edge_packed, jnp.where(low_half, behind, ahead), m)
    edge_s[0] = edge_packed
    total = flux + BED_DRAG * friction * w
    gain = 1.0 / total

    for load in loads[3:]:
        load.wait()
    ice = ice_v[...].astype(F32)
    coef = coef_v[...]
    stuck = ice * ground_v[...].astype(F32)
    source_gain = stuck * coef * gain
    fields = [
        source_gain * (slide_v[0] + slide_v[1]),
        source_gain * (slide_v[0] - slide_v[1]),
        0.5 * ice * weight_v[...],
        1.0 / (REG_GAMMA * (1.0 + 4.0 * REG_SMOOTH) + DIAG_SCALE * stuck * coef * coef),
        grad_v[...],
        warm_v[...],
    ]

    def pack_edges(values):
        packed = jnp.zeros((ROWS, LANES), F32)
        for f, value in enumerate(values):
            t0, t1 = tiles(value)
            both = lane_roll(jnp.where(low_half, t0, t1), 16 * f)
            group = ((lane_id + 8) % LANES) // 16 == f
            packed = jnp.where(group, both, packed)
        return packed

    for f, value in enumerate(fields):
        for k in range(2):
            put(first_s, (k, wtiles + f), tiles(value))
    edge_s[1] = pack_edges(fields)

    def count(*offsets):
        return 1 + sum(jnp.where(exists(*n), 1, 0) for n in offsets)

    pl.semaphore_wait(barrier, count((1, 0), (-1, 0)) * count((0, 1), (0, -1)) - 1)

    def send(*copies):
        for n, copy in copies:
            when(exists(*n), copy.start)
        return copies

    def sent(copies):
        for n, copy in copies:
            when(exists(*n), copy.wait_send)

    def arrive(copies):
        for (dx, dy), copy in copies:
            when(exists(-dx, -dy), copy.wait_recv)

    def exchange_edges(stage, edge, edge_in, row_of, rows_in):
        out = []
        for k, n in enumerate(SIDEWAYS):
            out.append((n, pltpu.make_async_remote_copy(
                src_ref=edge, dst_ref=edge_in.at[k],
                send_sem=local_sem.at[k], recv_sem=edge_recv.at[stage, k],
                device_id=at(*n), device_id_type=MESH,
            )))
        for k, dx in enumerate((1, -1)):
            out.append(((dx, 0), pltpu.make_async_remote_copy(
                src_ref=row_of(k), dst_ref=rows_in.at[k],
                send_sem=local_sem.at[6 + k], recv_sem=row_recv.at[stage, k],
                device_id=at(dx, 0), device_id_type=MESH,
            )))
        return send(*out)

    reaches = (1, 2, 4, 8)

    def around(round):
        reach = reaches[round]
        return [n for n in ((reach, 0), (-reach, 0), (0, reach), (0, -reach)) if abs(n[0]) < nx and abs(n[1]) < ny]

    def greet(round):
        for n in around(round):
            when(exists(*n), functools.partial(signal, known_sem.at[round], at(*n)))

    def greeted(round):
        pl.semaphore_wait(known_sem.at[round], count(*around(round)) - 1)

    w_copies = exchange_edges(0, edge_s, edge_r, lambda k: first_s.at[k], first_r)
    greet(0)


    u = jnp.ones((ROWS, 2 * LANES), F32)
    flux = SINK_RATE * eta_v[0] + BED_DRAG * friction
    u_v[0] = u
    for z in range(1, levels):
        u = u + flux * inva_v[z - 1]
        flux = flux + (SINK_RATE * eta_v[z]) * u
        u_v[z] = u

    has_up, has_down = exists(1, 0), exists(-1, 0)
    has_right, has_left = exists(0, 1), exists(0, -1)

    def inside(value, *flags):
        keep = flags[0]
        for flag in flags[1:]:
            keep = keep & flag
        return jnp.where(keep, value, 0.0)

    def join_edges(ref, part, from_right):
        def got(dx, dy):
            return ref[SIDEWAYS.index((-dx, -dy)), part]

        own = jnp.where(
            from_right, inside(got(0, 1), has_right), inside(got(0, -1), has_left)
        )
        up = jnp.where(
            from_right, inside(got(1, 1), has_right, has_up), inside(got(1, -1), has_left, has_up)
        )
        down = jnp.where(
            from_right,
            inside(got(-1, 1), has_right, has_down),
            inside(got(-1, -1), has_left, has_down),
        )
        return own, up, down

    row_packs = {}
    straight_edge = jnp.zeros((ROWS, LANES), F32)
    slanted_edge = jnp.zeros((ROWS, LANES), F32)
    sums = {n: [None, None] for n in NEIGHBOURS}

    def add(table, key, j, term):
        table[key][j] = term if table[key][j] is None else table[key][j] + term

    def seam(ahead0, ahead1, behind0, behind1):
        return (
            [jnp.where(lane_last, ahead1, ahead0), ahead1],
            [behind0, jnp.where(lane_first, behind0, behind1)],
        )

    for z in range(levels - 1, -1, -1):
        u = u_v[z]
        eu = eta_v[z] * u
        near_u = near_eu = None
        for other in (z - 1, z + 1):
            if 0 <= other < levels:
                beside = u_v[other]
                near_u = beside if near_u is None else near_u + beside
                beside = eta_v[other] * beside
                near_eu = beside if near_eu is None else near_eu + beside
        straight = (eu + 0.5 * near_eu, u + 0.5 * near_u)
        slanted = (0.5 * eu + (1.0 / 3.0) * near_eu, 0.5 * u + (1.0 / 3.0) * near_u)
        for f in range(2):
            m = slot(z, f)
            for kind, value in enumerate((straight[f], slanted[f])):
                for side, row in enumerate((0, ROWS - 1)):
                    packed = pack_row(row_packs.get((kind, side)), value, row, m)
                    row_packs[kind, side] = packed
                    if m % ROWS == ROWS - 1:
                        put(pack_v, (kind, side, m // ROWS), packed)
            s_pair, d_pair = tiles(straight[f]), tiles(slanted[f])
            straight_edge = pack_lanes(straight_edge, jnp.where(low_half, *s_pair), m)
            slanted_edge = pack_lanes(slanted_edge, jnp.where(low_half, *d_pair), m)
            t0, t1 = tiles(w_v[m])
            plus_pair, minus_pair = seam(wahead_v[m], lane_roll(t1, -1), lane_roll(t0, 1), wbehind_v[m])
            by_lane = {0: [t0, t1], 1: plus_pair, -1: minus_pair}
            for j in range(2):
                for dy in (-1, 1):
                    add(sums, (0, dy), j, s_pair[j] * by_lane[dy][j])
                for dx in (-1, 1):
                    s_rolled = row_roll(s_pair[j], dx)
                    d_rolled = row_roll(d_pair[j], dx)
                    for dy in (-1, 0, 1):
                        rolled = d_rolled if dy else s_rolled
                        add(sums, (dx, dy), j, rolled * by_lane[dy][j])

    greeted(0)
    greet(1)
    sent(w_copies)
    arrive(w_copies)
    greeted(1)
    greet(2)

    even_lane = lane_id % 2 == 0
    e_own, e_up, e_down = join_edges(edge_r, 0, ~even_lane)
    e_beyond = jnp.where(row_id < 4, e_up, e_down)
    edge_of = {
        0: e_own,
        1: row_roll(jnp.where(row_first, e_beyond, e_own), -1),
        -1: row_roll(jnp.where(row_last, e_beyond, e_own), 1),
    }
    edge_sums = {}
    for dx in (-1, 0, 1):
        product = (slanted_edge if dx else straight_edge) * edge_of[dx]
        for dy in (-1, 1):
            part = jnp.where(even_lane == (dy < 0), product, 0.0)
            edge_sums[dx, dy] = jnp.sum(part, axis=1, keepdims=True)

    row_sums = {(dx, dy): [None, None] for dx in (-1, 1) for dy in (-1, 0, 1)}
    for side, flag in ((0, has_down), (1, has_up)):
        dx = 2 * side - 1
        for g in range(2 * levels // ROWS):
            t0, t1 = tiles(inside(first_r[side, g], flag))
            plus_pair, minus_pair = seam(
                lane_roll(t0, -1), lane_roll(t1, -1), lane_roll(t0, 1), lane_roll(t1, 1)
            )
            by_lane = {0: [t0, t1], 1: plus_pair, -1: minus_pair}
            for dy in (-1, 0, 1):
                weight = tiles(pack_v[1 if dy else 0, side, g])
                for j in range(2):
                    add(row_sums, (dx, dy), j, weight[j] * by_lane[dy][j])

    for (dx, dy), pair in sums.items():
        for j in range(2):
            value = pair[j]
            if dx:
                beyond = jnp.sum(row_sums[dx, dy][j], axis=0, keepdims=True)
                value = jnp.where(row_last if dx > 0 else row_first, beyond, row_roll(value, -dx))
            if dy and j == (dy + 1) // 2:
                value = jnp.where(lane_last if dy > 0 else lane_first, edge_sums[dx, dy], value)
            pair[j] = value
    scaled = [(0.5 * OFFSET_WEIGHT) * t for t in tiles(gain)]
    coefs = []
    for i, n in enumerate(NEIGHBOURS):
        pair = [scaled[j] * sums[n][j] for j in range(2)]
        coefs.append(jnp.concatenate(pair, axis=1))
        krow_s[i, :, :LANES] = pair[0]
        krow_s[i, :, LANES:] = pair[1]
    kedge_s[0] = pack_edges(coefs)
    k_copies = exchange_edges(1, kedge_s, kedge_r, lambda k: krow_s, krow_r)

    group_right = lane_id % 16 < 8

    def wide(values, row_ref, start, edge_ref, part):
        joined = join_edges(edge_ref, part, group_right)
        out = []
        for f, value in enumerate(values):
            rows = [
                tiles(value),
                tiles(inside(row_ref[1, start + f], has_up)),
                tiles(inside(row_ref[0, start + f], has_down)),
            ]
            out.append(
                [rows[i] + [lane_roll(joined[i], -16 * f)] for i in range(3)]
            )
        return out

    *source, half_obs, diag, grad, warm = wide(fields, first_r, wtiles, edge_r, 1)

    def each(fn, *args):
        return [[fn(*(a[i][j] for a in args)) for j in range(3)] for i in range(len(args[0]))]

    def from_row(a, dx):
        if dx == 0:
            return a
        mask = row_first if dx > 0 else row_last
        return [
            [row_roll(jnp.where(mask, a[(i + dx) % len(a)][j], a[i][j]), -dx) for j in range(3)]
            for i in range(len(a))
        ]

    def from_lane(a, dy):
        if dy == 0:
            return a
        mask = lane_first if dy > 0 else lane_last
        return [
            [lane_roll(jnp.where(mask, a[i][(j + dy) % 3], a[i][j]), -dy) for j in range(3)]
            for i in range(len(a))
        ]

    def plus(*args):
        return each(lambda *t: functools.reduce(lambda a, b: a + b, t), *args)

    def times(a, b):
        return each(lambda s, t: s * t, a, b)

    def smooth(q):
        return each(
            lambda c, a, b, d, e: REG_GAMMA * (c + REG_SMOOTH * (4.0 * c - (a + b + d + e))),
            q, from_row(q, 1), from_row(q, -1), from_lane(q, 1), from_lane(q, -1),
        )

    def to_surface(op, q):
        out = []
        for c in range(2):
            spread = times(op.source[c], q)
            result = spread
            for dy in (-1, 0, 1):
                near_lane = from_lane(spread, dy)
                for dx in (-1, 0, 1):
                    if (dx, dy) != (0, 0):
                        result = plus(result, times(op.stencil[c][dx, dy], from_row(near_lane, dx)))
            out.append(result)
        return out

    def to_bed(op, surface):
        out = []
        for c in range(2):
            traction = times(op.half_obs, surface[c])
            result = traction
            for dy in (-1, 0, 1):
                gathered = None
                for dx in (-1, 0, 1):
                    if (dx, dy) != (0, 0):
                        term = from_row(times(op.stencil[c][-dx, -dy], traction), dx)
                        gathered = term if gathered is None else plus(gathered, term)
                result = plus(result, from_lane(gathered, dy))
            out.append(times(op.source[c], result))
        return plus(*out)

    def hessian(op, q):
        return plus(to_bed(op, to_surface(op, q)), smooth(q))

    def operator(source, half_obs, coefs):
        return Operator(source, half_obs, [
            {
                (dx, dy): each(lambda t: (1.0 + sign * CROSS_SHARE * dx * dy) * t, value) if dx * dy else value
                for (dx, dy), value in coefs.items()
            }
            for sign in (1, -1)
        ])

    def narrow(a):
        return [a[0], [jnp.where(row_id < ROWS // 2, a[1][j], a[2][j]) for j in range(3)]]

    greeted(2)
    greet(3)
    arrive(k_copies)
    coefs = dict(zip(NEIGHBOURS, wide(coefs, krow_r, 0, kedge_r, 0)))
    resid = each(lambda a, b: a - b, grad, hessian(operator(source, half_obs, coefs), warm))
    resid, diag = narrow(resid), narrow(diag)
    op = operator([narrow(t) for t in source], narrow(half_obs), {n: narrow(t) for n, t in coefs.items()})
    dir0 = times(diag, resid)
    img0 = hessian(op, dir0)
    dir1 = times(diag, img0)
    surf1 = to_surface(op, dir1)
    smooth1 = smooth(dir1)

    def own_sum(fn):
        t = fn(0) + fn(1)
        return jnp.sum(t, axis=0, keepdims=True)

    dots = [
        own_sum(lambda j: resid[0][j] * dir0[0][j]),
        own_sum(lambda j: dir0[0][j] * img0[0][j]),
        own_sum(lambda j: img0[0][j] * dir1[0][j]),
        own_sum(
            lambda j: half_obs[0][j] * (surf1[0][0][j] * surf1[0][0][j] + surf1[1][0][j] * surf1[1][0][j])
            + dir1[0][j] * smooth1[0][j]
        ),
    ]
    partial = jnp.zeros((ROWS, LANES), F32)
    for q, value in enumerate(dots):
        partial = jnp.where(row_id == q, value, partial)
    partial = jnp.sum(partial, axis=1, keepdims=True)
    partial = jnp.sum(jnp.where(lane_id // 32 == row_id, partial, 0.0), axis=0, keepdims=True)

    def spread_sums(value, stage_ref, recv_ref, send_sem, recv_sem, me, n, device):
        stage_ref[...] = value
        for k in range(1, n):
            pltpu.make_async_remote_copy(
                src_ref=stage_ref, dst_ref=recv_ref.at[me], send_sem=send_sem, recv_sem=recv_sem,
                device_id=device(k), device_id_type=MESH,
            ).start()
        recv_ref[me] = value

    def all_sent(sem, ref, n):
        whole = ref.at[pl.ds(0, n - 1)]
        pltpu.make_async_copy(whole, whole, sem).wait()

    def gather_sums(ref, sem, n):
        all_sent(sem, ref, n)
        value = ref[0]
        for k in range(1, n):
            value = value + ref[k]
        return value

    spread_sums(partial, suma_s, suma_r, sum_send, suma_recv, mx, nx, lambda k: (lax.rem(mx + k, nx), my))
    img1 = plus(to_bed(op, surf1), smooth1)
    sent(k_copies)
    partial = gather_sums(suma_r, suma_recv, nx)
    greeted(3)
    all_sent(sum_send, suma_r, nx)
    spread_sums(partial, sumb_s, sumb_r, sum_send, sumb_recv, my, ny, lambda k: (mx, lax.rem(my + k, ny)))
    partial = gather_sums(sumb_r, sumb_recv, ny)
    s0, s1, s2, s3 = (
        jnp.broadcast_to(partial[:, 32 * q : 32 * q + 1], (ROWS, LANES)) for q in range(4)
    )

    step0 = s0 / s1
    ratio = (step0 * step0 * s2 - s0) / s0
    grow = 1.0 + ratio
    bend = grow * grow * s1 - 2.0 * grow * step0 * s2 + step0 * step0 * s3
    step1 = ratio * s0 / bend
    for j in range(2):
        cols = slice(j * LANES, (j + 1) * LANES)
        sol_o[:, cols] = warm[0][j] + step0 * dir0[0][j]
        res_o[:, cols] = resid[0][j] - step0 * img0[0][j]
        step_o[:, cols] = step1
        along_o[:, cols] = grow * dir0[0][j] - step0 * dir1[0][j]
        image_o[:, cols] = grow * img0[0][j] - step0 * img1[0][j]

    all_sent(sum_send, sumb_r, ny)


def solution(mesh):
    nx, ny = mesh.shape["gx"], mesh.shape["gy"]

    def on_device(grad, warm, eta, coef, slide, weight, ice, ground):
        levels, rows, cols = eta.shape
        vmem = lambda *shape: pltpu.VMEM(shape, F32)
        wtiles = 2 * levels // ROWS
        dma = lambda *shape: pltpu.SemaphoreType.DMA(shape)
        call = pl.pallas_call(
            functools.partial(kernel, nx=nx, ny=ny, levels=levels),
            out_shape=(pltpu.VMEM((rows, cols), F32),) * 5,
            in_specs=[pl.BlockSpec(memory_space=pl.ANY)] * 8,
            out_specs=(pl.BlockSpec(memory_space=pltpu.VMEM),) * 5,
            scratch_shapes=[
                vmem(rows, cols), vmem(rows, cols), vmem(levels, rows, cols), vmem(rows, cols),
                vmem(2, rows, cols), vmem(rows, cols),
                pltpu.VMEM((rows, cols), jnp.int32), pltpu.VMEM((rows, cols), jnp.int32),
                vmem(2 * levels, rows, cols), vmem(2 * levels, rows, LANES), vmem(2 * levels, rows, LANES),
                vmem(levels, rows, cols), vmem(levels, rows, cols), vmem(2, 2, wtiles, rows, cols),
                vmem(2, wtiles + 6, rows, cols), vmem(2, wtiles + 6, rows, cols),
                vmem(2, rows, LANES), vmem(6, 2, rows, LANES),
                vmem(8, rows, cols), vmem(2, 8, rows, cols),
                vmem(1, rows, LANES), vmem(6, 1, rows, LANES),
                vmem(1, LANES), vmem(nx, 1, LANES),
                vmem(1, LANES), vmem(ny, 1, LANES),
                dma(8), dma(2, 2), dma(2, 6), pltpu.SemaphoreType.REGULAR((4,)), dma(), dma(), dma(),
            ],
            compiler_params=pltpu.CompilerParams(collective_id=0, has_side_effects=True),
        )
        sol, res, step, along, image = call(grad, warm, eta, coef, slide, weight, ice, ground)
        return sol + step * along, res - step * image

    return jax.shard_map(
        on_device,
        mesh=mesh,
        in_specs=(
            P("gx", "gy"), P("gx", "gy"), P(None, "gx", "gy"), P("gx", "gy"),
            P(None, "gx", "gy"), P("gx", "gy"), P("gx", "gy"), P("gx", "gy"),
        ),
        out_specs=(P("gx", "gy"), P("gx", "gy")),
        check_vma=False,
    )
```

```python
import collections
import functools

import jax
import jax.numpy as jnp
from jax import lax
from jax.experimental import pallas as pl
from jax.experimental.pallas import tpu as pltpu
from jax.sharding import PartitionSpec as P

MESH = pl.DeviceIdType.MESH
F32 = jnp.float32

VERT_COUPLING = 128.0
SINK_RATE = 0.0625
BED_DRAG = 0.5
OFFSET_WEIGHT = 0.0019
CROSS_SHARE = 0.5
REG_GAMMA = 0.02
REG_SMOOTH = 1.0
DIAG_SCALE = 0.003

ROWS = 8
LANES = 128
NEIGHBOURS = [(dx, dy) for dx in (-1, 0, 1) for dy in (-1, 0, 1) if (dx, dy) != (0, 0)]
CORNERS_FIRST = sorted(NEIGHBOURS, key=lambda n: -abs(n[0]) - abs(n[1]))
SIDEWAYS = [(dx, dy) for dx in (-1, 0, 1) for dy in (-1, 1)]

Operator = collections.namedtuple("Operator", "source half_obs stencil")


def row_roll(tile, shift):
    return pltpu.roll(tile, shift % ROWS, axis=0)


def lane_roll(tile, shift):
    shift = shift % LANES
    return tile if shift == 0 else pltpu.roll(tile, shift, axis=1)


def kernel(
    grad_h, warm_h, eta_h, coef_h, slide_h, weight_h, ice_h, ground_h,
    sol_o, res_o, step_o, along_o, image_o,
    grad_v, warm_v, eta_v, coef_v, slide_v, weight_v, ice_v, ground_v,
    w_v, wahead_v, wbehind_v, u_v, inva_v, pack_v,
    first_s, first_r, edge_s, edge_r,
    krow_s, krow_r, kedge_s, kedge_r,
    sum_s, sum_r,
    local_sem, row_recv, edge_recv, known_sem, sum_send, sum_recv,
    *, nx, ny, levels,
):
    mx = lax.axis_index("gx")
    my = lax.axis_index("gy")

    def at(dx, dy):
        return (mx + dx, my + dy)

    def exists(dx, dy):
        tests = []
        if dx:
            tests.append(mx < nx - dx if dx > 0 else mx >= -dx)
        if dy:
            tests.append(my < ny - dy if dy > 0 else my >= -dy)
        return functools.reduce(lambda a, b: a & b, tests)

    def when(flag, *actions):
        @pl.when(flag)
        def _():
            for action in actions:
                action()

    def signal(sem, peer):
        pl.semaphore_signal(sem, inc=1, device_id=peer, device_id_type=MESH)

    barrier = pltpu.get_barrier_semaphore()
    for n in CORNERS_FIRST:
        when(exists(*n), functools.partial(signal, barrier, at(*n)))

    pairs = [
        (eta_h, eta_v), (coef_h, coef_v), (ground_h, ground_v), (ice_h, ice_v),
        (slide_h, slide_v), (weight_h, weight_v), (grad_h, grad_v), (warm_h, warm_v),
    ]
    loads = [pltpu.make_async_copy(src, dst, local_sem.at[i]) for i, (src, dst) in enumerate(pairs)]
    for load in loads:
        load.start()

    row_id = lax.broadcasted_iota(jnp.int32, (ROWS, LANES), 0)
    lane_id = lax.broadcasted_iota(jnp.int32, (ROWS, LANES), 1)
    row_first = row_id == 0
    row_last = row_id == ROWS - 1
    lane_first = lane_id == 0
    lane_last = lane_id == LANES - 1
    low_half = lane_id < LANES // 2

    def tiles(value):
        return [value[:, :LANES], value[:, LANES:]]

    for load in loads[:3]:
        load.wait()
    friction = ground_v[...].astype(F32) * coef_v[...]

    slot = lambda z, f: 2 * (levels - 1 - z) + f
    wtiles = 2 * levels // ROWS

    def pack_row(packed, value, row, m):
        parts = [row_roll(t, m % ROWS - row) for t in tiles(value)]
        if m % ROWS == 0:
            return parts
        return [jnp.where(row_id == m % ROWS, a, b) for a, b in zip(parts, packed)]

    def put(ref, index, pair):
        ref[index + (slice(None), slice(0, LANES))] = pair[0]
        ref[index + (slice(None), slice(LANES, 2 * LANES))] = pair[1]

    def pack_lanes(packed, both, m):
        here = (lane_id == 2 * m) | (lane_id == (2 * m - 1) % LANES)
        return jnp.where(here, lane_roll(both, 2 * m), packed)

    first_rows = last_rows = None
    edge_packed = jnp.zeros((ROWS, LANES), F32)
    w = jnp.ones((ROWS, 2 * LANES), F32)
    eta = eta_v[levels - 1]
    flux = SINK_RATE * eta
    for z in range(levels - 1, -1, -1):
        if z < levels - 1:
            above, eta = eta, eta_v[z]
            inva = 1.0 / ((0.5 * VERT_COUPLING) * (above + eta))
            inva_v[z] = inva
            w = w + flux * inva
            flux = flux + (SINK_RATE * eta) * w
        for f, field in enumerate((w, eta * w)):
            m = slot(z, f)
            w_v[m] = field
            last_rows = pack_row(last_rows, field, ROWS - 1, m)
            first_rows = pack_row(first_rows, field, 0, m)
            if m % ROWS == ROWS - 1:
                put(first_s, (0, m // ROWS), last_rows)
                put(first_s, (1, m // ROWS), first_rows)
            t0, t1 = tiles(field)
            ahead = lane_roll(t0, -1)
            behind = lane_roll(t1, 1)
            wahead_v[m] = ahead
            wbehind_v[m] = behind
            edge_packed = pack_lanes(edge_packed, jnp.where(low_half, behind, ahead), m)
    edge_s[0] = edge_packed
    total = flux + BED_DRAG * friction * w
    gain = 1.0 / total

    for load in loads[3:]:
        load.wait()
    ice = ice_v[...].astype(F32)
    coef = coef_v[...]
    stuck = ice * ground_v[...].astype(F32)
    source_gain = stuck * coef * gain
    fields = [
        source_gain * (slide_v[0] + slide_v[1]),
        source_gain * (slide_v[0] - slide_v[1]),
        0.5 * ice * weight_v[...],
        1.0 / (REG_GAMMA * (1.0 + 4.0 * REG_SMOOTH) + DIAG_SCALE * stuck * coef * coef),
        grad_v[...],
        warm_v[...],
    ]

    def pack_edges(values):
        packed = jnp.zeros((ROWS, LANES), F32)
        for f, value in enumerate(values):
            t0, t1 = tiles(value)
            both = lane_roll(jnp.where(low_half, t0, t1), 16 * f)
            group = ((lane_id + 8) % LANES) // 16 == f
            packed = jnp.where(group, both, packed)
        return packed

    for f, value in enumerate(fields):
        for k in range(2):
            put(first_s, (k, wtiles + f), tiles(value))
    edge_s[1] = pack_edges(fields)

    def count(*offsets):
        return 1 + sum(jnp.where(exists(*n), 1, 0) for n in offsets)

    pl.semaphore_wait(barrier, count((1, 0), (-1, 0)) * count((0, 1), (0, -1)) - 1)

    def send(*copies):
        for n, copy in copies:
            when(exists(*n), copy.start)
        return copies

    def sent(copies):
        for n, copy in copies:
            when(exists(*n), copy.wait_send)

    def arrive(copies):
        for (dx, dy), copy in copies:
            when(exists(-dx, -dy), copy.wait_recv)

    def exchange_edges(stage, edge, edge_in, row_of, rows_in):
        out = []
        for k, n in enumerate(SIDEWAYS):
            out.append((n, pltpu.make_async_remote_copy(
                src_ref=edge, dst_ref=edge_in.at[k],
                send_sem=local_sem.at[k], recv_sem=edge_recv.at[stage, k],
                device_id=at(*n), device_id_type=MESH,
            )))
        for k, dx in enumerate((1, -1)):
            out.append(((dx, 0), pltpu.make_async_remote_copy(
                src_ref=row_of(k), dst_ref=rows_in.at[k],
                send_sem=local_sem.at[6 + k], recv_sem=row_recv.at[stage, k],
                device_id=at(dx, 0), device_id_type=MESH,
            )))
        return send(*out)

    reaches = (1, 2, 4, 8)

    def around(round):
        reach = reaches[round]
        return [(dx * reach, dy * reach) for dx, dy in NEIGHBOURS if abs(dx) * reach < nx and abs(dy) * reach < ny]

    def greet(round):
        for n in around(round):
            when(exists(*n), functools.partial(signal, known_sem.at[round], at(*n)))

    def greeted(round):
        pl.semaphore_wait(known_sem.at[round], count(*around(round)) - 1)

    w_copies = exchange_edges(0, edge_s, edge_r, lambda k: first_s.at[k], first_r)
    greet(0)


    u = jnp.ones((ROWS, 2 * LANES), F32)
    flux = SINK_RATE * eta_v[0] + BED_DRAG * friction
    u_v[0] = u
    for z in range(1, levels):
        u = u + flux * inva_v[z - 1]
        flux = flux + (SINK_RATE * eta_v[z]) * u
        u_v[z] = u

    has_up, has_down = exists(1, 0), exists(-1, 0)
    has_right, has_left = exists(0, 1), exists(0, -1)

    def inside(value, *flags):
        keep = flags[0]
        for flag in flags[1:]:
            keep = keep & flag
        return jnp.where(keep, value, 0.0)

    def join_edges(ref, part, from_right):
        def got(dx, dy):
            return ref[SIDEWAYS.index((-dx, -dy)), part]

        own = jnp.where(
            from_right, inside(got(0, 1), has_right), inside(got(0, -1), has_left)
        )
        up = jnp.where(
            from_right, inside(got(1, 1), has_right, has_up), inside(got(1, -1), has_left, has_up)
        )
        down = jnp.where(
            from_right,
            inside(got(-1, 1), has_right, has_down),
            inside(got(-1, -1), has_left, has_down),
        )
        return own, up, down

    row_packs = {}
    straight_edge = jnp.zeros((ROWS, LANES), F32)
    slanted_edge = jnp.zeros((ROWS, LANES), F32)
    sums = {n: [None, None] for n in NEIGHBOURS}

    def add(table, key, j, term):
        table[key][j] = term if table[key][j] is None else table[key][j] + term

    def seam(ahead0, ahead1, behind0, behind1):
        return (
            [jnp.where(lane_last, ahead1, ahead0), ahead1],
            [behind0, jnp.where(lane_first, behind0, behind1)],
        )

    for z in range(levels - 1, -1, -1):
        u = u_v[z]
        eu = eta_v[z] * u
        near_u = near_eu = None
        for other in (z - 1, z + 1):
            if 0 <= other < levels:
                beside = u_v[other]
                near_u = beside if near_u is None else near_u + beside
                beside = eta_v[other] * beside
                near_eu = beside if near_eu is None else near_eu + beside
        straight = (eu + 0.5 * near_eu, u + 0.5 * near_u)
        slanted = (0.5 * eu + (1.0 / 3.0) * near_eu, 0.5 * u + (1.0 / 3.0) * near_u)
        for f in range(2):
            m = slot(z, f)
            for kind, value in enumerate((straight[f], slanted[f])):
                for side, row in enumerate((0, ROWS - 1)):
                    packed = pack_row(row_packs.get((kind, side)), value, row, m)
                    row_packs[kind, side] = packed
                    if m % ROWS == ROWS - 1:
                        put(pack_v, (kind, side, m // ROWS), packed)
            s_pair, d_pair = tiles(straight[f]), tiles(slanted[f])
            straight_edge = pack_lanes(straight_edge, jnp.where(low_half, *s_pair), m)
            slanted_edge = pack_lanes(slanted_edge, jnp.where(low_half, *d_pair), m)
            t0, t1 = tiles(w_v[m])
            plus_pair, minus_pair = seam(wahead_v[m], lane_roll(t1, -1), lane_roll(t0, 1), wbehind_v[m])
            by_lane = {0: [t0, t1], 1: plus_pair, -1: minus_pair}
            for j in range(2):
                for dy in (-1, 1):
                    add(sums, (0, dy), j, s_pair[j] * by_lane[dy][j])
                for dx in (-1, 1):
                    s_rolled = row_roll(s_pair[j], dx)
                    d_rolled = row_roll(d_pair[j], dx)
                    for dy in (-1, 0, 1):
                        rolled = d_rolled if dy else s_rolled
                        add(sums, (dx, dy), j, rolled * by_lane[dy][j])

    greeted(0)
    greet(1)
    sent(w_copies)
    arrive(w_copies)

    even_lane = lane_id % 2 == 0
    e_own, e_up, e_down = join_edges(edge_r, 0, ~even_lane)
    e_beyond = jnp.where(row_id < 4, e_up, e_down)
    edge_of = {
        0: e_own,
        1: row_roll(jnp.where(row_first, e_beyond, e_own), -1),
        -1: row_roll(jnp.where(row_last, e_beyond, e_own), 1),
    }
    edge_sums = {}
    for dx in (-1, 0, 1):
        product = (slanted_edge if dx else straight_edge) * edge_of[dx]
        for dy in (-1, 1):
            part = jnp.where(even_lane == (dy < 0), product, 0.0)
            edge_sums[dx, dy] = jnp.sum(part, axis=1, keepdims=True)

    row_sums = {(dx, dy): [None, None] for dx in (-1, 1) for dy in (-1, 0, 1)}
    for side, flag in ((0, has_down), (1, has_up)):
        dx = 2 * side - 1
        for g in range(2 * levels // ROWS):
            t0, t1 = tiles(inside(first_r[side, g], flag))
            plus_pair, minus_pair = seam(
                lane_roll(t0, -1), lane_roll(t1, -1), lane_roll(t0, 1), lane_roll(t1, 1)
            )
            by_lane = {0: [t0, t1], 1: plus_pair, -1: minus_pair}
            for dy in (-1, 0, 1):
                weight = tiles(pack_v[1 if dy else 0, side, g])
                for j in range(2):
                    add(row_sums, (dx, dy), j, weight[j] * by_lane[dy][j])

    for (dx, dy), pair in sums.items():
        for j in range(2):
            value = pair[j]
            if dx:
                beyond = jnp.sum(row_sums[dx, dy][j], axis=0, keepdims=True)
                value = jnp.where(row_last if dx > 0 else row_first, beyond, row_roll(value, -dx))
            if dy and j == (dy + 1) // 2:
                value = jnp.where(lane_last if dy > 0 else lane_first, edge_sums[dx, dy], value)
            pair[j] = value
    scaled = [(0.5 * OFFSET_WEIGHT) * t for t in tiles(gain)]
    coefs = []
    for i, n in enumerate(NEIGHBOURS):
        pair = [scaled[j] * sums[n][j] for j in range(2)]
        coefs.append(jnp.concatenate(pair, axis=1))
        krow_s[i, :, :LANES] = pair[0]
        krow_s[i, :, LANES:] = pair[1]
    kedge_s[0] = pack_edges(coefs)
    k_copies = exchange_edges(1, kedge_s, kedge_r, lambda k: krow_s, krow_r)

    greeted(1)
    greet(2)

    group_right = lane_id % 16 < 8

    def wide(values, row_ref, start, edge_ref, part):
        joined = join_edges(edge_ref, part, group_right)
        out = []
        for f, value in enumerate(values):
            rows = [
                tiles(value),
                tiles(inside(row_ref[1, start + f], has_up)),
                tiles(inside(row_ref[0, start + f], has_down)),
            ]
            out.append(
                [rows[i] + [lane_roll(joined[i], -16 * f)] for i in range(3)]
            )
        return out

    *source, half_obs, diag, grad, warm = wide(fields, first_r, wtiles, edge_r, 1)

    def each(fn, *args):
        return [[fn(*(a[i][j] for a in args)) for j in range(3)] for i in range(len(args[0]))]

    def from_row(a, dx):
        if dx == 0:
            return a
        mask = row_first if dx > 0 else row_last
        return [
            [row_roll(jnp.where(mask, a[(i + dx) % len(a)][j], a[i][j]), -dx) for j in range(3)]
            for i in range(len(a))
        ]

    def from_lane(a, dy):
        if dy == 0:
            return a
        mask = lane_first if dy > 0 else lane_last
        return [
            [lane_roll(jnp.where(mask, a[i][(j + dy) % 3], a[i][j]), -dy) for j in range(3)]
            for i in range(len(a))
        ]

    def plus(*args):
        return each(lambda *t: functools.reduce(lambda a, b: a + b, t), *args)

    def times(a, b):
        return each(lambda s, t: s * t, a, b)

    def smooth(q):
        return each(
            lambda c, a, b, d, e: REG_GAMMA * (c + REG_SMOOTH * (4.0 * c - (a + b + d + e))),
            q, from_row(q, 1), from_row(q, -1), from_lane(q, 1), from_lane(q, -1),
        )

    def to_surface(op, q):
        out = []
        for c in range(2):
            spread = times(op.source[c], q)
            result = spread
            for dy in (-1, 0, 1):
                near_lane = from_lane(spread, dy)
                for dx in (-1, 0, 1):
                    if (dx, dy) != (0, 0):
                        result = plus(result, times(op.stencil[c][dx, dy], from_row(near_lane, dx)))
            out.append(result)
        return out

    def to_bed(op, surface):
        out = []
        for c in range(2):
            traction = times(op.half_obs, surface[c])
            result = traction
            for dy in (-1, 0, 1):
                gathered = None
                for dx in (-1, 0, 1):
                    if (dx, dy) != (0, 0):
                        term = from_row(times(op.stencil[c][-dx, -dy], traction), dx)
                        gathered = term if gathered is None else plus(gathered, term)
                result = plus(result, from_lane(gathered, dy))
            out.append(times(op.source[c], result))
        return plus(*out)

    def hessian(op, q):
        return plus(to_bed(op, to_surface(op, q)), smooth(q))

    def operator(source, half_obs, coefs):
        return Operator(source, half_obs, [
            {
                (dx, dy): each(lambda t: (1.0 + sign * CROSS_SHARE * dx * dy) * t, value) if dx * dy else value
                for (dx, dy), value in coefs.items()
            }
            for sign in (1, -1)
        ])

    def narrow(a):
        return [a[0], [jnp.where(row_id < ROWS // 2, a[1][j], a[2][j]) for j in range(3)]]

    greeted(2)
    greet(3)
    arrive(k_copies)
    coefs = dict(zip(NEIGHBOURS, wide(coefs, krow_r, 0, kedge_r, 0)))
    resid = each(lambda a, b: a - b, grad, hessian(operator(source, half_obs, coefs), warm))
    resid, diag = narrow(resid), narrow(diag)
    op = operator([narrow(t) for t in source], narrow(half_obs), {n: narrow(t) for n, t in coefs.items()})
    dir0 = times(diag, resid)
    img0 = hessian(op, dir0)
    dir1 = times(diag, img0)
    surf1 = to_surface(op, dir1)
    smooth1 = smooth(dir1)

    def own_sum(fn):
        t = fn(0) + fn(1)
        return jnp.sum(t, axis=0, keepdims=True)

    dots = [
        own_sum(lambda j: resid[0][j] * dir0[0][j]),
        own_sum(lambda j: dir0[0][j] * img0[0][j]),
        own_sum(lambda j: img0[0][j] * dir1[0][j]),
        own_sum(
            lambda j: half_obs[0][j] * (surf1[0][0][j] * surf1[0][0][j] + surf1[1][0][j] * surf1[1][0][j])
            + dir1[0][j] * smooth1[0][j]
        ),
    ]
    partial = jnp.zeros((ROWS, LANES), F32)
    for q, value in enumerate(dots):
        partial = jnp.where(row_id == q, value, partial)
    partial = jnp.sum(partial, axis=1, keepdims=True)
    partial = jnp.sum(jnp.where(lane_id // 32 == row_id, partial, 0.0), axis=0, keepdims=True)

    def all_sent(sem, ref, n):
        whole = ref.at[pl.ds(0, n - 1)]
        pltpu.make_async_copy(whole, whole, sem).wait()

    def gather_sums(ref, sem, n):
        all_sent(sem, ref, n)
        value = ref[0]
        for k in range(1, n):
            value = value + ref[k]
        return value

    sum_s[...] = partial
    me = my * nx + mx
    greeted(3)
    circ = lambda v, n: min(v % n, n - v % n)
    far = lambda o: circ(o[0] / 2, nx // 2) + circ(o[1] % 4, 4) + circ(o[1] // 4, 4)
    offsets = sorted(
        [(i, j) for i in range(nx) for j in range(ny) if (i, j) != (0, 0)], key=far, reverse=True
    )
    for i, j in offsets:
        pltpu.make_async_remote_copy(
            src_ref=sum_s, dst_ref=sum_r.at[me], send_sem=sum_send, recv_sem=sum_recv,
            device_id=(lax.rem(mx + i, nx), lax.rem(my + j, ny)), device_id_type=MESH,
        ).start()
    sum_r[me] = partial
    img1 = plus(to_bed(op, surf1), smooth1)
    sent(k_copies)
    partial = gather_sums(sum_r, sum_recv, nx * ny)
    s0, s1, s2, s3 = (
        jnp.broadcast_to(partial[:, 32 * q : 32 * q + 1], (ROWS, LANES)) for q in range(4)
    )

    step0 = s0 / s1
    ratio = (step0 * step0 * s2 - s0) / s0
    grow = 1.0 + ratio
    bend = grow * grow * s1 - 2.0 * grow * step0 * s2 + step0 * step0 * s3
    step1 = ratio * s0 / bend
    for j in range(2):
        cols = slice(j * LANES, (j + 1) * LANES)
        sol_o[:, cols] = warm[0][j] + step0 * dir0[0][j]
        res_o[:, cols] = resid[0][j] - step0 * img0[0][j]
        step_o[:, cols] = step1
        along_o[:, cols] = grow * dir0[0][j] - step0 * dir1[0][j]
        image_o[:, cols] = grow * img0[0][j] - step0 * img1[0][j]

    all_sent(sum_send, sum_r, nx * ny)


def solution(mesh):
    nx, ny = mesh.shape["gx"], mesh.shape["gy"]

    def on_device(grad, warm, eta, coef, slide, weight, ice, ground):
        levels, rows, cols = eta.shape
        vmem = lambda *shape: pltpu.VMEM(shape, F32)
        wtiles = 2 * levels // ROWS
        dma = lambda *shape: pltpu.SemaphoreType.DMA(shape)
        call = pl.pallas_call(
            functools.partial(kernel, nx=nx, ny=ny, levels=levels),
            out_shape=(pltpu.VMEM((rows, cols), F32),) * 5,
            in_specs=[pl.BlockSpec(memory_space=pl.ANY)] * 8,
            out_specs=(pl.BlockSpec(memory_space=pltpu.VMEM),) * 5,
            scratch_shapes=[
                vmem(rows, cols), vmem(rows, cols), vmem(levels, rows, cols), vmem(rows, cols),
                vmem(2, rows, cols), vmem(rows, cols),
                pltpu.VMEM((rows, cols), jnp.int32), pltpu.VMEM((rows, cols), jnp.int32),
                vmem(2 * levels, rows, cols), vmem(2 * levels, rows, LANES), vmem(2 * levels, rows, LANES),
                vmem(levels, rows, cols), vmem(levels, rows, cols), vmem(2, 2, wtiles, rows, cols),
                vmem(2, wtiles + 6, rows, cols), vmem(2, wtiles + 6, rows, cols),
                vmem(2, rows, LANES), vmem(6, 2, rows, LANES),
                vmem(8, rows, cols), vmem(2, 8, rows, cols),
                vmem(1, rows, LANES), vmem(6, 1, rows, LANES),
                vmem(1, LANES), vmem(nx * ny, 1, LANES),
                dma(8), dma(2, 2), dma(2, 6), pltpu.SemaphoreType.REGULAR((4,)), dma(), dma(),
            ],
            compiler_params=pltpu.CompilerParams(collective_id=0, has_side_effects=True),
        )
        sol, res, step, along, image = call(grad, warm, eta, coef, slide, weight, ice, ground)
        return sol + step * along, res - step * image

    return jax.shard_map(
        on_device,
        mesh=mesh,
        in_specs=(
            P("gx", "gy"), P("gx", "gy"), P(None, "gx", "gy"), P("gx", "gy"),
            P(None, "gx", "gy"), P("gx", "gy"), P("gx", "gy"), P("gx", "gy"),
        ),
        out_specs=(P("gx", "gy"), P("gx", "gy")),
        check_vma=False,
    )
```

```python
import collections
import functools

import jax
import jax.numpy as jnp
from jax import lax
from jax.experimental import pallas as pl
from jax.experimental.pallas import tpu as pltpu
from jax.sharding import PartitionSpec as P

MESH = pl.DeviceIdType.MESH
F32 = jnp.float32

VERT_COUPLING = 128.0
SINK_RATE = 0.0625
BED_DRAG = 0.5
OFFSET_WEIGHT = 0.0019
CROSS_SHARE = 0.5
REG_GAMMA = 0.02
REG_SMOOTH = 1.0
DIAG_SCALE = 0.003

ROWS = 8
LANES = 128
NEIGHBOURS = [(dx, dy) for dx in (-1, 0, 1) for dy in (-1, 0, 1) if (dx, dy) != (0, 0)]
CORNERS_FIRST = sorted(NEIGHBOURS, key=lambda n: -abs(n[0]) - abs(n[1]))
SIDEWAYS = [(dx, dy) for dx in (-1, 0, 1) for dy in (-1, 1)]

Operator = collections.namedtuple("Operator", "source half_obs stencil")


def row_roll(tile, shift):
    return pltpu.roll(tile, shift % ROWS, axis=0)


def lane_roll(tile, shift):
    shift = shift % LANES
    return tile if shift == 0 else pltpu.roll(tile, shift, axis=1)


def kernel(
    grad_h, warm_h, eta_h, coef_h, slide_h, weight_h, ice_h, ground_h,
    sol_o, res_o, step_o, along_o, image_o,
    grad_v, warm_v, eta_v, coef_v, slide_v, weight_v, ice_v, ground_v,
    w_v, wahead_v, wbehind_v, u_v, inva_v, pack_v,
    first_s, first_r, edge_s, edge_r,
    krow_s, krow_r, kedge_s, kedge_r,
    sum_s, sum_r,
    load_sem, send_sem, recv_sem, known_sem, sum_send, sum_recv,
    *, nx, ny, levels,
):
    mx = lax.axis_index("gx")
    my = lax.axis_index("gy")

    def at(dx, dy):
        return (mx + dx, my + dy)

    def exists(dx, dy):
        tests = []
        if dx:
            tests.append(mx < nx - dx if dx > 0 else mx >= -dx)
        if dy:
            tests.append(my < ny - dy if dy > 0 else my >= -dy)
        return functools.reduce(lambda a, b: a & b, tests)

    def when(flag, *actions):
        @pl.when(flag)
        def _():
            for action in actions:
                action()

    def signal(sem, peer):
        pl.semaphore_signal(sem, inc=1, device_id=peer, device_id_type=MESH)

    barrier = pltpu.get_barrier_semaphore()
    for n in CORNERS_FIRST:
        when(exists(*n), functools.partial(signal, barrier, at(*n)))

    pairs = [
        (eta_h, eta_v), (coef_h, coef_v), (ground_h, ground_v), (ice_h, ice_v),
        (slide_h, slide_v), (weight_h, weight_v), (grad_h, grad_v), (warm_h, warm_v),
    ]
    for i, (src, dst) in enumerate(pairs):
        pltpu.make_async_copy(src, dst, load_sem.at[0 if i < 3 else 1]).start()

    def settle(ref, count, sem):
        whole = ref.at[pl.ds(0, count)]
        pltpu.make_async_copy(whole, whole, sem).wait()

    row_id = lax.broadcasted_iota(jnp.int32, (ROWS, LANES), 0)
    lane_id = lax.broadcasted_iota(jnp.int32, (ROWS, LANES), 1)
    row_first = row_id == 0
    row_last = row_id == ROWS - 1
    lane_first = lane_id == 0
    lane_last = lane_id == LANES - 1
    low_half = lane_id < LANES // 2

    def tiles(value):
        return [value[:, :LANES], value[:, LANES:]]

    settle(w_v, levels + 2, load_sem.at[0])
    friction = ground_v[...].astype(F32) * coef_v[...]

    slot = lambda z, f: 2 * (levels - 1 - z) + f
    wtiles = 2 * levels // ROWS

    def pack_row(packed, value, row, m):
        parts = [row_roll(t, m % ROWS - row) for t in tiles(value)]
        if m % ROWS == 0:
            return parts
        return [jnp.where(row_id == m % ROWS, a, b) for a, b in zip(parts, packed)]

    def put(ref, index, pair):
        ref[index + (slice(None), slice(0, LANES))] = pair[0]
        ref[index + (slice(None), slice(LANES, 2 * LANES))] = pair[1]

    def pack_lanes(packed, both, m):
        here = (lane_id == 2 * m) | (lane_id == (2 * m - 1) % LANES)
        return jnp.where(here, lane_roll(both, 2 * m), packed)

    first_rows = last_rows = None
    edge_packed = jnp.zeros((ROWS, LANES), F32)
    w = jnp.ones((ROWS, 2 * LANES), F32)
    eta = eta_v[levels - 1]
    flux = SINK_RATE * eta
    for z in range(levels - 1, -1, -1):
        if z < levels - 1:
            above, eta = eta, eta_v[z]
            inva = 1.0 / ((0.5 * VERT_COUPLING) * (above + eta))
            inva_v[z] = inva
            w = w + flux * inva
            flux = flux + (SINK_RATE * eta) * w
        for f, field in enumerate((w, eta * w)):
            m = slot(z, f)
            w_v[m] = field
            last_rows = pack_row(last_rows, field, ROWS - 1, m)
            first_rows = pack_row(first_rows, field, 0, m)
            if m % ROWS == ROWS - 1:
                put(first_s, (0, m // ROWS), last_rows)
                put(first_s, (1, m // ROWS), first_rows)
            t0, t1 = tiles(field)
            ahead = lane_roll(t0, -1)
            behind = lane_roll(t1, 1)
            wahead_v[m] = ahead
            wbehind_v[m] = behind
            edge_packed = pack_lanes(edge_packed, jnp.where(low_half, behind, ahead), m)
    edge_s[0] = edge_packed
    total = flux + BED_DRAG * friction * w
    gain = 1.0 / total

    settle(w_v, 6, load_sem.at[1])
    ice = ice_v[...].astype(F32)
    coef = coef_v[...]
    stuck = ice * ground_v[...].astype(F32)
    source_gain = stuck * coef * gain
    fields = [
        source_gain * (slide_v[0] + slide_v[1]),
        source_gain * (slide_v[0] - slide_v[1]),
        0.5 * ice * weight_v[...],
        1.0 / (REG_GAMMA * (1.0 + 4.0 * REG_SMOOTH) + DIAG_SCALE * stuck * coef * coef),
        grad_v[...],
        warm_v[...],
    ]

    def pack_edges(values):
        packed = jnp.zeros((ROWS, LANES), F32)
        for f, value in enumerate(values):
            t0, t1 = tiles(value)
            both = lane_roll(jnp.where(low_half, t0, t1), 16 * f)
            group = ((lane_id + 8) % LANES) // 16 == f
            packed = jnp.where(group, both, packed)
        return packed

    for f, value in enumerate(fields):
        for k in range(2):
            put(first_s, (k, wtiles + f), tiles(value))
    edge_s[1] = pack_edges(fields)

    def count(*offsets):
        return 1 + sum(jnp.where(exists(*n), 1, 0) for n in offsets)

    pl.semaphore_wait(barrier, count((1, 0), (-1, 0)) * count((0, 1), (0, -1)) - 1)

    def all_neighbours(ref, per_row, per_edge, sem):
        for beside in (1, 2):
            for aside in (1, 2):
                many_rows = exists(1, 0) & exists(-1, 0) if beside == 2 else ~(exists(1, 0) & exists(-1, 0))
                many_edges = exists(0, 1) & exists(0, -1) if aside == 2 else ~(exists(0, 1) & exists(0, -1))
                size = beside * per_row + (beside + 1) * aside * per_edge
                when(many_rows & many_edges, functools.partial(settle, ref, size, sem))

    def exchange_edges(stage, edge, edge_in, row_of, rows_in):
        for k, n in enumerate(SIDEWAYS):
            when(exists(*n), pltpu.make_async_remote_copy(
                src_ref=edge, dst_ref=edge_in.at[k],
                send_sem=send_sem.at[stage], recv_sem=recv_sem.at[stage],
                device_id=at(*n), device_id_type=MESH,
            ).start)
        for k, dx in enumerate((1, -1)):
            when(exists(dx, 0), pltpu.make_async_remote_copy(
                src_ref=row_of(k), dst_ref=rows_in.at[k],
                send_sem=send_sem.at[stage], recv_sem=recv_sem.at[stage],
                device_id=at(dx, 0), device_id_type=MESH,
            ).start)

    reaches = (1, 2, 4, 8)

    def around(round):
        reach = reaches[round]
        return [(dx * reach, dy * reach) for dx, dy in NEIGHBOURS if abs(dx) * reach < nx and abs(dy) * reach < ny]

    def greet(round):
        for n in around(round):
            when(exists(*n), functools.partial(signal, known_sem.at[round], at(*n)))

    def greeted(round):
        pl.semaphore_wait(known_sem.at[round], count(*around(round)) - 1)

    exchange_edges(0, edge_s, edge_r, lambda k: first_s.at[k], first_r)
    greet(0)


    u = jnp.ones((ROWS, 2 * LANES), F32)
    flux = SINK_RATE * eta_v[0] + BED_DRAG * friction
    u_v[0] = u
    for z in range(1, levels):
        u = u + flux * inva_v[z - 1]
        flux = flux + (SINK_RATE * eta_v[z]) * u
        u_v[z] = u

    has_up, has_down = exists(1, 0), exists(-1, 0)
    has_right, has_left = exists(0, 1), exists(0, -1)

    def inside(value, *flags):
        keep = flags[0]
        for flag in flags[1:]:
            keep = keep & flag
        return jnp.where(keep, value, 0.0)

    def join_edges(ref, part, from_right):
        def got(dx, dy):
            return ref[SIDEWAYS.index((-dx, -dy)), part]

        own = jnp.where(
            from_right, inside(got(0, 1), has_right), inside(got(0, -1), has_left)
        )
        up = jnp.where(
            from_right, inside(got(1, 1), has_right, has_up), inside(got(1, -1), has_left, has_up)
        )
        down = jnp.where(
            from_right,
            inside(got(-1, 1), has_right, has_down),
            inside(got(-1, -1), has_left, has_down),
        )
        return own, up, down

    row_packs = {}
    straight_edge = jnp.zeros((ROWS, LANES), F32)
    slanted_edge = jnp.zeros((ROWS, LANES), F32)
    sums = {n: [None, None] for n in NEIGHBOURS}

    def add(table, key, j, term):
        table[key][j] = term if table[key][j] is None else table[key][j] + term

    def seam(ahead0, ahead1, behind0, behind1):
        return (
            [jnp.where(lane_last, ahead1, ahead0), ahead1],
            [behind0, jnp.where(lane_first, behind0, behind1)],
        )

    for z in range(levels - 1, -1, -1):
        u = u_v[z]
        eu = eta_v[z] * u
        near_u = near_eu = None
        for other in (z - 1, z + 1):
            if 0 <= other < levels:
                beside = u_v[other]
                near_u = beside if near_u is None else near_u + beside
                beside = eta_v[other] * beside
                near_eu = beside if near_eu is None else near_eu + beside
        straight = (eu + 0.5 * near_eu, u + 0.5 * near_u)
        slanted = (0.5 * eu + (1.0 / 3.0) * near_eu, 0.5 * u + (1.0 / 3.0) * near_u)
        for f in range(2):
            m = slot(z, f)
            for kind, value in enumerate((straight[f], slanted[f])):
                for side, row in enumerate((0, ROWS - 1)):
                    packed = pack_row(row_packs.get((kind, side)), value, row, m)
                    row_packs[kind, side] = packed
                    if m % ROWS == ROWS - 1:
                        put(pack_v, (kind, side, m // ROWS), packed)
            s_pair, d_pair = tiles(straight[f]), tiles(slanted[f])
            straight_edge = pack_lanes(straight_edge, jnp.where(low_half, *s_pair), m)
            slanted_edge = pack_lanes(slanted_edge, jnp.where(low_half, *d_pair), m)
            t0, t1 = tiles(w_v[m])
            plus_pair, minus_pair = seam(wahead_v[m], lane_roll(t1, -1), lane_roll(t0, 1), wbehind_v[m])
            by_lane = {0: [t0, t1], 1: plus_pair, -1: minus_pair}
            for j in range(2):
                for dy in (-1, 1):
                    add(sums, (0, dy), j, s_pair[j] * by_lane[dy][j])
                for dx in (-1, 1):
                    s_rolled = row_roll(s_pair[j], dx)
                    d_rolled = row_roll(d_pair[j], dx)
                    for dy in (-1, 0, 1):
                        rolled = d_rolled if dy else s_rolled
                        add(sums, (dx, dy), j, rolled * by_lane[dy][j])

    greeted(0)
    greet(1)
    all_neighbours(w_v, wtiles + 6, 1, send_sem.at[0])
    all_neighbours(w_v, wtiles + 6, 1, recv_sem.at[0])

    even_lane = lane_id % 2 == 0
    e_own, e_up, e_down = join_edges(edge_r, 0, ~even_lane)
    e_beyond = jnp.where(row_id < 4, e_up, e_down)
    edge_of = {
        0: e_own,
        1: row_roll(jnp.where(row_first, e_beyond, e_own), -1),
        -1: row_roll(jnp.where(row_last, e_beyond, e_own), 1),
    }
    edge_sums = {}
    for dx in (-1, 0, 1):
        product = (slanted_edge if dx else straight_edge) * edge_of[dx]
        for dy in (-1, 1):
            part = jnp.where(even_lane == (dy < 0), product, 0.0)
            edge_sums[dx, dy] = jnp.sum(part, axis=1, keepdims=True)

    row_sums = {(dx, dy): [None, None] for dx in (-1, 1) for dy in (-1, 0, 1)}
    for side, flag in ((0, has_down), (1, has_up)):
        dx = 2 * side - 1
        for g in range(2 * levels // ROWS):
            t0, t1 = tiles(inside(first_r[side, g], flag))
            plus_pair, minus_pair = seam(
                lane_roll(t0, -1), lane_roll(t1, -1), lane_roll(t0, 1), lane_roll(t1, 1)
            )
            by_lane = {0: [t0, t1], 1: plus_pair, -1: minus_pair}
            for dy in (-1, 0, 1):
                weight = tiles(pack_v[1 if dy else 0, side, g])
                for j in range(2):
                    add(row_sums, (dx, dy), j, weight[j] * by_lane[dy][j])

    for (dx, dy), pair in sums.items():
        for j in range(2):
            value = pair[j]
            if dx:
                beyond = jnp.sum(row_sums[dx, dy][j], axis=0, keepdims=True)
                value = jnp.where(row_last if dx > 0 else row_first, beyond, row_roll(value, -dx))
            if dy and j == (dy + 1) // 2:
                value = jnp.where(lane_last if dy > 0 else lane_first, edge_sums[dx, dy], value)
            pair[j] = value
    scaled = [(0.5 * OFFSET_WEIGHT) * t for t in tiles(gain)]
    coefs = []
    for i, n in enumerate(NEIGHBOURS):
        pair = [scaled[j] * sums[n][j] for j in range(2)]
        coefs.append(jnp.concatenate(pair, axis=1))
        krow_s[i, :, :LANES] = pair[0]
        krow_s[i, :, LANES:] = pair[1]
    kedge_s[0] = pack_edges(coefs)
    exchange_edges(1, kedge_s, kedge_r, lambda k: krow_s, krow_r)

    greeted(1)
    greet(2)

    group_right = lane_id % 16 < 8

    def wide(values, row_ref, start, edge_ref, part):
        joined = join_edges(edge_ref, part, group_right)
        out = []
        for f, value in enumerate(values):
            rows = [
                tiles(value),
                tiles(inside(row_ref[1, start + f], has_up)),
                tiles(inside(row_ref[0, start + f], has_down)),
            ]
            out.append(
                [rows[i] + [lane_roll(joined[i], -16 * f)] for i in range(3)]
            )
        return out

    *source, half_obs, diag, grad, warm = wide(fields, first_r, wtiles, edge_r, 1)

    def each(fn, *args):
        return [[fn(*(a[i][j] for a in args)) for j in range(3)] for i in range(len(args[0]))]

    def from_row(a, dx):
        if dx == 0:
            return a
        mask = row_first if dx > 0 else row_last
        return [
            [row_roll(jnp.where(mask, a[(i + dx) % len(a)][j], a[i][j]), -dx) for j in range(3)]
            for i in range(len(a))
        ]

    def from_lane(a, dy):
        if dy == 0:
            return a
        mask = lane_first if dy > 0 else lane_last
        return [
            [lane_roll(jnp.where(mask, a[i][(j + dy) % 3], a[i][j]), -dy) for j in range(3)]
            for i in range(len(a))
        ]

    def plus(*args):
        return each(lambda *t: functools.reduce(lambda a, b: a + b, t), *args)

    def times(a, b):
        return each(lambda s, t: s * t, a, b)

    def smooth(q):
        return each(
            lambda c, a, b, d, e: REG_GAMMA * (c + REG_SMOOTH * (4.0 * c - (a + b + d + e))),
            q, from_row(q, 1), from_row(q, -1), from_lane(q, 1), from_lane(q, -1),
        )

    def to_surface(op, q):
        out = []
        for c in range(2):
            spread = times(op.source[c], q)
            result = spread
            for dy in (-1, 0, 1):
                near_lane = from_lane(spread, dy)
                for dx in (-1, 0, 1):
                    if (dx, dy) != (0, 0):
                        result = plus(result, times(op.stencil[c][dx, dy], from_row(near_lane, dx)))
            out.append(result)
        return out

    def to_bed(op, surface):
        out = []
        for c in range(2):
            traction = times(op.half_obs, surface[c])
            result = traction
            for dy in (-1, 0, 1):
                gathered = None
                for dx in (-1, 0, 1):
                    if (dx, dy) != (0, 0):
                        term = from_row(times(op.stencil[c][-dx, -dy], traction), dx)
                        gathered = term if gathered is None else plus(gathered, term)
                result = plus(result, from_lane(gathered, dy))
            out.append(times(op.source[c], result))
        return plus(*out)

    def hessian(op, q):
        return plus(to_bed(op, to_surface(op, q)), smooth(q))

    def operator(source, half_obs, coefs):
        return Operator(source, half_obs, [
            {
                (dx, dy): each(lambda t: (1.0 + sign * CROSS_SHARE * dx * dy) * t, value) if dx * dy else value
                for (dx, dy), value in coefs.items()
            }
            for sign in (1, -1)
        ])

    def narrow(a):
        return [a[0], [jnp.where(row_id < ROWS // 2, a[1][j], a[2][j]) for j in range(3)]]

    greeted(2)
    greet(3)
    all_neighbours(wahead_v, 16, 1, recv_sem.at[1])
    coefs = dict(zip(NEIGHBOURS, wide(coefs, krow_r, 0, kedge_r, 0)))
    resid = each(lambda a, b: a - b, grad, hessian(operator(source, half_obs, coefs), warm))
    resid, diag = narrow(resid), narrow(diag)
    op = operator([narrow(t) for t in source], narrow(half_obs), {n: narrow(t) for n, t in coefs.items()})
    dir0 = times(diag, resid)
    img0 = hessian(op, dir0)
    dir1 = times(diag, img0)
    surf1 = to_surface(op, dir1)
    smooth1 = smooth(dir1)

    def own_sum(fn):
        t = fn(0) + fn(1)
        return jnp.sum(t, axis=0, keepdims=True)

    dots = [
        own_sum(lambda j: resid[0][j] * dir0[0][j]),
        own_sum(lambda j: dir0[0][j] * img0[0][j]),
        own_sum(lambda j: img0[0][j] * dir1[0][j]),
        own_sum(
            lambda j: half_obs[0][j] * (surf1[0][0][j] * surf1[0][0][j] + surf1[1][0][j] * surf1[1][0][j])
            + dir1[0][j] * smooth1[0][j]
        ),
    ]
    partial = jnp.zeros((ROWS, LANES), F32)
    for q, value in enumerate(dots):
        partial = jnp.where(row_id == q, value, partial)
    partial = jnp.sum(partial, axis=1, keepdims=True)
    partial = jnp.sum(jnp.where(lane_id // 32 == row_id, partial, 0.0), axis=0, keepdims=True)

    def gather_sums(ref, sem, n):
        settle(ref, n - 1, sem)
        value = ref[0]
        for k in range(1, n):
            value = value + ref[k]
        return value

    sum_s[...] = partial
    me = my * nx + mx
    greeted(3)
    circ = lambda v, n: min(v % n, n - v % n)
    far = lambda o: circ(o[0] / 2, nx // 2) + circ(o[1] % 4, 4) + circ(o[1] // 4, 4)
    offsets = sorted(
        [(i, j) for i in range(nx) for j in range(ny) if (i, j) != (0, 0)], key=far, reverse=True
    )
    for i, j in offsets:
        pltpu.make_async_remote_copy(
            src_ref=sum_s, dst_ref=sum_r.at[me], send_sem=sum_send, recv_sem=sum_recv,
            device_id=(lax.rem(mx + i, nx), lax.rem(my + j, ny)), device_id_type=MESH,
        ).start()
    sum_r[me] = partial
    img1 = plus(to_bed(op, surf1), smooth1)
    all_neighbours(wahead_v, 16, 1, send_sem.at[1])
    partial = gather_sums(sum_r, sum_recv, nx * ny)
    s0, s1, s2, s3 = (
        jnp.broadcast_to(partial[:, 32 * q : 32 * q + 1], (ROWS, LANES)) for q in range(4)
    )

    step0 = s0 / s1
    ratio = (step0 * step0 * s2 - s0) / s0
    grow = 1.0 + ratio
    bend = grow * grow * s1 - 2.0 * grow * step0 * s2 + step0 * step0 * s3
    step1 = ratio * s0 / bend
    for j in range(2):
        cols = slice(j * LANES, (j + 1) * LANES)
        sol_o[:, cols] = warm[0][j] + step0 * dir0[0][j]
        res_o[:, cols] = resid[0][j] - step0 * img0[0][j]
        step_o[:, cols] = step1
        along_o[:, cols] = grow * dir0[0][j] - step0 * dir1[0][j]
        image_o[:, cols] = grow * img0[0][j] - step0 * img1[0][j]

    settle(sum_r, nx * ny - 1, sum_send)


def solution(mesh):
    nx, ny = mesh.shape["gx"], mesh.shape["gy"]

    def on_device(grad, warm, eta, coef, slide, weight, ice, ground):
        levels, rows, cols = eta.shape
        vmem = lambda *shape: pltpu.VMEM(shape, F32)
        wtiles = 2 * levels // ROWS
        dma = lambda *shape: pltpu.SemaphoreType.DMA(shape)
        call = pl.pallas_call(
            functools.partial(kernel, nx=nx, ny=ny, levels=levels),
            out_shape=(pltpu.VMEM((rows, cols), F32),) * 5,
            in_specs=[pl.BlockSpec(memory_space=pl.ANY)] * 8,
            out_specs=(pl.BlockSpec(memory_space=pltpu.VMEM),) * 5,
            scratch_shapes=[
                vmem(rows, cols), vmem(rows, cols), vmem(levels, rows, cols), vmem(rows, cols),
                vmem(2, rows, cols), vmem(rows, cols),
                pltpu.VMEM((rows, cols), jnp.int32), pltpu.VMEM((rows, cols), jnp.int32),
                vmem(2 * levels, rows, cols), vmem(2 * levels, rows, LANES), vmem(2 * levels, rows, LANES),
                vmem(levels, rows, cols), vmem(levels, rows, cols), vmem(2, 2, wtiles, rows, cols),
                vmem(2, wtiles + 6, rows, cols), vmem(2, wtiles + 6, rows, cols),
                vmem(2, rows, LANES), vmem(6, 2, rows, LANES),
                vmem(8, rows, cols), vmem(2, 8, rows, cols),
                vmem(1, rows, LANES), vmem(6, 1, rows, LANES),
                vmem(1, LANES), vmem(nx * ny, 1, LANES),
                dma(2), dma(2), dma(2), pltpu.SemaphoreType.REGULAR((4,)), dma(), dma(),
            ],
            compiler_params=pltpu.CompilerParams(collective_id=0, has_side_effects=True),
        )
        sol, res, step, along, image = call(grad, warm, eta, coef, slide, weight, ice, ground)
        return sol + step * along, res - step * image

    return jax.shard_map(
        on_device,
        mesh=mesh,
        in_specs=(
            P("gx", "gy"), P("gx", "gy"), P(None, "gx", "gy"), P("gx", "gy"),
            P(None, "gx", "gy"), P("gx", "gy"), P("gx", "gy"), P("gx", "gy"),
        ),
        out_specs=(P("gx", "gy"), P("gx", "gy")),
        check_vma=False,
    )
```

```python
import collections
import functools

import jax
import jax.numpy as jnp
from jax import lax
from jax.experimental import pallas as pl
from jax.experimental.pallas import tpu as pltpu
from jax.sharding import PartitionSpec as P

MESH = pl.DeviceIdType.MESH
F32 = jnp.float32

VERT_COUPLING = 128.0
SINK_RATE = 0.0625
BED_DRAG = 0.5
OFFSET_WEIGHT = 0.0019
CROSS_SHARE = 0.5
REG_GAMMA = 0.02
REG_SMOOTH = 1.0
DIAG_SCALE = 0.003

ROWS = 8
LANES = 128
NEIGHBOURS = [(dx, dy) for dx in (-1, 0, 1) for dy in (-1, 0, 1) if (dx, dy) != (0, 0)]
CORNERS_FIRST = sorted(NEIGHBOURS, key=lambda n: -abs(n[0]) - abs(n[1]))
SIDEWAYS = [(dx, dy) for dx in (-1, 0, 1) for dy in (-1, 1)]

Operator = collections.namedtuple("Operator", "source half_obs stencil")


def row_roll(tile, shift):
    return pltpu.roll(tile, shift % ROWS, axis=0)


def lane_roll(tile, shift):
    shift = shift % LANES
    return tile if shift == 0 else pltpu.roll(tile, shift, axis=1)


def kernel(
    grad_h, warm_h, eta_h, coef_h, slide_h, weight_h, ice_h, ground_h,
    sol_o, res_o, step_o, along_o, image_o,
    grad_v, warm_v, eta_v, coef_v, slide_v, weight_v, ice_v, ground_v,
    w_v, wahead_v, wbehind_v, u_v, inva_v, pack_v,
    first_s, first_r, edge_s, edge_r,
    krow_s, krow_r, kedge_s, kedge_r,
    sum_s, sum_r,
    load_sem, send_sem, recv_sem, known_sem, sum_send, sum_recv,
    *, nx, ny, levels,
):
    mx = lax.axis_index("gx")
    my = lax.axis_index("gy")

    def at(dx, dy):
        return (mx + dx, my + dy)

    def exists(dx, dy):
        tests = []
        if dx:
            tests.append(mx < nx - dx if dx > 0 else mx >= -dx)
        if dy:
            tests.append(my < ny - dy if dy > 0 else my >= -dy)
        return functools.reduce(lambda a, b: a & b, tests)

    def when(flag, *actions):
        @pl.when(flag)
        def _():
            for action in actions:
                action()

    def signal(sem, peer):
        pl.semaphore_signal(sem, inc=1, device_id=peer, device_id_type=MESH)

    barrier = pltpu.get_barrier_semaphore()
    for n in CORNERS_FIRST:
        when(exists(*n), functools.partial(signal, barrier, at(*n)))

    pairs = [
        (eta_h, eta_v), (coef_h, coef_v), (ground_h, ground_v), (ice_h, ice_v),
        (slide_h, slide_v), (weight_h, weight_v), (grad_h, grad_v), (warm_h, warm_v),
    ]
    for i, (src, dst) in enumerate(pairs):
        pltpu.make_async_copy(src, dst, load_sem.at[0 if i < 3 else 1]).start()

    def settle(ref, count, sem):
        whole = ref.at[pl.ds(0, count)]
        pltpu.make_async_copy(whole, whole, sem).wait()

    row_id = lax.broadcasted_iota(jnp.int32, (ROWS, LANES), 0)
    lane_id = lax.broadcasted_iota(jnp.int32, (ROWS, LANES), 1)
    row_first = row_id == 0
    row_last = row_id == ROWS - 1
    lane_first = lane_id == 0
    lane_last = lane_id == LANES - 1
    low_half = lane_id < LANES // 2

    def tiles(value):
        return [value[:, :LANES], value[:, LANES:]]

    settle(w_v, levels + 2, load_sem.at[0])
    friction = ground_v[...].astype(F32) * coef_v[...]

    slot = lambda z, f: 2 * (levels - 1 - z) + f
    wtiles = 2 * levels // ROWS

    def pack_row(packed, value, row, m):
        parts = [row_roll(t, m % ROWS - row) for t in tiles(value)]
        if m % ROWS == 0:
            return parts
        return [jnp.where(row_id == m % ROWS, a, b) for a, b in zip(parts, packed)]

    def put(ref, index, pair):
        ref[index + (slice(None), slice(0, LANES))] = pair[0]
        ref[index + (slice(None), slice(LANES, 2 * LANES))] = pair[1]

    def pack_lanes(packed, both, m):
        here = (lane_id == 2 * m) | (lane_id == (2 * m - 1) % LANES)
        return jnp.where(here, lane_roll(both, 2 * m), packed)

    first_rows = last_rows = None
    edge_packed = jnp.zeros((ROWS, LANES), F32)
    w = jnp.ones((ROWS, 2 * LANES), F32)
    eta = eta_v[levels - 1]
    flux = SINK_RATE * eta
    for z in range(levels - 1, -1, -1):
        if z < levels - 1:
            above, eta = eta, eta_v[z]
            inva = 1.0 / ((0.5 * VERT_COUPLING) * (above + eta))
            inva_v[z] = inva
            w = w + flux * inva
            flux = flux + (SINK_RATE * eta) * w
        for f, field in enumerate((w, eta * w)):
            m = slot(z, f)
            w_v[m] = field
            last_rows = pack_row(last_rows, field, ROWS - 1, m)
            first_rows = pack_row(first_rows, field, 0, m)
            if m % ROWS == ROWS - 1:
                put(first_s, (0, m // ROWS), last_rows)
                put(first_s, (1, m // ROWS), first_rows)
            t0, t1 = tiles(field)
            ahead = lane_roll(t0, -1)
            behind = lane_roll(t1, 1)
            wahead_v[m] = ahead
            wbehind_v[m] = behind
            edge_packed = pack_lanes(edge_packed, jnp.where(low_half, behind, ahead), m)
    edge_s[0] = edge_packed
    total = flux + BED_DRAG * friction * w
    gain = 1.0 / total

    settle(w_v, 6, load_sem.at[1])
    ice = ice_v[...].astype(F32)
    coef = coef_v[...]
    stuck = ice * ground_v[...].astype(F32)
    source_gain = stuck * coef * gain
    fields = [
        source_gain * (slide_v[0] + slide_v[1]),
        source_gain * (slide_v[0] - slide_v[1]),
        0.5 * ice * weight_v[...],
        1.0 / (REG_GAMMA * (1.0 + 4.0 * REG_SMOOTH) + DIAG_SCALE * stuck * coef * coef),
        grad_v[...],
        warm_v[...],
    ]

    def pack_edges(values):
        packed = jnp.zeros((ROWS, LANES), F32)
        for f, value in enumerate(values):
            t0, t1 = tiles(value)
            both = lane_roll(jnp.where(low_half, t0, t1), 16 * f)
            group = ((lane_id + 8) % LANES) // 16 == f
            packed = jnp.where(group, both, packed)
        return packed

    for f, value in enumerate(fields):
        for k in range(2):
            put(first_s, (k, wtiles + f), tiles(value))
    edge_s[1] = pack_edges(fields)

    def count(*offsets):
        return 1 + sum(jnp.where(exists(*n), 1, 0) for n in offsets)

    pl.semaphore_wait(barrier, count((1, 0), (-1, 0)) * count((0, 1), (0, -1)) - 1)

    def all_neighbours(ref, per_row, per_edge, sem):
        for beside in (1, 2):
            for aside in (1, 2):
                many_rows = exists(1, 0) & exists(-1, 0) if beside == 2 else ~(exists(1, 0) & exists(-1, 0))
                many_edges = exists(0, 1) & exists(0, -1) if aside == 2 else ~(exists(0, 1) & exists(0, -1))
                size = beside * per_row + (beside + 1) * aside * per_edge
                when(many_rows & many_edges, functools.partial(settle, ref, size, sem))

    def exchange_edges(stage, edge, edge_in, row_of, rows_in):
        for k, n in enumerate(SIDEWAYS):
            when(exists(*n), pltpu.make_async_remote_copy(
                src_ref=edge, dst_ref=edge_in.at[k],
                send_sem=send_sem.at[stage], recv_sem=recv_sem.at[stage],
                device_id=at(*n), device_id_type=MESH,
            ).start)
        for k, dx in enumerate((1, -1)):
            when(exists(dx, 0), pltpu.make_async_remote_copy(
                src_ref=row_of(k), dst_ref=rows_in.at[k],
                send_sem=send_sem.at[stage], recv_sem=recv_sem.at[stage],
                device_id=at(dx, 0), device_id_type=MESH,
            ).start)

    reaches = (1, 2, 4, 8)

    def around(round):
        reach = reaches[round]
        return [(dx * reach, dy * reach) for dx, dy in NEIGHBOURS if abs(dx) * reach < nx and abs(dy) * reach < ny]

    def greet(round):
        for n in around(round):
            when(exists(*n), functools.partial(signal, known_sem.at[round], at(*n)))

    def greeted(round):
        pl.semaphore_wait(known_sem.at[round], count(*around(round)) - 1)

    exchange_edges(0, edge_s, edge_r, lambda k: first_s.at[k], first_r)
    greet(0)


    u = jnp.ones((ROWS, 2 * LANES), F32)
    flux = SINK_RATE * eta_v[0] + BED_DRAG * friction
    u_v[0] = u
    for z in range(1, levels):
        u = u + flux * inva_v[z - 1]
        flux = flux + (SINK_RATE * eta_v[z]) * u
        u_v[z] = u

    has_up, has_down = exists(1, 0), exists(-1, 0)
    has_right, has_left = exists(0, 1), exists(0, -1)

    def inside(value, *flags):
        keep = flags[0]
        for flag in flags[1:]:
            keep = keep & flag
        return jnp.where(keep, value, 0.0)

    def join_edges(ref, part, from_right):
        def got(dx, dy):
            return ref[SIDEWAYS.index((-dx, -dy)), part]

        own = jnp.where(
            from_right, inside(got(0, 1), has_right), inside(got(0, -1), has_left)
        )
        up = jnp.where(
            from_right, inside(got(1, 1), has_right, has_up), inside(got(1, -1), has_left, has_up)
        )
        down = jnp.where(
            from_right,
            inside(got(-1, 1), has_right, has_down),
            inside(got(-1, -1), has_left, has_down),
        )
        return own, up, down

    row_packs = {}
    straight_edge = jnp.zeros((ROWS, LANES), F32)
    slanted_edge = jnp.zeros((ROWS, LANES), F32)
    sums = {n: [None, None] for n in NEIGHBOURS}

    def add(table, key, j, term):
        table[key][j] = term if table[key][j] is None else table[key][j] + term

    def seam(ahead0, ahead1, behind0, behind1):
        return (
            [jnp.where(lane_last, ahead1, ahead0), ahead1],
            [behind0, jnp.where(lane_first, behind0, behind1)],
        )

    for z in range(levels - 1, -1, -1):
        u = u_v[z]
        eu = eta_v[z] * u
        near_u = near_eu = None
        for other in (z - 1, z + 1):
            if 0 <= other < levels:
                beside = u_v[other]
                near_u = beside if near_u is None else near_u + beside
                beside = eta_v[other] * beside
                near_eu = beside if near_eu is None else near_eu + beside
        straight = (eu + 0.5 * near_eu, u + 0.5 * near_u)
        slanted = (0.5 * eu + (1.0 / 3.0) * near_eu, 0.5 * u + (1.0 / 3.0) * near_u)
        for f in range(2):
            m = slot(z, f)
            for kind, value in enumerate((straight[f], slanted[f])):
                for side, row in enumerate((0, ROWS - 1)):
                    packed = pack_row(row_packs.get((kind, side)), value, row, m)
                    row_packs[kind, side] = packed
                    if m % ROWS == ROWS - 1:
                        put(pack_v, (kind, side, m // ROWS), packed)
            s_pair, d_pair = tiles(straight[f]), tiles(slanted[f])
            straight_edge = pack_lanes(straight_edge, jnp.where(low_half, *s_pair), m)
            slanted_edge = pack_lanes(slanted_edge, jnp.where(low_half, *d_pair), m)
            t0, t1 = tiles(w_v[m])
            plus_pair, minus_pair = seam(wahead_v[m], lane_roll(t1, -1), lane_roll(t0, 1), wbehind_v[m])
            by_lane = {0: [t0, t1], 1: plus_pair, -1: minus_pair}
            for j in range(2):
                for dy in (-1, 1):
                    add(sums, (0, dy), j, s_pair[j] * by_lane[dy][j])
                for dx in (-1, 1):
                    s_rolled = row_roll(s_pair[j], dx)
                    d_rolled = row_roll(d_pair[j], dx)
                    for dy in (-1, 0, 1):
                        rolled = d_rolled if dy else s_rolled
                        add(sums, (dx, dy), j, rolled * by_lane[dy][j])

    greeted(0)
    greet(1)
    all_neighbours(w_v, wtiles + 6, 1, send_sem.at[0])
    all_neighbours(w_v, wtiles + 6, 1, recv_sem.at[0])

    even_lane = lane_id % 2 == 0
    e_own, e_up, e_down = join_edges(edge_r, 0, ~even_lane)
    e_beyond = jnp.where(row_id < 4, e_up, e_down)
    edge_of = {
        0: e_own,
        1: row_roll(jnp.where(row_first, e_beyond, e_own), -1),
        -1: row_roll(jnp.where(row_last, e_beyond, e_own), 1),
    }
    edge_sums = {}
    for dx in (-1, 0, 1):
        product = (slanted_edge if dx else straight_edge) * edge_of[dx]
        for dy in (-1, 1):
            part = jnp.where(even_lane == (dy < 0), product, 0.0)
            edge_sums[dx, dy] = jnp.sum(part, axis=1, keepdims=True)

    row_sums = {(dx, dy): [None, None] for dx in (-1, 1) for dy in (-1, 0, 1)}
    for side, flag in ((0, has_down), (1, has_up)):
        dx = 2 * side - 1
        for g in range(2 * levels // ROWS):
            t0, t1 = tiles(inside(first_r[side, g], flag))
            plus_pair, minus_pair = seam(
                lane_roll(t0, -1), lane_roll(t1, -1), lane_roll(t0, 1), lane_roll(t1, 1)
            )
            by_lane = {0: [t0, t1], 1: plus_pair, -1: minus_pair}
            for dy in (-1, 0, 1):
                weight = tiles(pack_v[1 if dy else 0, side, g])
                for j in range(2):
                    add(row_sums, (dx, dy), j, weight[j] * by_lane[dy][j])

    for (dx, dy), pair in sums.items():
        for j in range(2):
            value = pair[j]
            if dx:
                beyond = jnp.sum(row_sums[dx, dy][j], axis=0, keepdims=True)
                value = jnp.where(row_last if dx > 0 else row_first, beyond, row_roll(value, -dx))
            if dy and j == (dy + 1) // 2:
                value = jnp.where(lane_last if dy > 0 else lane_first, edge_sums[dx, dy], value)
            pair[j] = value
    scaled = [(0.5 * OFFSET_WEIGHT) * t for t in tiles(gain)]
    coefs = []
    for i, n in enumerate(NEIGHBOURS):
        pair = [scaled[j] * sums[n][j] for j in range(2)]
        coefs.append(jnp.concatenate(pair, axis=1))
        krow_s[i, :, :LANES] = pair[0]
        krow_s[i, :, LANES:] = pair[1]
    kedge_s[0] = pack_edges(coefs)
    exchange_edges(1, kedge_s, kedge_r, lambda k: krow_s, krow_r)

    greeted(1)
    greet(2)

    group_right = lane_id % 16 < 8

    def wide(values, row_ref, start, edge_ref, part):
        joined = join_edges(edge_ref, part, group_right)
        out = []
        for f, value in enumerate(values):
            rows = [
                tiles(value),
                tiles(inside(row_ref[1, start + f], has_up)),
                tiles(inside(row_ref[0, start + f], has_down)),
            ]
            out.append(
                [rows[i] + [lane_roll(joined[i], -16 * f)] for i in range(3)]
            )
        return out

    *source, half_obs, diag, grad, warm = wide(fields, first_r, wtiles, edge_r, 1)

    def each(fn, *args):
        return [[fn(*(a[i][j] for a in args)) for j in range(3)] for i in range(len(args[0]))]

    def from_row(a, dx):
        if dx == 0:
            return a
        mask = row_first if dx > 0 else row_last
        return [
            [row_roll(jnp.where(mask, a[(i + dx) % len(a)][j], a[i][j]), -dx) for j in range(3)]
            for i in range(len(a))
        ]

    def from_lane(a, dy):
        if dy == 0:
            return a
        mask = lane_first if dy > 0 else lane_last
        return [
            [lane_roll(jnp.where(mask, a[i][(j + dy) % 3], a[i][j]), -dy) for j in range(3)]
            for i in range(len(a))
        ]

    def plus(*args):
        return each(lambda *t: functools.reduce(lambda a, b: a + b, t), *args)

    def times(a, b):
        return each(lambda s, t: s * t, a, b)

    def smooth(q):
        return each(
            lambda c, a, b, d, e: REG_GAMMA * (c + REG_SMOOTH * (4.0 * c - (a + b + d + e))),
            q, from_row(q, 1), from_row(q, -1), from_lane(q, 1), from_lane(q, -1),
        )

    def to_surface(op, q):
        out = []
        for c in range(2):
            spread = times(op.source[c], q)
            result = spread
            for dy in (-1, 0, 1):
                near_lane = from_lane(spread, dy)
                for dx in (-1, 0, 1):
                    if (dx, dy) != (0, 0):
                        result = plus(result, times(op.stencil[c][dx, dy], from_row(near_lane, dx)))
            out.append(result)
        return out

    def to_bed(op, surface):
        out = []
        for c in range(2):
            traction = times(op.half_obs, surface[c])
            result = traction
            for dy in (-1, 0, 1):
                gathered = None
                for dx in (-1, 0, 1):
                    if (dx, dy) != (0, 0):
                        term = from_row(times(op.stencil[c][-dx, -dy], traction), dx)
                        gathered = term if gathered is None else plus(gathered, term)
                result = plus(result, from_lane(gathered, dy))
            out.append(times(op.source[c], result))
        return plus(*out)

    def hessian(op, q):
        return plus(to_bed(op, to_surface(op, q)), smooth(q))

    def operator(source, half_obs, coefs):
        return Operator(source, half_obs, [
            {
                (dx, dy): each(lambda t: (1.0 + sign * CROSS_SHARE * dx * dy) * t, value) if dx * dy else value
                for (dx, dy), value in coefs.items()
            }
            for sign in (1, -1)
        ])

    def narrow(a):
        return [a[0], [jnp.where(row_id < ROWS // 2, a[1][j], a[2][j]) for j in range(3)]]

    greeted(2)
    greet(3)
    all_neighbours(wahead_v, 16, 1, recv_sem.at[1])
    coefs = dict(zip(NEIGHBOURS, wide(coefs, krow_r, 0, kedge_r, 0)))
    resid = each(lambda a, b: a - b, grad, hessian(operator(source, half_obs, coefs), warm))
    resid, diag = narrow(resid), narrow(diag)
    op = operator([narrow(t) for t in source], narrow(half_obs), {n: narrow(t) for n, t in coefs.items()})
    dir0 = times(diag, resid)
    img0 = hessian(op, dir0)
    dir1 = times(diag, img0)
    surf1 = to_surface(op, dir1)
    smooth1 = smooth(dir1)

    def own_sum(fn):
        t = fn(0) + fn(1)
        return jnp.sum(t, axis=0, keepdims=True)

    dots = [
        own_sum(lambda j: resid[0][j] * dir0[0][j]),
        own_sum(lambda j: dir0[0][j] * img0[0][j]),
        own_sum(lambda j: img0[0][j] * dir1[0][j]),
        own_sum(
            lambda j: half_obs[0][j] * (surf1[0][0][j] * surf1[0][0][j] + surf1[1][0][j] * surf1[1][0][j])
            + dir1[0][j] * smooth1[0][j]
        ),
    ]
    partial = jnp.zeros((ROWS, LANES), F32)
    for q, value in enumerate(dots):
        partial = jnp.where(row_id == q, value, partial)
    partial = jnp.sum(partial, axis=1, keepdims=True)
    partial = jnp.sum(jnp.where(lane_id // 32 == row_id, partial, 0.0), axis=0, keepdims=True)

    def gather_sums(ref, sem, n):
        settle(ref, n - 1, sem)
        parts = [ref[k] for k in range(min(8, n))]
        for k in range(8, n):
            parts[k % 8] = parts[k % 8] + ref[k]
        while len(parts) > 1:
            parts = [functools.reduce(lambda a, b: a + b, parts[k : k + 2]) for k in range(0, len(parts), 2)]
        return parts[0]

    sum_s[...] = partial
    me = my * nx + mx
    greeted(3)
    circ = lambda v, n: min(v % n, n - v % n)
    far = lambda o: circ(o[0] / 2, nx // 2) + circ(o[1] % 4, 4) + circ(o[1] // 4, 4)
    offsets = sorted(
        [(i, j) for i in range(nx) for j in range(ny) if (i, j) != (0, 0)], key=far, reverse=True
    )
    for i, j in offsets:
        pltpu.make_async_remote_copy(
            src_ref=sum_s, dst_ref=sum_r.at[me], send_sem=sum_send, recv_sem=sum_recv,
            device_id=(lax.rem(mx + i, nx), lax.rem(my + j, ny)), device_id_type=MESH,
        ).start()
    sum_r[me] = partial
    img1 = plus(to_bed(op, surf1), smooth1)
    all_neighbours(wahead_v, 16, 1, send_sem.at[1])
    partial = gather_sums(sum_r, sum_recv, nx * ny)
    s0, s1, s2, s3 = (
        jnp.broadcast_to(partial[:, 32 * q : 32 * q + 1], (ROWS, LANES)) for q in range(4)
    )

    step0 = s0 / s1
    ratio = (step0 * step0 * s2 - s0) / s0
    grow = 1.0 + ratio
    bend = grow * grow * s1 - 2.0 * grow * step0 * s2 + step0 * step0 * s3
    step1 = ratio * s0 / bend
    for j in range(2):
        cols = slice(j * LANES, (j + 1) * LANES)
        sol_o[:, cols] = warm[0][j] + step0 * dir0[0][j]
        res_o[:, cols] = resid[0][j] - step0 * img0[0][j]
        step_o[:, cols] = step1
        along_o[:, cols] = grow * dir0[0][j] - step0 * dir1[0][j]
        image_o[:, cols] = grow * img0[0][j] - step0 * img1[0][j]

    settle(sum_r, nx * ny - 1, sum_send)


def solution(mesh):
    nx, ny = mesh.shape["gx"], mesh.shape["gy"]

    def on_device(grad, warm, eta, coef, slide, weight, ice, ground):
        levels, rows, cols = eta.shape
        vmem = lambda *shape: pltpu.VMEM(shape, F32)
        wtiles = 2 * levels // ROWS
        dma = lambda *shape: pltpu.SemaphoreType.DMA(shape)
        call = pl.pallas_call(
            functools.partial(kernel, nx=nx, ny=ny, levels=levels),
            out_shape=(pltpu.VMEM((rows, cols), F32),) * 5,
            in_specs=[pl.BlockSpec(memory_space=pl.ANY)] * 8,
            out_specs=(pl.BlockSpec(memory_space=pltpu.VMEM),) * 5,
            scratch_shapes=[
                vmem(rows, cols), vmem(rows, cols), vmem(levels, rows, cols), vmem(rows, cols),
                vmem(2, rows, cols), vmem(rows, cols),
                pltpu.VMEM((rows, cols), jnp.int32), pltpu.VMEM((rows, cols), jnp.int32),
                vmem(2 * levels, rows, cols), vmem(2 * levels, rows, LANES), vmem(2 * levels, rows, LANES),
                vmem(levels, rows, cols), vmem(levels, rows, cols), vmem(2, 2, wtiles, rows, cols),
                vmem(2, wtiles + 6, rows, cols), vmem(2, wtiles + 6, rows, cols),
                vmem(2, rows, LANES), vmem(6, 2, rows, LANES),
                vmem(8, rows, cols), vmem(2, 8, rows, cols),
                vmem(1, rows, LANES), vmem(6, 1, rows, LANES),
                vmem(1, LANES), vmem(nx * ny, 1, LANES),
                dma(2), dma(2), dma(2), pltpu.SemaphoreType.REGULAR((4,)), dma(), dma(),
            ],
            compiler_params=pltpu.CompilerParams(collective_id=0, has_side_effects=True),
        )
        sol, res, step, along, image = call(grad, warm, eta, coef, slide, weight, ice, ground)
        return sol + step * along, res - step * image

    return jax.shard_map(
        on_device,
        mesh=mesh,
        in_specs=(
            P("gx", "gy"), P("gx", "gy"), P(None, "gx", "gy"), P("gx", "gy"),
            P(None, "gx", "gy"), P("gx", "gy"), P("gx", "gy"), P("gx", "gy"),
        ),
        out_specs=(P("gx", "gy"), P("gx", "gy")),
        check_vma=False,
    )
```

```python
import collections
import functools

import jax
import jax.numpy as jnp
from jax import lax
from jax.experimental import pallas as pl
from jax.experimental.pallas import tpu as pltpu
from jax.sharding import PartitionSpec as P

MESH = pl.DeviceIdType.MESH
F32 = jnp.float32

VERT_COUPLING = 128.0
SINK_RATE = 0.0625
BED_DRAG = 0.5
OFFSET_WEIGHT = 0.0019
CROSS_SHARE = 0.5
REG_GAMMA = 0.02
REG_SMOOTH = 1.0
DIAG_SCALE = 0.003

ROWS = 8
LANES = 128
NEIGHBOURS = [(dx, dy) for dx in (-1, 0, 1) for dy in (-1, 0, 1) if (dx, dy) != (0, 0)]
CORNERS_FIRST = sorted(NEIGHBOURS, key=lambda n: -abs(n[0]) - abs(n[1]))
SIDEWAYS = [(dx, dy) for dx in (-1, 0, 1) for dy in (-1, 1)]

Operator = collections.namedtuple("Operator", "source half_obs stencil")


def row_roll(tile, shift):
    return pltpu.roll(tile, shift % ROWS, axis=0)


def lane_roll(tile, shift):
    shift = shift % LANES
    return tile if shift == 0 else pltpu.roll(tile, shift, axis=1)


def kernel(
    grad_h, warm_h, eta_h, coef_h, slide_h, weight_h, ice_h, ground_h,
    sol_o, res_o, step_o, along_o, image_o,
    grad_v, warm_v, eta_v, coef_v, slide_v, weight_v, ice_v, ground_v,
    w_v, wahead_v, wbehind_v, u_v, inva_v, pack_v,
    first_s, first_r, edge_s, edge_r,
    krow_s, krow_r, kedge_s, kedge_r,
    sum_s, sum_r,
    load_sem, send_sem, recv_sem, known_sem, sum_send, sum_recv,
    *, nx, ny, levels,
):
    mx = lax.axis_index("gx")
    my = lax.axis_index("gy")

    def at(dx, dy):
        return (mx + dx, my + dy)

    def exists(dx, dy):
        tests = []
        if dx:
            tests.append(mx < nx - dx if dx > 0 else mx >= -dx)
        if dy:
            tests.append(my < ny - dy if dy > 0 else my >= -dy)
        return functools.reduce(lambda a, b: a & b, tests)

    def when(flag, *actions):
        @pl.when(flag)
        def _():
            for action in actions:
                action()

    def signal(sem, peer):
        pl.semaphore_signal(sem, inc=1, device_id=peer, device_id_type=MESH)

    barrier = pltpu.get_barrier_semaphore()
    for n in CORNERS_FIRST:
        when(exists(*n), functools.partial(signal, barrier, at(*n)))

    pairs = [
        (eta_h, eta_v), (coef_h, coef_v), (ground_h, ground_v), (ice_h, ice_v),
        (slide_h, slide_v), (weight_h, weight_v), (grad_h, grad_v), (warm_h, warm_v),
    ]
    for i, (src, dst) in enumerate(pairs):
        pltpu.make_async_copy(src, dst, load_sem.at[0 if i < 3 else 1]).start()

    def settle(ref, count, sem):
        whole = ref.at[pl.ds(0, count)]
        pltpu.make_async_copy(whole, whole, sem).wait()

    row_id = lax.broadcasted_iota(jnp.int32, (ROWS, LANES), 0)
    lane_id = lax.broadcasted_iota(jnp.int32, (ROWS, LANES), 1)
    row_first = row_id == 0
    row_last = row_id == ROWS - 1
    lane_first = lane_id == 0
    lane_last = lane_id == LANES - 1
    low_half = lane_id < LANES // 2

    def tiles(value):
        return [value[:, :LANES], value[:, LANES:]]

    settle(w_v, levels + 2, load_sem.at[0])
    friction = ground_v[...].astype(F32) * coef_v[...]

    slot = lambda z, f: 2 * (levels - 1 - z) + f
    wtiles = 2 * levels // ROWS

    def pack_row(packed, value, row, m):
        parts = [row_roll(t, m % ROWS - row) for t in tiles(value)]
        if m % ROWS == 0:
            return parts
        return [jnp.where(row_id == m % ROWS, a, b) for a, b in zip(parts, packed)]

    def put(ref, index, pair):
        ref[index + (slice(None), slice(0, LANES))] = pair[0]
        ref[index + (slice(None), slice(LANES, 2 * LANES))] = pair[1]

    def pack_lanes(packed, both, m):
        here = (lane_id == 2 * m) | (lane_id == (2 * m - 1) % LANES)
        return jnp.where(here, lane_roll(both, 2 * m), packed)

    first_rows = last_rows = None
    edge_packed = jnp.zeros((ROWS, LANES), F32)
    w = jnp.ones((ROWS, 2 * LANES), F32)
    eta = eta_v[levels - 1]
    flux = SINK_RATE * eta
    for z in range(levels - 1, -1, -1):
        if z < levels - 1:
            above, eta = eta, eta_v[z]
            inva = 1.0 / ((0.5 * VERT_COUPLING) * (above + eta))
            inva_v[z] = inva
            w = w + flux * inva
            flux = flux + (SINK_RATE * eta) * w
        for f, field in enumerate((w, eta * w)):
            m = slot(z, f)
            w_v[m] = field
            last_rows = pack_row(last_rows, field, ROWS - 1, m)
            first_rows = pack_row(first_rows, field, 0, m)
            if m % ROWS == ROWS - 1:
                put(first_s, (0, m // ROWS), last_rows)
                put(first_s, (1, m // ROWS), first_rows)
            t0, t1 = tiles(field)
            ahead = lane_roll(t0, -1)
            behind = lane_roll(t1, 1)
            wahead_v[m] = ahead
            wbehind_v[m] = behind
            edge_packed = pack_lanes(edge_packed, jnp.where(low_half, behind, ahead), m)
    edge_s[0] = edge_packed
    total = flux + BED_DRAG * friction * w
    gain = 1.0 / total

    settle(w_v, 6, load_sem.at[1])
    ice = ice_v[...].astype(F32)
    coef = coef_v[...]
    stuck = ice * ground_v[...].astype(F32)
    source_gain = stuck * coef * gain
    fields = [
        source_gain * (slide_v[0] + slide_v[1]),
        source_gain * (slide_v[0] - slide_v[1]),
        0.5 * ice * weight_v[...],
        1.0 / (REG_GAMMA * (1.0 + 4.0 * REG_SMOOTH) + DIAG_SCALE * stuck * coef * coef),
        grad_v[...],
        warm_v[...],
    ]

    def pack_edges(values):
        packed = jnp.zeros((ROWS, LANES), F32)
        for f, value in enumerate(values):
            t0, t1 = tiles(value)
            both = lane_roll(jnp.where(low_half, t0, t1), 16 * f)
            group = ((lane_id + 8) % LANES) // 16 == f
            packed = jnp.where(group, both, packed)
        return packed

    for f, value in enumerate(fields):
        for k in range(2):
            put(first_s, (k, wtiles + f), tiles(value))
    edge_s[1] = pack_edges(fields)

    def count(*offsets):
        return 1 + sum(jnp.where(exists(*n), 1, 0) for n in offsets)

    pl.semaphore_wait(barrier, count((1, 0), (-1, 0)) * count((0, 1), (0, -1)) - 1)

    def all_neighbours(ref, per_row, per_edge, sem):
        for beside in (1, 2):
            for aside in (1, 2):
                many_rows = exists(1, 0) & exists(-1, 0) if beside == 2 else ~(exists(1, 0) & exists(-1, 0))
                many_edges = exists(0, 1) & exists(0, -1) if aside == 2 else ~(exists(0, 1) & exists(0, -1))
                size = beside * per_row + (beside + 1) * aside * per_edge
                when(many_rows & many_edges, functools.partial(settle, ref, size, sem))

    def exchange_edges(stage, edge, edge_in, row_of, rows_in):
        for k, n in enumerate(SIDEWAYS):
            when(exists(*n), pltpu.make_async_remote_copy(
                src_ref=edge, dst_ref=edge_in.at[k],
                send_sem=send_sem.at[stage], recv_sem=recv_sem.at[stage],
                device_id=at(*n), device_id_type=MESH,
            ).start)
        for k, dx in enumerate((1, -1)):
            when(exists(dx, 0), pltpu.make_async_remote_copy(
                src_ref=row_of(k), dst_ref=rows_in.at[k],
                send_sem=send_sem.at[stage], recv_sem=recv_sem.at[stage],
                device_id=at(dx, 0), device_id_type=MESH,
            ).start)

    reaches = (1, 2, 4, 8)

    def around(round):
        reach = reaches[round]
        return [(dx * reach, dy * reach) for dx, dy in NEIGHBOURS if abs(dx) * reach < nx and abs(dy) * reach < ny]

    def greet(round):
        for n in around(round):
            when(exists(*n), functools.partial(signal, known_sem.at[round], at(*n)))

    def greeted(round):
        pl.semaphore_wait(known_sem.at[round], count(*around(round)) - 1)

    exchange_edges(0, edge_s, edge_r, lambda k: first_s.at[k], first_r)
    greet(0)


    u = jnp.ones((ROWS, 2 * LANES), F32)
    flux = SINK_RATE * eta_v[0] + BED_DRAG * friction
    u_v[0] = u
    for z in range(1, levels):
        u = u + flux * inva_v[z - 1]
        flux = flux + (SINK_RATE * eta_v[z]) * u
        u_v[z] = u

    has_up, has_down = exists(1, 0), exists(-1, 0)
    has_right, has_left = exists(0, 1), exists(0, -1)

    def inside(value, *flags):
        keep = flags[0]
        for flag in flags[1:]:
            keep = keep & flag
        return jnp.where(keep, value, 0.0)

    def join_edges(ref, part, from_right):
        def got(dx, dy):
            return ref[SIDEWAYS.index((-dx, -dy)), part]

        own = jnp.where(
            from_right, inside(got(0, 1), has_right), inside(got(0, -1), has_left)
        )
        up = jnp.where(
            from_right, inside(got(1, 1), has_right, has_up), inside(got(1, -1), has_left, has_up)
        )
        down = jnp.where(
            from_right,
            inside(got(-1, 1), has_right, has_down),
            inside(got(-1, -1), has_left, has_down),
        )
        return own, up, down

    row_packs = {}
    straight_edge = jnp.zeros((ROWS, LANES), F32)
    slanted_edge = jnp.zeros((ROWS, LANES), F32)
    sums = {n: [None, None] for n in NEIGHBOURS}

    def add(table, key, j, term):
        table[key][j] = term if table[key][j] is None else table[key][j] + term

    def seam(ahead0, ahead1, behind0, behind1):
        return (
            [jnp.where(lane_last, ahead1, ahead0), ahead1],
            [behind0, jnp.where(lane_first, behind0, behind1)],
        )

    for z in range(levels - 1, -1, -1):
        u = u_v[z]
        eu = eta_v[z] * u
        near_u = near_eu = None
        for other in (z - 1, z + 1):
            if 0 <= other < levels:
                beside = u_v[other]
                near_u = beside if near_u is None else near_u + beside
                beside = eta_v[other] * beside
                near_eu = beside if near_eu is None else near_eu + beside
        straight = (eu + 0.5 * near_eu, u + 0.5 * near_u)
        slanted = (0.5 * eu + (1.0 / 3.0) * near_eu, 0.5 * u + (1.0 / 3.0) * near_u)
        for f in range(2):
            m = slot(z, f)
            for kind, value in enumerate((straight[f], slanted[f])):
                for side, row in enumerate((0, ROWS - 1)):
                    packed = pack_row(row_packs.get((kind, side)), value, row, m)
                    row_packs[kind, side] = packed
                    if m % ROWS == ROWS - 1:
                        put(pack_v, (kind, side, m // ROWS), packed)
            s_pair, d_pair = tiles(straight[f]), tiles(slanted[f])
            straight_edge = pack_lanes(straight_edge, jnp.where(low_half, *s_pair), m)
            slanted_edge = pack_lanes(slanted_edge, jnp.where(low_half, *d_pair), m)
            t0, t1 = tiles(w_v[m])
            plus_pair, minus_pair = seam(wahead_v[m], lane_roll(t1, -1), lane_roll(t0, 1), wbehind_v[m])
            by_lane = {0: [t0, t1], 1: plus_pair, -1: minus_pair}
            for j in range(2):
                for dy in (-1, 1):
                    add(sums, (0, dy), j, s_pair[j] * by_lane[dy][j])
                for dx in (-1, 1):
                    s_rolled = row_roll(s_pair[j], dx)
                    d_rolled = row_roll(d_pair[j], dx)
                    for dy in (-1, 0, 1):
                        rolled = d_rolled if dy else s_rolled
                        add(sums, (dx, dy), j, rolled * by_lane[dy][j])

    greeted(0)
    greet(1)
    all_neighbours(w_v, wtiles + 6, 1, send_sem.at[0])
    all_neighbours(w_v, wtiles + 6, 1, recv_sem.at[0])

    even_lane = lane_id % 2 == 0
    e_own, e_up, e_down = join_edges(edge_r, 0, ~even_lane)
    e_beyond = jnp.where(row_id < 4, e_up, e_down)
    edge_of = {
        0: e_own,
        1: row_roll(jnp.where(row_first, e_beyond, e_own), -1),
        -1: row_roll(jnp.where(row_last, e_beyond, e_own), 1),
    }
    edge_sums = {}
    for dx in (-1, 0, 1):
        product = (slanted_edge if dx else straight_edge) * edge_of[dx]
        for dy in (-1, 1):
            part = jnp.where(even_lane == (dy < 0), product, 0.0)
            edge_sums[dx, dy] = jnp.sum(part, axis=1, keepdims=True)

    row_sums = {(dx, dy): [None, None] for dx in (-1, 1) for dy in (-1, 0, 1)}
    for side, flag in ((0, has_down), (1, has_up)):
        dx = 2 * side - 1
        for g in range(2 * levels // ROWS):
            t0, t1 = tiles(inside(first_r[side, g], flag))
            plus_pair, minus_pair = seam(
                lane_roll(t0, -1), lane_roll(t1, -1), lane_roll(t0, 1), lane_roll(t1, 1)
            )
            by_lane = {0: [t0, t1], 1: plus_pair, -1: minus_pair}
            for dy in (-1, 0, 1):
                weight = tiles(pack_v[1 if dy else 0, side, g])
                for j in range(2):
                    add(row_sums, (dx, dy), j, weight[j] * by_lane[dy][j])

    for (dx, dy), pair in sums.items():
        for j in range(2):
            value = pair[j]
            if dx:
                beyond = jnp.sum(row_sums[dx, dy][j], axis=0, keepdims=True)
                value = jnp.where(row_last if dx > 0 else row_first, beyond, row_roll(value, -dx))
            if dy and j == (dy + 1) // 2:
                value = jnp.where(lane_last if dy > 0 else lane_first, edge_sums[dx, dy], value)
            pair[j] = value
    scaled = [(0.5 * OFFSET_WEIGHT) * t for t in tiles(gain)]
    coefs = []
    for i, n in enumerate(NEIGHBOURS):
        pair = [scaled[j] * sums[n][j] for j in range(2)]
        coefs.append(jnp.concatenate(pair, axis=1))
        krow_s[i, :, :LANES] = pair[0]
        krow_s[i, :, LANES:] = pair[1]
    kedge_s[0] = pack_edges(coefs)
    exchange_edges(1, kedge_s, kedge_r, lambda k: krow_s, krow_r)

    greeted(1)
    greet(2)

    group_right = lane_id % 16 < 8

    def wide(values, row_ref, start, edge_ref, part):
        joined = join_edges(edge_ref, part, group_right)
        out = []
        for f, value in enumerate(values):
            rows = [
                tiles(value),
                tiles(inside(row_ref[1, start + f], has_up)),
                tiles(inside(row_ref[0, start + f], has_down)),
            ]
            out.append(
                [rows[i] + [lane_roll(joined[i], -16 * f)] for i in range(3)]
            )
        return out

    *source, half_obs, diag, grad, warm = wide(fields, first_r, wtiles, edge_r, 1)

    def each(fn, *args):
        return [[fn(*(a[i][j] for a in args)) for j in range(3)] for i in range(len(args[0]))]

    def from_row(a, dx):
        if dx == 0:
            return a
        mask = row_first if dx > 0 else row_last
        return [
            [row_roll(jnp.where(mask, a[(i + dx) % len(a)][j], a[i][j]), -dx) for j in range(3)]
            for i in range(len(a))
        ]

    def from_lane(a, dy):
        if dy == 0:
            return a
        mask = lane_first if dy > 0 else lane_last
        return [
            [lane_roll(jnp.where(mask, a[i][(j + dy) % 3], a[i][j]), -dy) for j in range(3)]
            for i in range(len(a))
        ]

    def plus(*args):
        return each(lambda *t: functools.reduce(lambda a, b: a + b, t), *args)

    def times(a, b):
        return each(lambda s, t: s * t, a, b)

    def narrow(a):
        return [a[0], [jnp.where(row_id < ROWS // 2, a[1][j], a[2][j]) for j in range(3)]]

    def from_row_narrow(a, dx):
        if len(a) == 2:
            return from_row(a, dx)
        if dx == 0:
            return narrow(a)
        mask, last_up = (row_first, ROWS // 2) if dx > 0 else (row_last, ROWS // 2 - 2)
        beyond = [jnp.where(row_id <= last_up, a[1][j], a[2][j]) for j in range(3)]
        return [
            [row_roll(jnp.where(mask, a[dx % 3][j], a[0][j]), -dx) for j in range(3)],
            [row_roll(jnp.where(mask, a[0][j], beyond[j]), -dx) for j in range(3)],
        ]

    def inner(a):
        return from_row_narrow(a, 0)

    def smooth(q):
        return each(
            lambda c, a, b, d, e: REG_GAMMA * (c + REG_SMOOTH * (4.0 * c - (a + b + d + e))),
            inner(q), from_row_narrow(q, 1), from_row_narrow(q, -1),
            from_lane(inner(q), 1), from_lane(inner(q), -1),
        )

    def to_surface(op, q):
        out = []
        for c in range(2):
            spread = times(op.source[c], q)
            result = spread
            for dy in (-1, 0, 1):
                near_lane = from_lane(spread, dy)
                for dx in (-1, 0, 1):
                    if (dx, dy) != (0, 0):
                        result = plus(result, times(op.stencil[c][dx, dy], from_row(near_lane, dx)))
            out.append(result)
        return out

    def to_bed(op, surface):
        out = []
        for c in range(2):
            traction = times(op.half_obs, surface[c])
            result = inner(traction)
            for dy in (-1, 0, 1):
                gathered = None
                for dx in (-1, 0, 1):
                    if (dx, dy) != (0, 0):
                        term = from_row_narrow(times(op.stencil[c][-dx, -dy], traction), dx)
                        gathered = term if gathered is None else plus(gathered, term)
                result = plus(result, from_lane(gathered, dy))
            out.append(times(inner(op.source[c]), result))
        return plus(*out)

    def hessian(op, q):
        return plus(to_bed(op, to_surface(op, q)), smooth(q))

    def operator(source, half_obs, coefs):
        return Operator(source, half_obs, [
            {
                (dx, dy): each(lambda t: (1.0 + sign * CROSS_SHARE * dx * dy) * t, value) if dx * dy else value
                for (dx, dy), value in coefs.items()
            }
            for sign in (1, -1)
        ])

    greeted(2)
    greet(3)
    all_neighbours(wahead_v, 16, 1, recv_sem.at[1])
    coefs = dict(zip(NEIGHBOURS, wide(coefs, krow_r, 0, kedge_r, 0)))
    resid = each(lambda a, b: a - b, narrow(grad), hessian(operator(source, half_obs, coefs), warm))
    diag = narrow(diag)
    op = operator([narrow(t) for t in source], narrow(half_obs), {n: narrow(t) for n, t in coefs.items()})
    dir0 = times(diag, resid)
    img0 = hessian(op, dir0)
    dir1 = times(diag, img0)
    surf1 = to_surface(op, dir1)
    smooth1 = smooth(dir1)

    def own_sum(fn):
        t = fn(0) + fn(1)
        return jnp.sum(t, axis=0, keepdims=True)

    dots = [
        own_sum(lambda j: resid[0][j] * dir0[0][j]),
        own_sum(lambda j: dir0[0][j] * img0[0][j]),
        own_sum(lambda j: img0[0][j] * dir1[0][j]),
        own_sum(
            lambda j: half_obs[0][j] * (surf1[0][0][j] * surf1[0][0][j] + surf1[1][0][j] * surf1[1][0][j])
            + dir1[0][j] * smooth1[0][j]
        ),
    ]
    partial = jnp.zeros((ROWS, LANES), F32)
    for q, value in enumerate(dots):
        partial = jnp.where(row_id == q, value, partial)
    partial = jnp.sum(partial, axis=1, keepdims=True)
    partial = jnp.sum(jnp.where(lane_id // 32 == row_id, partial, 0.0), axis=0, keepdims=True)

    def gather_sums(ref, sem, n):
        settle(ref, n - 1, sem)
        parts = [ref[k] for k in range(min(8, n))]
        for k in range(8, n):
            parts[k % 8] = parts[k % 8] + ref[k]
        while len(parts) > 1:
            parts = [functools.reduce(lambda a, b: a + b, parts[k : k + 2]) for k in range(0, len(parts), 2)]
        return parts[0]

    sum_s[...] = partial
    me = my * nx + mx
    greeted(3)
    circ = lambda v, n: min(v % n, n - v % n)
    far = lambda o: circ(o[0] / 2, nx // 2) + circ(o[1] % 4, 4) + circ(o[1] // 4, 4)
    offsets = sorted(
        [(i, j) for i in range(nx) for j in range(ny) if (i, j) != (0, 0)], key=far, reverse=True
    )
    for i, j in offsets:
        pltpu.make_async_remote_copy(
            src_ref=sum_s, dst_ref=sum_r.at[me], send_sem=sum_send, recv_sem=sum_recv,
            device_id=(lax.rem(mx + i, nx), lax.rem(my + j, ny)), device_id_type=MESH,
        ).start()
    sum_r[me] = partial
    img1 = plus(to_bed(op, surf1), smooth1)
    all_neighbours(wahead_v, 16, 1, send_sem.at[1])
    partial = gather_sums(sum_r, sum_recv, nx * ny)
    s0, s1, s2, s3 = (
        jnp.broadcast_to(partial[:, 32 * q : 32 * q + 1], (ROWS, LANES)) for q in range(4)
    )

    step0 = s0 / s1
    ratio = (step0 * step0 * s2 - s0) / s0
    grow = 1.0 + ratio
    bend = grow * grow * s1 - 2.0 * grow * step0 * s2 + step0 * step0 * s3
    step1 = ratio * s0 / bend
    for j in range(2):
        cols = slice(j * LANES, (j + 1) * LANES)
        sol_o[:, cols] = warm[0][j] + step0 * dir0[0][j]
        res_o[:, cols] = resid[0][j] - step0 * img0[0][j]
        step_o[:, cols] = step1
        along_o[:, cols] = grow * dir0[0][j] - step0 * dir1[0][j]
        image_o[:, cols] = grow * img0[0][j] - step0 * img1[0][j]

    settle(sum_r, nx * ny - 1, sum_send)


def solution(mesh):
    nx, ny = mesh.shape["gx"], mesh.shape["gy"]

    def on_device(grad, warm, eta, coef, slide, weight, ice, ground):
        levels, rows, cols = eta.shape
        vmem = lambda *shape: pltpu.VMEM(shape, F32)
        wtiles = 2 * levels // ROWS
        dma = lambda *shape: pltpu.SemaphoreType.DMA(shape)
        call = pl.pallas_call(
            functools.partial(kernel, nx=nx, ny=ny, levels=levels),
            out_shape=(pltpu.VMEM((rows, cols), F32),) * 5,
            in_specs=[pl.BlockSpec(memory_space=pl.ANY)] * 8,
            out_specs=(pl.BlockSpec(memory_space=pltpu.VMEM),) * 5,
            scratch_shapes=[
                vmem(rows, cols), vmem(rows, cols), vmem(levels, rows, cols), vmem(rows, cols),
                vmem(2, rows, cols), vmem(rows, cols),
                pltpu.VMEM((rows, cols), jnp.int32), pltpu.VMEM((rows, cols), jnp.int32),
                vmem(2 * levels, rows, cols), vmem(2 * levels, rows, LANES), vmem(2 * levels, rows, LANES),
                vmem(levels, rows, cols), vmem(levels, rows, cols), vmem(2, 2, wtiles, rows, cols),
                vmem(2, wtiles + 6, rows, cols), vmem(2, wtiles + 6, rows, cols),
                vmem(2, rows, LANES), vmem(6, 2, rows, LANES),
                vmem(8, rows, cols), vmem(2, 8, rows, cols),
                vmem(1, rows, LANES), vmem(6, 1, rows, LANES),
                vmem(1, LANES), vmem(nx * ny, 1, LANES),
                dma(2), dma(2), dma(2), pltpu.SemaphoreType.REGULAR((4,)), dma(), dma(),
            ],
            compiler_params=pltpu.CompilerParams(collective_id=0, has_side_effects=True),
        )
        sol, res, step, along, image = call(grad, warm, eta, coef, slide, weight, ice, ground)
        return sol + step * along, res - step * image

    return jax.shard_map(
        on_device,
        mesh=mesh,
        in_specs=(
            P("gx", "gy"), P("gx", "gy"), P(None, "gx", "gy"), P("gx", "gy"),
            P(None, "gx", "gy"), P("gx", "gy"), P("gx", "gy"), P("gx", "gy"),
        ),
        out_specs=(P("gx", "gy"), P("gx", "gy")),
        check_vma=False,
    )
```
